32 devices in a mesh: wide: 8 (over z, y), narrow: 4 (over x, core).
Axes of the slice: x: 2, y: 2, z: 4, core: 2. Of those that a mesh axis runs over, the one named last changes fastest.
Arguments:
- targets: float32 [32768, 64], P(('wide', 'narrow')), may hold values from -6 to 6
- train_features: bfloat16 [32768, 128], P(('wide', 'narrow')), may hold values from -6 to 6
- test_features: bfloat16 [1024, 128], P(('wide', 'narrow')), may hold values from -6 to 6
- left_factors: float32 [32768, 4, 128], P(('wide', 'narrow')), may hold values from -0.5 to 0.5
- right_factors: float32 [32768, 4, 128], P(('wide', 'narrow')), may hold values from -0.03125 to 0.03125
- capacitance: float32 [15, 256, 256], replicated, may hold values from -0.375 to 0.375
- pivots: int32 [15, 256], replicated, may hold values from 0 to 255, each once within a row
Outputs:
- solved_targets: float32 [32768, 64], P(('wide', 'narrow'))
- predictions: float32 [1024, 64], P(('wide', 'narrow'))
The draws below stay inside these ranges and needn't reach their ends.
Inputs may be any that keep to these rules, and one draw needn't show every extreme that they name: `pivots`: each row is a permutation of 0 .. 255.
All inputs are finite; a program needn't handle non-finite values.
Results may differ from the reference program's by a relative error of at most 0.0049.
Values may be sent and summed in bfloat16 or wider, within the bound.
A program may use at most 128 MiB of HBM per device.

```python
import jax
import jax.numpy as jnp
from jax import lax

R = 128
FEAT = 128
TARGETS = 64
LEVELS = 4
NODES = 15
POINTS = 32768
TESTS = 1024


def steps_of(own_key, extent, pieces, low, top_value):
    factor_of = 1.0
    for dim, shards_of in pieces:
        steps = jax.random.uniform(jax.random.fold_in(jax.random.fold_in(own_key, 6), dim), (shards_of,), jnp.float32, low / len(pieces), top_value / len(pieces))
        factor_of = factor_of * jnp.repeat(jnp.exp(steps), extent[dim] // shards_of).reshape((-1,) + (1,) * (len(extent) - 1 - dim))
    return factor_of


def bell_draw(own_key, extent, scale, most, shards=(), kind=jnp.bfloat16):
    entries = jax.random.normal(own_key, extent, jnp.float32) * scale
    if len(shards) > 0:
        entries = steps_of(own_key, extent, shards, -0.22, 0.18) * entries
    return jnp.clip(entries, min=-most, max=most).astype(kind)


def setup_inputs(seed: int = 0) -> dict:
    key_of = jax.random.split(jax.random.key(seed), 8)
    return {
        "targets": bell_draw(key_of[0], (POINTS, TARGETS), 1.0, 6.0, ((0, 32),), jnp.float32),
        "train_features": bell_draw(key_of[1], (POINTS, FEAT), 1.0, 6.0, ((0, 32),)),
        "test_features": bell_draw(key_of[2], (TESTS, FEAT), 1.0, 6.0, ((0, 32),)),
        "left_factors": bell_draw(key_of[3], (POINTS, LEVELS, R), R ** -0.5, 0.5, ((0, 32),), jnp.float32),
        "right_factors": bell_draw(key_of[4], (POINTS, LEVELS, R), POINTS ** -0.5, 0.03125, ((0, 32),), jnp.float32),
        "capacitance": bell_draw(key_of[5], (NODES, 2 * R, 2 * R), (2 * R) ** -0.5, 0.375, (), jnp.float32),
        "pivots": jax.vmap(lambda own: jax.random.permutation(own, 2 * R))(jax.random.split(key_of[6], NODES)).reshape((NODES, 2 * R)).astype(jnp.int32),
    }


spread_coef = 3.0


def level_update(current, left_level, right_level, capacitance, pivots, tree_level):
    children = 2 ** tree_level
    nodes = children // 2
    offset = nodes - 1
    per_child = POINTS // children
    right_blocks = right_level.reshape(children, per_child, R)
    left_blocks = left_level.reshape(children, per_child, R)
    value_blocks = current.reshape(children, per_child, TARGETS)
    projected = jnp.einsum("cpr,cpt->crt", right_blocks, value_blocks, precision=lax.Precision.HIGHEST)
    paired = projected.reshape(nodes, 2, R, TARGETS)
    stacked = jnp.concatenate([paired[:, 1], paired[:, 0]], axis=1)
    node_pivots = pivots[offset:offset + nodes].astype(jnp.int32)
    permuted = jnp.take_along_axis(stacked, node_pivots[:, :, None], axis=1)
    caps = capacitance[offset:offset + nodes]
    solved = jnp.einsum("nij,njt->nit", caps, permuted, precision=lax.Precision.HIGHEST)
    shares = solved.reshape(children, R, TARGETS)
    update = jnp.einsum("cpr,crt->cpt", left_blocks, shares, precision=lax.Precision.HIGHEST)
    return current - update.reshape(POINTS, TARGETS)


def reference(targets, train_features, test_features, left_factors, right_factors, capacitance, pivots):
    current = targets.astype(jnp.float32)
    for tree_level in range(1, LEVELS + 1):
        current = level_update(current, left_factors[:, tree_level - 1, :], right_factors[:, tree_level - 1, :], capacitance, pivots, tree_level)
    weights_bf = current.astype(jnp.bfloat16)
    train_float = train_features.astype(jnp.float32)
    train_sq = jnp.sum(train_float * train_float, axis=1)
    block_rows = 128 if TESTS % 128 == 0 else TESTS
    blocks = test_features.reshape(TESTS // block_rows, block_rows, FEAT)

    def predict_block(rows_in):
        rows_float = rows_in.astype(jnp.float32)
        row_sq = jnp.sum(rows_float * rows_float, axis=1)
        inner = lax.dot_general(rows_in, train_features, (((1,), (1,)), ((), ())), preferred_element_type=jnp.float32)
        dist = row_sq[:, None] + train_sq[None, :] - 2.0 * inner
        kernel = jnp.exp(-(spread_coef / FEAT) * dist).astype(jnp.bfloat16)
        return jnp.dot(kernel, weights_bf, preferred_element_type=jnp.float32)

    predictions = lax.map(predict_block, blocks).reshape(TESTS, TARGETS)
    return current, predictions
```

```python
import functools
import math
import types

import jax
import jax.numpy as jnp
from jax import lax
from jax.experimental import pallas as pl
from jax.experimental.pallas import tpu as pltpu
from jax.sharding import PartitionSpec as P

LEVELS = 4
OCTET = 8
spread_coef = 3.0
MESH = pl.DeviceIdType.MESH
f32, bf16 = jnp.float32, jnp.bfloat16


def dot(a, b):
    return jnp.dot(a, b, preferred_element_type=f32)


def dot_nt(a, b):
    return lax.dot_general(a, b, (((1,), (1,)), ((), ())), preferred_element_type=f32)


def split(value):
    high = value.astype(bf16)
    return high, (value - high.astype(f32)).astype(bf16)


def halves_of(value):
    high = value.astype(bf16).astype(f32)
    return high, value - high


def group_of(n_dev, level):
    node = n_dev >> (level - 1)
    size = min(OCTET, node)
    return size, node // size


def kernel(n_dev, narrow, names, *refs):
    r = types.SimpleNamespace(**dict(zip(names, refs)))
    pos = lax.axis_index("wide") * narrow + lax.axis_index("narrow")
    width, points = r.tgt.shape
    rank = r.right.shape[2]
    feat = r.train.shape[2]
    rows = r.test_h.shape[0]
    half = rows // 2
    pairs = n_dev // 2
    parity = pos % 2
    slot = pos // 2
    own_rows = pl.ds(pl.multiple_of(slot * half, half), half)

    def coords(dev):
        return (dev // narrow, dev % narrow)

    def flip(mask):
        dev = pos
        for bit in range(mask.bit_length()):
            if mask >> bit & 1:
                dev = dev + (1 << bit) * (1 - 2 * ((pos // (1 << bit)) % 2))
        return coords(dev)

    def remote(src, dst, send_sem, recv_sem, where):
        pltpu.make_async_remote_copy(
            src_ref=src, dst_ref=dst, send_sem=send_sem, recv_sem=recv_sem,
            device_id=where, device_id_type=MESH,
        ).start()

    def drain(part, sem):
        pltpu.make_async_copy(part, part, sem).wait()

    def load(src, dst, sem):
        copy = pltpu.make_async_copy(src, dst, sem)
        copy.start()
        return copy

    test_loads = [
        load(r.test_h.at[pl.ds(h * half, half)], r.gath.at[h, own_rows], r.load_sem.at[0 + h])
        for h in range(2)
    ]
    tgt_load = load(r.tgt_h, r.tgt, r.load_sem.at[2])
    right_loads, left_loads = [], []
    train_load = None
    for lev in range(LEVELS):
        right_loads.append(load(r.right_h.at[:, lev, :], r.right.at[lev], r.load_sem.at[4 + lev]))
        if lev == 0:
            train_load = load(r.train_h, r.train.at[0], r.load_sem.at[3])
        left_loads.append(
            load(r.left_h.at[:, lev, :], r.left.at[lev], r.load_sem.at[4 + LEVELS + lev])
        )
    cap_loads, odds, heaps = [], [], []
    for level in range(1, LEVELS + 1):
        child = pos // (n_dev >> level)
        odd = child % 2
        odds.append(odd)
        heaps.append((1 << level - 1) - 1 + child // 2)
        cap_loads.append([
            load(
                r.cap_h.at[heaps[-1], pl.ds(pl.multiple_of(which * rank, rank), rank)],
                r.cap.at[level - 1, pl.ds(at * rank, rank)],
                r.cap_sem.at[level - 1, at],
            )
            for at, which in enumerate((odd, 1 - odd))
        ])

    barrier = pltpu.get_barrier_semaphore()

    def greet(k, carry):
        pl.semaphore_signal(
            barrier, inc=1, device_id=coords((pos + 2 * k) % n_dev), device_id_type=MESH
        )
        return carry

    lax.fori_loop(1, pairs, greet, 0)
    crossing = range(1, OCTET, 2)
    for k in crossing:
        pl.semaphore_signal(barrier, inc=1, device_id=flip(k), device_id_type=MESH)
    pl.semaphore_wait(barrier, pairs - 1 + len(crossing))

    for copy in test_loads:
        copy.wait()
    own_test = r.gath.at[:, own_rows]

    def spread(k, carry):
        remote(own_test, own_test, r.ag_send, r.ag_recv, coords((pos + 2 * k) % n_dev))
        return carry

    lax.fori_loop(1, pairs, spread, 0)

    def first_send(level):
        size, _ = group_of(n_dev, level)
        mine = pos % size
        lev = level - 1
        for k in range(1, size):
            to = mine
            for bit in range(k.bit_length()):
                if k >> bit & 1:
                    to = to + (1 << bit) * (1 - 2 * ((mine // (1 << bit)) % 2))
            remote(
                getattr(r, f"send{level}").at[to], getattr(r, f"recv{level}").at[k],
                r.p1_send.at[lev], r.p1_recv.at[lev], flip(k),
            )

    def gram(level):
        lev = level - 1
        size, _ = group_of(n_dev, level)
        right_loads[lev].wait()
        high, low = split(r.right[lev])
        product = dot(r.stack[pl.ds(0, 2 * width + lev * rank)], high)
        t = product[:width] + product[width : 2 * width] + dot(r.stack[pl.ds(0, width)], low)
        t_high, t_low = halves_of(t)
        part = width // size
        both = jnp.concatenate(
            [t_high.reshape(size, part, rank), t_low.reshape(size, part, rank)], axis=1
        )
        send = getattr(r, f"send{level}")
        send[:, pl.ds(0, 2 * part)] = both.astype(bf16)
        cut = rank // size
        for k in range(lev):
            piece = product[2 * width + k * rank : 2 * width + (k + 1) * rank]
            send[:, pl.ds(2 * part + k * cut, cut)] = piece.astype(bf16).reshape(size, cut, rank)
        first_send(level)

    def turn(lev):
        left_loads[lev].wait()
        high, low = split(r.left[lev].T)
        r.stack[pl.ds(2 * width + lev * rank, rank)] = high
        r.ltl[pl.ds(lev * rank, rank)] = low

    sums = {}

    def joined(value, level):
        part = width // group_of(n_dev, level)[0]
        top = value[:part] + value[part : 2 * part]
        return top if level == 1 else jnp.concatenate([top, value[2 * part :]], axis=0)

    def packed(value, level):
        part = width // group_of(n_dev, level)[0]
        high, low = halves_of(value[:part])
        pieces = [high, low] if level == 1 else [high, low, value[part:]]
        return jnp.concatenate(pieces, axis=0).astype(bf16)

    def first_take(level):
        size, count = group_of(n_dev, level)
        lev = level - 1
        recv, send = getattr(r, f"recv{level}"), getattr(r, f"send{level}")
        drain(recv.at[pl.ds(1, size - 1)], r.p1_recv.at[lev])
        near = send[pos % size].astype(f32)
        far = None
        for k in range(1, size):
            value = recv[k].astype(f32)
            if count > 1 or k < size // 2:
                near = near + value
            else:
                far = value if far is None else far + value
        near = joined(near, level)
        if count == 1:
            sums[level] = (near, joined(far, level))
            return
        sums[level] = (near, None)
        hop = getattr(r, f"hop{level}")
        hop[0] = packed(near, level)
        for j in range(1, count):
            remote(hop.at[0], hop.at[j], r.p2_send.at[lev], r.p2_recv.at[lev], flip(j * OCTET))

    def second_take(level):
        size, count = group_of(n_dev, level)
        if count == 1:
            return
        hop = getattr(r, f"hop{level}")
        drain(hop.at[pl.ds(1, count - 1)], r.p2_recv.at[level - 1])
        near, far = sums[level][0], None
        for j in range(1, count):
            value = joined(hop[j].astype(f32), level)
            if j < count // 2:
                near = near + value
            else:
                far = value if far is None else far + value
        sums[level] = (near, far)

    def solve(level):
        size, count = group_of(n_dev, level)
        lev = level - 1
        near, far = sums[level]
        cols = near.shape[0]
        both = jnp.concatenate([near, far], axis=1)
        high, low = halves_of(both)
        moved = dot(jnp.concatenate([high, low], axis=0).astype(bf16), r.chosen[lev])
        kids = 1 if count > 1 else 2
        cap_high = r.caps[0, lev, pl.ds(0, kids * rank)]
        cap_low = r.caps[1, lev, pl.ds(0, kids * rank)]
        result = dot_nt(moved.astype(bf16), cap_high)
        result = result[:cols] + result[cols:] + dot_nt(moved[:cols].astype(bf16), cap_low)
        share, out = getattr(r, f"share{level}"), getattr(r, f"out{level}")
        for kid in range(kids):
            out[kid] = packed(result[:, kid * rank : (kid + 1) * rank], level)
        mine = pos % size
        for k in range(1, size):
            kid = 1 if count == 1 and k >= size // 2 else 0
            remote(
                out.at[kid], share.at[mine], r.p3_send.at[lev], r.p3_recv.at[lev], flip(k)
            )
        share[mine] = out[0]

    def gathered(level):
        size, _ = group_of(n_dev, level)
        share = getattr(r, f"share{level}")
        drain(share.at[pl.ds(0, size - 1)], r.p3_recv.at[level - 1])
        part, cut = width // size, rank // size
        top = share[:, pl.ds(0, 2 * part)].astype(f32)
        top = (top[:, :part] + top[:, part:]).reshape(width, rank)
        return [top] + [
            share[:, pl.ds(2 * part + k * cut, cut)].reshape(rank, rank) for k in range(level - 1)
        ]

    def prepare(lev):
        for copy in cap_loads[lev]:
            copy.wait()
        high, low = split(r.cap[lev])
        r.caps[0, lev] = high
        r.caps[1, lev] = low
        order = lax.broadcasted_iota(jnp.int32, (2 * rank, 2 * rank), 0)
        pivots = r.piv_ref[pl.ds(heaps[lev], 1), :]
        at = pivots + rank * (1 - odds[lev])
        at = jnp.where(at >= 2 * rank, at - 2 * rank, at)
        r.chosen[lev] = (order == at).astype(f32).astype(bf16)

    def widened(value, own_squares_at, ones_at):
        value_f = value.astype(f32)
        high, low = split(value_f * value_f)
        squares = dot(
            jnp.concatenate([high, low], axis=1), jnp.ones((2 * feat, feat), bf16)
        )
        one = squares.astype(bf16).astype(f32)
        two = (squares - one).astype(bf16).astype(f32)
        three = squares - one - two
        lane = lax.broadcasted_iota(jnp.int32, squares.shape, 1)
        extra = jnp.where((lane >= ones_at) & (lane < ones_at + 3), 1.0, 0.0)
        for i, piece in enumerate((one, two, three)):
            extra = jnp.where(lane == own_squares_at + i, -piece, extra)
        return extra.astype(bf16)

    def widen_train(which):
        value = r.train[which]
        r.train_w[which, :, pl.ds(0, feat)] = value + value
        r.train_w[which, :, pl.ds(feat, feat)] = widened(value, 3, 0)

    def widen_tests():
        def step(i, carry):
            part = pl.ds(pl.multiple_of(i * wide_rows, wide_rows), wide_rows)
            for h in range(2):
                value = r.gath[h, part]
                r.test_w[h, part, pl.ds(0, feat)] = value
                r.test_w[h, part, pl.ds(feat, feat)] = widened(value, 0, 3)
            return carry

        wide_rows = min(256, pairs * half)
        lax.fori_loop(0, pairs * half // wide_rows, step, 0)

    rate = spread_coef / feat * math.log2(math.e)
    chunk = min(128, pairs * half)

    def fill(which, h):
        def step(i, carry):
            part = pl.ds(pl.multiple_of(i * chunk, chunk), chunk)
            negative = dot_nt(r.test_w[h, part], r.train_w[which])
            r.kmat[h, part, pl.ds(which * points, points)] = jnp.exp2(rate * negative).astype(bf16)
            return carry

        lax.fori_loop(0, pairs * half // chunk, step, 0)

    train_load.wait()
    remote(r.train.at[0], r.train.at[1], r.tr_send, r.tr_recv, flip(1))
    tgt_load.wait()
    high, low = split(r.tgt[...])
    r.stack[pl.ds(0, width)] = high
    r.stack[pl.ds(width, width)] = low
    gram(1)
    widen_train(0)
    for level in range(2, LEVELS + 1):
        turn(level - 2)
        gram(level)
    for lev in range(LEVELS):
        prepare(lev)
    drain(r.gath.at[:, pl.ds(0, (pairs - 1) * half)], r.ag_recv)
    widen_tests()
    first_take(1)
    first_take(2)
    fill(0, 0)
    first_take(3)
    if group_of(n_dev, 3)[1] == 1:
        solve(3)
    second_take(1)
    solve(1)
    second_take(2)
    solve(2)
    if group_of(n_dev, 3)[1] > 1:
        second_take(3)
        solve(3)
    first_take(4)
    second_take(4)
    solve(4)
    drain(r.train.at[0], r.tr_recv)
    widen_train(1)
    fill(0, 1)
    fill(1, 0)
    fill(1, 1)
    turn(LEVELS - 1)
    zero = jnp.zeros((width, points), bf16)
    for which in range(2):
        r.wts[which, 0, pl.ds(width, width)] = zero
        r.wts[which, 1, pl.ds(0, width)] = zero

    pairs_ab = {}
    for level in range(2, LEVELS + 1):
        blocks = gathered(level)
        value = jnp.concatenate([blocks[0], blocks[1].astype(f32)], axis=0)
        for k in range(2, level):
            ab_high, ab_low = pairs_ab[k]
            value = value - dot(ab_high, blocks[k]) - dot(ab_low, blocks[k])
        pairs_ab[level] = split(value)
        r.ab[:, pl.ds((level - 2) * rank, rank)] = value
    b_high, b_low = split(r.ab[pl.ds(width, rank)])
    first = gathered(1)[0]
    s_high, s_low = split(first)
    later = r.ab[pl.ds(0, width)] - (dot(s_high, b_high) + dot(s_low, b_high) + dot(s_high, b_low))
    shares = jnp.concatenate([first, later], axis=1)
    share_high, share_low = split(shares)
    left_high = r.stack[pl.ds(2 * width, LEVELS * rank)]
    current = r.tgt[...] - (
        dot(share_high, left_high) + dot(share_low, left_high) + dot(share_high, r.ltl[...])
    )
    r.cur[...] = current
    weights = current.astype(bf16)
    r.wts[0, 0, pl.ds(0, width)] = weights
    r.wts[0, 1, pl.ds(width, width)] = weights
    r.wt[0] = weights
    remote(r.wt.at[0], r.wt.at[1], r.wt_send, r.wt_recv, flip(1))
    cur_copy = pltpu.make_async_copy(r.cur, r.cur_out, r.out_sem)
    cur_copy.start()

    big = min(256, pairs * half)

    def weigh(which):
        def step(i, carry):
            part = pl.ds(pl.multiple_of(i * big, big), big)
            there = pl.ds(which * points, points)
            value = dot_nt(r.kmat[0, part, there], r.wts[which, 0]) + dot_nt(
                r.kmat[1, part, there], r.wts[which, 1]
            )
            if which == 0:
                r.terms[part] = value
            else:
                r.term_b[part] = (r.terms[part] + value).astype(bf16)
            return carry

        lax.fori_loop(0, pairs * half // big, step, 0)

    weigh(0)
    drain(r.wt.at[1], r.wt_recv)
    weights = r.wt[1]
    r.wts[1, 0, pl.ds(0, width)] = weights
    r.wts[1, 1, pl.ds(width, width)] = weights
    weigh(1)

    def scatter(k, carry):
        to = (slot + k) % pairs
        remote(
            r.term_b.at[pl.ds(pl.multiple_of(to * half, half), half)],
            r.term_in.at[pl.ds(pl.multiple_of((k - 1) * half, half), half)],
            r.rs_send, r.rs_recv, coords(2 * to + parity),
        )
        return carry

    lax.fori_loop(1, pairs, scatter, 0)
    drain(r.gath.at[:, pl.ds(0, (pairs - 1) * half)], r.ag_send)
    drain(r.train.at[0], r.tr_send)
    drain(r.wt.at[0], r.wt_send)
    for level in range(1, LEVELS + 1):
        size, count = group_of(n_dev, level)
        lev = level - 1
        drain(getattr(r, f"recv{level}").at[pl.ds(1, size - 1)], r.p1_send.at[lev])
        if count > 1:
            drain(getattr(r, f"hop{level}").at[pl.ds(1, count - 1)], r.p2_send.at[lev])
        drain(getattr(r, f"share{level}").at[pl.ds(0, size - 1)], r.p3_send.at[lev])
    cur_copy.wait()
    total = r.term_b[own_rows].astype(f32)
    drain(r.term_in, r.rs_recv)
    total = total + jnp.sum(r.term_in[...].astype(f32).reshape(pairs - 1, half, 2 * width), axis=0)
    r.pred_out[pl.ds(0, half)] = total[:, :width]
    r.pred_out[pl.ds(half, half)] = total[:, width:]
    drain(r.term_in, r.rs_send)


def body(n_dev, narrow, targets, train, test, left, right, cap, pivots):
    points, width = targets.shape
    rank = left.shape[2]
    feat = train.shape[1]
    rows = test.shape[0]
    half = rows // 2
    pairs = n_dev // 2
    vmem = pltpu.VMEM
    dma = pltpu.SemaphoreType.DMA
    hbm_spec = pl.BlockSpec(memory_space=pl.ANY)
    vmem_spec = pl.BlockSpec(memory_space=pltpu.VMEM)
    scratch = {
        "tgt": vmem((width, points), f32),
        "train": vmem((2, points, feat), bf16),
        "gath": vmem((2, pairs * half, feat), bf16),
        "left": vmem((LEVELS, points, rank), f32),
        "right": vmem((LEVELS, points, rank), f32),
        "cap": vmem((LEVELS, 2 * rank, 2 * rank), f32),
        "caps": vmem((2, LEVELS, 2 * rank, 2 * rank), bf16),
        "chosen": vmem((LEVELS, 2 * rank, 2 * rank), bf16),
        "stack": vmem((2 * width + LEVELS * rank, points), bf16),
        "ltl": vmem((LEVELS * rank, points), bf16),
        "train_w": vmem((2, points, 2 * feat), bf16),
        "test_w": vmem((2, pairs * half, 2 * feat), bf16),
        "kmat": vmem((2, pairs * half, 2 * points), bf16),
        "ab": vmem((width + rank, (LEVELS - 1) * rank), f32),
        "cur": vmem((width, points), f32),
        "wt": vmem((2, width, points), bf16),
        "wts": vmem((2, 2, 2 * width, points), bf16),
        "terms": vmem((pairs * half, 2 * width), f32),
        "term_b": vmem((pairs * half, 2 * width), bf16),
        "term_in": vmem(((pairs - 1) * half, 2 * width), bf16),
    }
    for level in range(1, LEVELS + 1):
        size, count = group_of(n_dev, level)
        tall = (2 * width + (level - 1) * rank) // size
        for name in ("send", "recv", "share"):
            scratch[f"{name}{level}"] = vmem((size, tall, rank), bf16)
        scratch[f"out{level}"] = vmem((2, tall, rank), bf16)
        if count > 1:
            scratch[f"hop{level}"] = vmem((count, tall, rank), bf16)
    scratch["load_sem"] = dma((4 + 2 * LEVELS,))
    scratch["cap_sem"] = dma((LEVELS, 2))
    for name in ("p1_send", "p1_recv", "p2_send", "p2_recv", "p3_send", "p3_recv"):
        scratch[name] = dma((LEVELS,))
    for name in (
        "ag_send", "ag_recv", "tr_send", "tr_recv", "wt_send", "wt_recv", "rs_send", "rs_recv",
        "out_sem",
    ):
        scratch[name] = dma
    names = ["tgt_h", "train_h", "test_h", "left_h", "right_h", "cap_h", "piv_ref"]
    names += ["cur_out", "pred_out"] + list(scratch)
    current, predictions = pl.pallas_call(
        functools.partial(kernel, n_dev, narrow, names),
        out_shape=(
            jax.ShapeDtypeStruct((width, points), f32),
            jax.ShapeDtypeStruct((rows, width), f32),
        ),
        in_specs=[hbm_spec] * 6 + [vmem_spec],
        out_specs=(hbm_spec, vmem_spec),
        scratch_shapes=list(scratch.values()),
        compiler_params=pltpu.CompilerParams(
            collective_id=0, has_side_effects=True, vmem_limit_bytes=60 * 1024 * 1024
        ),
    )(targets.T, train, test, left, right, cap, pivots)
    return current.T, predictions


def solution(mesh):
    both = ("wide", "narrow")
    placed = (
        P(both, None), P(both, None), P(both, None),
        P(both, None, None), P(both, None, None), P(), P(),
    )
    sizes = dict(mesh.shape)
    return jax.shard_map(
        functools.partial(body, sizes["wide"] * sizes["narrow"], sizes["narrow"]),
        mesh=mesh,
        in_specs=placed,
        out_specs=(P(both, None), P(both, None)),
        check_vma=False,
    )
```

```python
import functools
import math
import types

import jax
import jax.numpy as jnp
from jax import lax
from jax.experimental import pallas as pl
from jax.experimental.pallas import tpu as pltpu
from jax.sharding import PartitionSpec as P

LEVELS = 4
OCTET = 8
spread_coef = 3.0
MESH = pl.DeviceIdType.MESH
f32, bf16 = jnp.float32, jnp.bfloat16


def dot(a, b):
    return jnp.dot(a, b, preferred_element_type=f32)


def dot_nt(a, b):
    return lax.dot_general(a, b, (((1,), (1,)), ((), ())), preferred_element_type=f32)


def split(value):
    high = value.astype(bf16)
    return high, (value - high.astype(f32)).astype(bf16)


def halves_of(value):
    high = value.astype(bf16).astype(f32)
    return high, value - high


def group_of(n_dev, level):
    node = n_dev >> (level - 1)
    size = min(OCTET, node)
    return size, node // size


def kernel(n_dev, narrow, names, *refs):
    r = types.SimpleNamespace(**dict(zip(names, refs)))
    pos = lax.axis_index("wide") * narrow + lax.axis_index("narrow")
    width, points = r.tgt.shape
    rank = r.right.shape[2]
    feat = r.train.shape[2]
    rows = r.test_h.shape[0]
    half = rows // 2
    pairs = n_dev // 2
    parity = pos % 2
    slot = pos // 2
    octets = n_dev // OCTET
    seat = slot % (OCTET // 2)
    own_block = seat * octets + slot // (OCTET // 2)
    own_rows = pl.ds(pl.multiple_of(own_block * half, half), half)
    seat_rows = pl.ds(pl.multiple_of(seat * octets * half, octets * half), octets * half)

    def coords(dev):
        return (dev // narrow, dev % narrow)

    def flip(mask):
        dev = pos
        for bit in range(mask.bit_length()):
            if mask >> bit & 1:
                dev = dev + (1 << bit) * (1 - 2 * ((pos // (1 << bit)) % 2))
        return coords(dev)

    def remote(src, dst, send_sem, recv_sem, where):
        pltpu.make_async_remote_copy(
            src_ref=src, dst_ref=dst, send_sem=send_sem, recv_sem=recv_sem,
            device_id=where, device_id_type=MESH,
        ).start()

    def drain(part, sem):
        pltpu.make_async_copy(part, part, sem).wait()

    def load(src, dst, sem):
        copy = pltpu.make_async_copy(src, dst, sem)
        copy.start()
        return copy

    test_loads = [
        load(r.test_h.at[pl.ds(h * half, half)], r.gath.at[h, own_rows], r.load_sem.at[0 + h])
        for h in range(2)
    ]
    tgt_load = load(r.tgt_h, r.tgt, r.load_sem.at[2])
    piv_load = load(r.piv_h, r.piv, r.piv_sem)
    right_loads, left_loads = [], []
    train_load = None
    for lev in range(LEVELS):
        right_loads.append(load(r.right_h.at[:, lev, :], r.right.at[lev], r.load_sem.at[4 + lev]))
        if lev == 0:
            train_load = load(r.train_h, r.train.at[0], r.load_sem.at[3])
        left_loads.append(
            load(r.left_h.at[:, lev, :], r.left.at[lev], r.load_sem.at[4 + LEVELS + lev])
        )
    cap_loads, odds, heaps = [], [], []
    for level in range(1, LEVELS + 1):
        child = pos // (n_dev >> level)
        odd = child % 2
        odds.append(odd)
        heaps.append((1 << level - 1) - 1 + child // 2)
        cap_loads.append([
            load(
                r.cap_h.at[heaps[-1], pl.ds(pl.multiple_of(which * rank, rank), rank)],
                r.cap.at[level - 1, pl.ds(at * rank, rank)],
                r.cap_sem.at[level - 1, at],
            )
            for at, which in enumerate((odd, 1 - odd))
        ])

    barrier = pltpu.get_barrier_semaphore()

    def greet(k, carry):
        pl.semaphore_signal(
            barrier, inc=1, device_id=coords((pos + OCTET * k) % n_dev), device_id_type=MESH
        )
        return carry

    lax.fori_loop(1, octets, greet, 0)
    for k in range(1, OCTET):
        pl.semaphore_signal(barrier, inc=1, device_id=flip(k), device_id_type=MESH)

    def first_send(level):
        size, _ = group_of(n_dev, level)
        mine = pos % size
        lev = level - 1
        for k in range(1, size):
            to = mine
            for bit in range(k.bit_length()):
                if k >> bit & 1:
                    to = to + (1 << bit) * (1 - 2 * ((mine // (1 << bit)) % 2))
            remote(
                getattr(r, f"send{level}").at[to], getattr(r, f"recv{level}").at[k],
                r.p1_send.at[lev], r.p1_recv.at[lev], flip(k),
            )

    def gram(level):
        lev = level - 1
        size, _ = group_of(n_dev, level)
        right_loads[lev].wait()
        high, low = split(r.right[lev])
        product = dot(r.stack[pl.ds(0, 2 * width + lev * rank)], high)
        t = product[:width] + product[width : 2 * width] + dot(r.stack[pl.ds(0, width)], low)
        t_high, t_low = halves_of(t)
        part = width // size
        both = jnp.concatenate(
            [t_high.reshape(size, part, rank), t_low.reshape(size, part, rank)], axis=1
        )
        send = getattr(r, f"send{level}")
        send[:, pl.ds(0, 2 * part)] = both.astype(bf16)
        cut = rank // size
        for k in range(lev):
            piece = product[2 * width + k * rank : 2 * width + (k + 1) * rank]
            send[:, pl.ds(2 * part + k * cut, cut)] = piece.astype(bf16).reshape(size, cut, rank)

    def turn(lev):
        left_loads[lev].wait()
        high, low = split(r.left[lev].T)
        r.stack[pl.ds(2 * width + lev * rank, rank)] = high
        r.ltl[pl.ds(lev * rank, rank)] = low

    sums = {}

    def joined(value, level):
        part = width // group_of(n_dev, level)[0]
        top = value[:part] + value[part : 2 * part]
        return top if level == 1 else jnp.concatenate([top, value[2 * part :]], axis=0)

    def packed(value, level):
        part = width // group_of(n_dev, level)[0]
        high, low = halves_of(value[:part])
        pieces = [high, low] if level == 1 else [high, low, value[part:]]
        return jnp.concatenate(pieces, axis=0).astype(bf16)

    def first_take(level):
        size, count = group_of(n_dev, level)
        lev = level - 1
        recv, send = getattr(r, f"recv{level}"), getattr(r, f"send{level}")
        drain(recv.at[pl.ds(1, size - 1)], r.p1_recv.at[lev])
        near = send[pos % size].astype(f32)
        far = None
        for k in range(1, size):
            value = recv[k].astype(f32)
            if count > 1 or k < size // 2:
                near = near + value
            else:
                far = value if far is None else far + value
        near = joined(near, level)
        if count == 1:
            sums[level] = (near, joined(far, level))
            return
        sums[level] = (near, None)
        hop = getattr(r, f"hop{level}")
        hop[0] = packed(near, level)
        for j in range(1, count):
            remote(hop.at[0], hop.at[j], r.p2_send.at[lev], r.p2_recv.at[lev], flip(j * OCTET))

    def second_take(level):
        size, count = group_of(n_dev, level)
        if count == 1:
            return
        hop = getattr(r, f"hop{level}")
        drain(hop.at[pl.ds(1, count - 1)], r.p2_recv.at[level - 1])
        near, far = sums[level][0], None
        for j in range(1, count):
            value = joined(hop[j].astype(f32), level)
            if j < count // 2:
                near = near + value
            else:
                far = value if far is None else far + value
        sums[level] = (near, far)

    def solve(level):
        size, count = group_of(n_dev, level)
        lev = level - 1
        near, far = sums[level]
        cols = near.shape[0]
        both = jnp.concatenate([near, far], axis=1)
        high, low = halves_of(both)
        moved = dot(jnp.concatenate([high, low], axis=0).astype(bf16), r.chosen[lev])
        kids = 1 if count > 1 else 2
        cap_high = r.caps[0, lev, pl.ds(0, kids * rank)]
        cap_low = r.caps[1, lev, pl.ds(0, kids * rank)]
        result = dot_nt(moved.astype(bf16), cap_high)
        result = result[:cols] + result[cols:] + dot_nt(moved[:cols].astype(bf16), cap_low)
        share, out = getattr(r, f"share{level}"), getattr(r, f"out{level}")
        for kid in range(kids):
            out[kid] = packed(result[:, kid * rank : (kid + 1) * rank], level)
        mine = pos % size
        for k in range(1, size):
            kid = 1 if count == 1 and k >= size // 2 else 0
            remote(
                out.at[kid], share.at[mine], r.p3_send.at[lev], r.p3_recv.at[lev], flip(k)
            )
        share[mine] = out[0]

    def gathered(level):
        size, _ = group_of(n_dev, level)
        share = getattr(r, f"share{level}")
        drain(share.at[pl.ds(0, size - 1)], r.p3_recv.at[level - 1])
        part, cut = width // size, rank // size
        top = share[:, pl.ds(0, 2 * part)].astype(f32)
        top = (top[:, :part] + top[:, part:]).reshape(width, rank)
        return [top] + [
            share[:, pl.ds(2 * part + k * cut, cut)].reshape(rank, rank) for k in range(level - 1)
        ]

    def prepare(lev):
        for copy in cap_loads[lev]:
            copy.wait()
        high, low = split(r.cap[lev])
        r.caps[0, lev] = high
        r.caps[1, lev] = low
        order = lax.broadcasted_iota(jnp.int32, (2 * rank, 2 * rank), 0)
        pivots = r.piv[pl.ds(heaps[lev], 1), :]
        at = pivots + rank * (1 - odds[lev])
        at = jnp.where(at >= 2 * rank, at - 2 * rank, at)
        r.chosen[lev] = (order == at).astype(f32).astype(bf16)

    def widened(value, own_squares_at, ones_at):
        value_f = value.astype(f32)
        high, low = split(value_f * value_f)
        squares = dot(
            jnp.concatenate([high, low], axis=1), jnp.ones((2 * feat, feat), bf16)
        )
        one = squares.astype(bf16).astype(f32)
        two = (squares - one).astype(bf16).astype(f32)
        three = squares - one - two
        lane = lax.broadcasted_iota(jnp.int32, squares.shape, 1)
        extra = jnp.where((lane >= ones_at) & (lane < ones_at + 3), 1.0, 0.0)
        for i, piece in enumerate((one, two, three)):
            extra = jnp.where(lane == own_squares_at + i, -piece, extra)
        return extra.astype(bf16)

    def widen_train(which):
        value = r.train[which]
        r.train_w[which, :, pl.ds(0, feat)] = value + value
        r.train_w[which, :, pl.ds(feat, feat)] = widened(value, 3, 0)

    def widen_tests():
        def step(i, carry):
            part = pl.ds(pl.multiple_of(i * wide_rows, wide_rows), wide_rows)
            for h in range(2):
                value = r.gath[h, part]
                r.test_w[h, part, pl.ds(0, feat)] = value
                r.test_w[h, part, pl.ds(feat, feat)] = widened(value, 0, 3)
            return carry

        wide_rows = min(256, pairs * half)
        lax.fori_loop(0, pairs * half // wide_rows, step, 0)

    rate = spread_coef / feat * math.log2(math.e)
    chunk = min(128, pairs * half)

    def fill(which, h):
        def step(i, carry):
            part = pl.ds(pl.multiple_of(i * chunk, chunk), chunk)
            negative = dot_nt(r.test_w[h, part], r.train_w[which])
            r.kmat[h, part, pl.ds(which * points, points)] = jnp.exp2(rate * negative).astype(bf16)
            return carry

        lax.fori_loop(0, pairs * half // chunk, step, 0)

    tgt_load.wait()
    high, low = split(r.tgt[...])
    r.stack[pl.ds(0, width)] = high
    r.stack[pl.ds(width, width)] = low
    gram(1)
    turn(0)
    gram(2)
    for copy in test_loads:
        copy.wait()
    train_load.wait()
    pl.semaphore_wait(barrier, octets - 1 + OCTET - 1)
    first_send(1)
    own_test = r.gath.at[:, own_rows]

    def spread(k, carry):
        remote(own_test, own_test, r.ag_send, r.ag_recv, coords((pos + OCTET * k) % n_dev))
        return carry

    lax.fori_loop(1, octets, spread, 0)
    first_send(2)
    remote(r.train.at[0], r.train.at[1], r.tr_send, r.tr_recv, flip(1))
    turn(1)
    gram(3)
    first_send(3)
    turn(2)
    gram(4)
    first_send(4)
    widen_train(0)
    piv_load.wait()
    for lev in range(LEVELS):
        prepare(lev)
    first_take(1)
    first_take(2)
    drain(r.gath.at[:, pl.ds(0, (octets - 1) * half)], r.ag_recv)
    seat_test = r.gath.at[:, seat_rows]
    for k in range(2, OCTET, 2):
        remote(seat_test, seat_test, r.fw_send, r.fw_recv, flip(k))
    first_take(3)
    if group_of(n_dev, 3)[1] == 1:
        solve(3)
    first_take(4)
    if group_of(n_dev, 4)[1] == 1:
        solve(4)
    drain(r.train.at[0], r.tr_recv)
    widen_train(1)
    turn(LEVELS - 1)
    zero = jnp.zeros((width, points), bf16)
    for which in range(2):
        r.wts[which, 0, pl.ds(width, width)] = zero
        r.wts[which, 1, pl.ds(0, width)] = zero
    for level in (4, 3, 2, 1):
        if group_of(n_dev, level)[1] > 1:
            second_take(level)
            solve(level)
    drain(r.gath.at[:, pl.ds(0, (OCTET // 2 - 1) * octets * half)], r.fw_recv)
    widen_tests()
    fill(0, 0)
    fill(0, 1)
    fill(1, 0)
    fill(1, 1)

    pairs_ab = {}
    for level in range(2, LEVELS + 1):
        blocks = gathered(level)
        value = jnp.concatenate([blocks[0], blocks[1].astype(f32)], axis=0)
        for k in range(2, level):
            ab_high, ab_low = pairs_ab[k]
            value = value - dot(ab_high, blocks[k]) - dot(ab_low, blocks[k])
        pairs_ab[level] = split(value)
        r.ab[:, pl.ds((level - 2) * rank, rank)] = value
    b_high, b_low = split(r.ab[pl.ds(width, rank)])
    first = gathered(1)[0]
    s_high, s_low = split(first)
    later = r.ab[pl.ds(0, width)] - (dot(s_high, b_high) + dot(s_low, b_high) + dot(s_high, b_low))
    shares = jnp.concatenate([first, later], axis=1)
    share_high, share_low = split(shares)
    left_high = r.stack[pl.ds(2 * width, LEVELS * rank)]
    current = r.tgt[...] - (
        dot(share_high, left_high) + dot(share_low, left_high) + dot(share_high, r.ltl[...])
    )
    r.cur[...] = current
    weights = current.astype(bf16)
    r.wts[0, 0, pl.ds(0, width)] = weights
    r.wts[0, 1, pl.ds(width, width)] = weights
    r.wt[0] = weights
    remote(r.wt.at[0], r.wt.at[1], r.wt_send, r.wt_recv, flip(1))
    cur_copy = pltpu.make_async_copy(r.cur, r.cur_out, r.out_sem)
    cur_copy.start()

    big = min(256, pairs * half)

    def weigh(which):
        def step(i, carry):
            part = pl.ds(pl.multiple_of(i * big, big), big)
            there = pl.ds(which * points, points)
            value = dot_nt(r.kmat[0, part, there], r.wts[which, 0]) + dot_nt(
                r.kmat[1, part, there], r.wts[which, 1]
            )
            if which == 0:
                r.terms[part] = value
            else:
                r.term_b[part] = (r.terms[part] + value).astype(bf16)
            return carry

        lax.fori_loop(0, pairs * half // big, step, 0)

    weigh(0)
    drain(r.wt.at[1], r.wt_recv)
    weights = r.wt[1]
    r.wts[1, 0, pl.ds(0, width)] = weights
    r.wts[1, 1, pl.ds(width, width)] = weights
    weigh(1)

    def scatter(k, carry):
        block = (own_block + k) % pairs
        to = (block % octets) * (OCTET // 2) + block // octets
        remote(
            r.term_b.at[pl.ds(pl.multiple_of(block * half, half), half)],
            r.term_in.at[pl.ds(pl.multiple_of((k - 1) * half, half), half)],
            r.rs_send, r.rs_recv, coords(2 * to + parity),
        )
        return carry

    lax.fori_loop(1, pairs, scatter, 0)
    drain(r.gath.at[:, pl.ds(0, (octets - 1) * half)], r.ag_send)
    drain(r.gath.at[:, pl.ds(0, (OCTET // 2 - 1) * octets * half)], r.fw_send)
    drain(r.train.at[0], r.tr_send)
    drain(r.wt.at[0], r.wt_send)
    for level in range(1, LEVELS + 1):
        size, count = group_of(n_dev, level)
        lev = level - 1
        drain(getattr(r, f"recv{level}").at[pl.ds(1, size - 1)], r.p1_send.at[lev])
        if count > 1:
            drain(getattr(r, f"hop{level}").at[pl.ds(1, count - 1)], r.p2_send.at[lev])
        drain(getattr(r, f"share{level}").at[pl.ds(0, size - 1)], r.p3_send.at[lev])
    cur_copy.wait()
    total = r.term_b[own_rows].astype(f32)
    drain(r.term_in, r.rs_recv)
    total = total + jnp.sum(r.term_in[...].astype(f32).reshape(pairs - 1, half, 2 * width), axis=0)
    r.pred_out[pl.ds(0, half)] = total[:, :width]
    r.pred_out[pl.ds(half, half)] = total[:, width:]
    drain(r.term_in, r.rs_send)


def body(n_dev, narrow, targets, train, test, left, right, cap, pivots):
    points, width = targets.shape
    rank = left.shape[2]
    feat = train.shape[1]
    rows = test.shape[0]
    half = rows // 2
    pairs = n_dev // 2
    vmem = pltpu.VMEM
    dma = pltpu.SemaphoreType.DMA
    hbm_spec = pl.BlockSpec(memory_space=pl.ANY)
    vmem_spec = pl.BlockSpec(memory_space=pltpu.VMEM)
    scratch = {
        "tgt": vmem((width, points), f32),
        "piv": vmem(pivots.shape, jnp.int32),
        "train": vmem((2, points, feat), bf16),
        "gath": vmem((2, pairs * half, feat), bf16),
        "left": vmem((LEVELS, points, rank), f32),
        "right": vmem((LEVELS, points, rank), f32),
        "cap": vmem((LEVELS, 2 * rank, 2 * rank), f32),
        "caps": vmem((2, LEVELS, 2 * rank, 2 * rank), bf16),
        "chosen": vmem((LEVELS, 2 * rank, 2 * rank), bf16),
        "stack": vmem((2 * width + LEVELS * rank, points), bf16),
        "ltl": vmem((LEVELS * rank, points), bf16),
        "train_w": vmem((2, points, 2 * feat), bf16),
        "test_w": vmem((2, pairs * half, 2 * feat), bf16),
        "kmat": vmem((2, pairs * half, 2 * points), bf16),
        "ab": vmem((width + rank, (LEVELS - 1) * rank), f32),
        "cur": vmem((width, points), f32),
        "wt": vmem((2, width, points), bf16),
        "wts": vmem((2, 2, 2 * width, points), bf16),
        "terms": vmem((pairs * half, 2 * width), f32),
        "term_b": vmem((pairs * half, 2 * width), bf16),
        "term_in": vmem(((pairs - 1) * half, 2 * width), bf16),
    }
    for level in range(1, LEVELS + 1):
        size, count = group_of(n_dev, level)
        tall = (2 * width + (level - 1) * rank) // size
        for name in ("send", "recv", "share"):
            scratch[f"{name}{level}"] = vmem((size, tall, rank), bf16)
        scratch[f"out{level}"] = vmem((2, tall, rank), bf16)
        if count > 1:
            scratch[f"hop{level}"] = vmem((count, tall, rank), bf16)
    scratch["load_sem"] = dma((4 + 2 * LEVELS,))
    scratch["cap_sem"] = dma((LEVELS, 2))
    for name in ("p1_send", "p1_recv", "p2_send", "p2_recv", "p3_send", "p3_recv"):
        scratch[name] = dma((LEVELS,))
    for name in (
        "ag_send", "ag_recv", "tr_send", "tr_recv", "wt_send", "wt_recv", "rs_send", "rs_recv",
        "out_sem", "piv_sem", "fw_send", "fw_recv",
    ):
        scratch[name] = dma
    names = ["tgt_h", "train_h", "test_h", "left_h", "right_h", "cap_h", "piv_h"]
    names += ["cur_out", "pred_out"] + list(scratch)
    current, predictions = pl.pallas_call(
        functools.partial(kernel, n_dev, narrow, names),
        out_shape=(
            jax.ShapeDtypeStruct((width, points), f32),
            jax.ShapeDtypeStruct((rows, width), f32),
        ),
        in_specs=[hbm_spec] * 7,
        out_specs=(hbm_spec, vmem_spec),
        scratch_shapes=list(scratch.values()),
        compiler_params=pltpu.CompilerParams(
            collective_id=0, has_side_effects=True, vmem_limit_bytes=48 * 1024 * 1024
        ),
    )(targets.T, train, test, left, right, cap, pivots)
    return current.T, predictions


def solution(mesh):
    both = ("wide", "narrow")
    placed = (
        P(both, None), P(both, None), P(both, None),
        P(both, None, None), P(both, None, None), P(), P(),
    )
    sizes = dict(mesh.shape)
    return jax.shard_map(
        functools.partial(body, sizes["wide"] * sizes["narrow"], sizes["narrow"]),
        mesh=mesh,
        in_specs=placed,
        out_specs=(P(both, None), P(both, None)),
        check_vma=False,
    )
```

```python
import functools
import math
import types

import jax
import jax.numpy as jnp
from jax import lax
from jax.experimental import pallas as pl
from jax.experimental.pallas import tpu as pltpu
from jax.sharding import PartitionSpec as P

LEVELS = 4
OCTET = 8
spread_coef = 3.0
MESH = pl.DeviceIdType.MESH
f32, bf16 = jnp.float32, jnp.bfloat16


def dot(a, b):
    return jnp.dot(a, b, preferred_element_type=f32)


def dot_nt(a, b):
    return lax.dot_general(a, b, (((1,), (1,)), ((), ())), preferred_element_type=f32)


def split(value):
    high = value.astype(bf16)
    return high, (value - high.astype(f32)).astype(bf16)


def halves_of(value):
    high = value.astype(bf16).astype(f32)
    return high, value - high


def group_of(n_dev, level):
    node = n_dev >> (level - 1)
    size = min(OCTET, node)
    return size, node // size


def kernel(n_dev, narrow, names, *refs):
    r = types.SimpleNamespace(**dict(zip(names, refs)))
    pos = lax.axis_index("wide") * narrow + lax.axis_index("narrow")
    width, points = r.tgt.shape
    rank = r.right.shape[2]
    feat = r.train.shape[2]
    rows = r.test_h.shape[0]
    half = rows // 2
    pairs = n_dev // 2
    parity = pos % 2
    slot = pos // 2
    octets = n_dev // OCTET
    seat = slot % (OCTET // 2)
    own_block = seat * octets + slot // (OCTET // 2)
    own_rows = pl.ds(pl.multiple_of(own_block * half, half), half)
    seat_rows = pl.ds(pl.multiple_of(seat * octets * half, octets * half), octets * half)

    def coords(dev):
        return (dev // narrow, dev % narrow)

    def flip(mask):
        dev = pos
        for bit in range(mask.bit_length()):
            if mask >> bit & 1:
                dev = dev + (1 << bit) * (1 - 2 * ((pos // (1 << bit)) % 2))
        return coords(dev)

    def remote(src, dst, send_sem, recv_sem, where):
        pltpu.make_async_remote_copy(
            src_ref=src, dst_ref=dst, send_sem=send_sem, recv_sem=recv_sem,
            device_id=where, device_id_type=MESH,
        ).start()

    def drain(part, sem):
        pltpu.make_async_copy(part, part, sem).wait()

    def load(src, dst, sem):
        copy = pltpu.make_async_copy(src, dst, sem)
        copy.start()
        return copy

    test_loads = [
        load(r.test_h.at[pl.ds(h * half, half)], r.gath.at[h, own_rows], r.load_sem.at[0 + h])
        for h in range(2)
    ]
    tgt_load = load(r.tgt_h, r.tgt, r.load_sem.at[2])
    piv_load = load(r.piv_h, r.piv, r.piv_sem)
    right_loads, left_loads = [], []
    train_load = None
    for lev in range(LEVELS):
        right_loads.append(load(r.right_h.at[:, lev, :], r.right.at[lev], r.load_sem.at[4 + lev]))
        if lev == 0:
            train_load = load(r.train_h, r.train.at[0], r.load_sem.at[3])
        left_loads.append(
            load(r.left_h.at[:, lev, :], r.left.at[lev], r.load_sem.at[4 + LEVELS + lev])
        )
    cap_loads, odds, heaps = [], [], []
    for level in range(1, LEVELS + 1):
        child = pos // (n_dev >> level)
        odd = child % 2
        odds.append(odd)
        heaps.append((1 << level - 1) - 1 + child // 2)
        cap_loads.append([
            load(
                r.cap_h.at[heaps[-1], pl.ds(pl.multiple_of(which * rank, rank), rank)],
                r.cap.at[level - 1, pl.ds(at * rank, rank)],
                r.cap_sem.at[level - 1, at],
            )
            for at, which in enumerate((odd, 1 - odd))
        ])

    barrier = pltpu.get_barrier_semaphore()

    def greet(k, carry):
        pl.semaphore_signal(
            barrier, inc=1, device_id=coords((pos + OCTET * k) % n_dev), device_id_type=MESH
        )
        return carry

    lax.fori_loop(1, octets, greet, 0)
    for k in range(1, OCTET):
        pl.semaphore_signal(barrier, inc=1, device_id=flip(k), device_id_type=MESH)

    def first_send(level):
        size, _ = group_of(n_dev, level)
        mine = pos % size
        lev = level - 1
        for k in range(1, size):
            to = mine
            for bit in range(k.bit_length()):
                if k >> bit & 1:
                    to = to + (1 << bit) * (1 - 2 * ((mine // (1 << bit)) % 2))
            remote(
                getattr(r, f"send{level}").at[to], getattr(r, f"recv{level}").at[k],
                r.p1_send.at[lev], r.p1_recv.at[lev], flip(k),
            )

    def gram(level):
        lev = level - 1
        size, _ = group_of(n_dev, level)
        right_loads[lev].wait()
        high, low = split(r.right[lev])
        product = dot(r.stack[pl.ds(0, 2 * width + lev * rank)], high)
        t = product[:width] + product[width : 2 * width] + dot(r.stack[pl.ds(0, width)], low)
        t_high, t_low = halves_of(t)
        part = width // size
        both = jnp.concatenate(
            [t_high.reshape(size, part, rank), t_low.reshape(size, part, rank)], axis=1
        )
        send = getattr(r, f"send{level}")
        send[:, pl.ds(0, 2 * part)] = both.astype(bf16)
        cut = rank // size
        for k in range(lev):
            piece = product[2 * width + k * rank : 2 * width + (k + 1) * rank]
            send[:, pl.ds(2 * part + k * cut, cut)] = piece.astype(bf16).reshape(size, cut, rank)

    def turn(lev):
        left_loads[lev].wait()
        high, low = split(r.left[lev].T)
        r.stack[pl.ds(2 * width + lev * rank, rank)] = high
        r.ltl[pl.ds(lev * rank, rank)] = low

    sums = {}

    def joined(value, level):
        part = width // group_of(n_dev, level)[0]
        top = value[:part] + value[part : 2 * part]
        return top if level == 1 else jnp.concatenate([top, value[2 * part :]], axis=0)

    def packed(value, level):
        part = width // group_of(n_dev, level)[0]
        high, low = halves_of(value[:part])
        pieces = [high, low] if level == 1 else [high, low, value[part:]]
        return jnp.concatenate(pieces, axis=0).astype(bf16)

    def first_take(level):
        size, count = group_of(n_dev, level)
        lev = level - 1
        recv, send = getattr(r, f"recv{level}"), getattr(r, f"send{level}")
        drain(recv.at[pl.ds(1, size - 1)], r.p1_recv.at[lev])
        near = send[pos % size].astype(f32)
        far = None
        for k in range(1, size):
            value = recv[k].astype(f32)
            if count > 1 or k < size // 2:
                near = near + value
            else:
                far = value if far is None else far + value
        near = joined(near, level)
        if count == 1:
            sums[level] = (near, joined(far, level))
            return
        sums[level] = (near, None)
        hop = getattr(r, f"hop{level}")
        hop[0] = packed(near, level)
        for j in range(1, count):
            remote(hop.at[0], hop.at[j], r.p2_send.at[lev], r.p2_recv.at[lev], flip(j * OCTET))

    def second_take(level):
        size, count = group_of(n_dev, level)
        if count == 1:
            return
        hop = getattr(r, f"hop{level}")
        drain(hop.at[pl.ds(1, count - 1)], r.p2_recv.at[level - 1])
        near, far = sums[level][0], None
        for j in range(1, count):
            value = joined(hop[j].astype(f32), level)
            if j < count // 2:
                near = near + value
            else:
                far = value if far is None else far + value
        sums[level] = (near, far)

    def solve(level):
        size, count = group_of(n_dev, level)
        lev = level - 1
        near, far = sums[level]
        cols = near.shape[0]
        both = jnp.concatenate([near, far], axis=1)
        high, low = halves_of(both)
        moved = dot(jnp.concatenate([high, low], axis=0).astype(bf16), r.chosen[lev])
        kids = 1 if count > 1 else 2
        cap_high = r.caps[0, lev, pl.ds(0, kids * rank)]
        cap_low = r.caps[1, lev, pl.ds(0, kids * rank)]
        result = dot_nt(moved.astype(bf16), cap_high)
        result = result[:cols] + result[cols:] + dot_nt(moved[:cols].astype(bf16), cap_low)
        share, out = getattr(r, f"share{level}"), getattr(r, f"out{level}")
        for kid in range(kids):
            out[kid] = packed(result[:, kid * rank : (kid + 1) * rank], level)
        mine = pos % size
        for k in range(1, size):
            kid = 1 if count == 1 and k >= size // 2 else 0
            remote(
                out.at[kid], share.at[mine], r.p3_send.at[lev], r.p3_recv.at[lev], flip(k)
            )
        share[mine] = out[0]

    def gathered(level):
        size, _ = group_of(n_dev, level)
        share = getattr(r, f"share{level}")
        drain(share.at[pl.ds(0, size - 1)], r.p3_recv.at[level - 1])
        part, cut = width // size, rank // size
        top = share[:, pl.ds(0, 2 * part)].astype(f32)
        top = (top[:, :part] + top[:, part:]).reshape(width, rank)
        return [top] + [
            share[:, pl.ds(2 * part + k * cut, cut)].reshape(rank, rank) for k in range(level - 1)
        ]

    def prepare(lev):
        for copy in cap_loads[lev]:
            copy.wait()
        high, low = split(r.cap[lev])
        r.caps[0, lev] = high
        r.caps[1, lev] = low
        order = lax.broadcasted_iota(jnp.int32, (2 * rank, 2 * rank), 0)
        pivots = r.piv[pl.ds(heaps[lev], 1), :]
        at = pivots + rank * (1 - odds[lev])
        at = jnp.where(at >= 2 * rank, at - 2 * rank, at)
        r.chosen[lev] = (order == at).astype(f32).astype(bf16)

    def widened(value, own_squares_at, ones_at):
        value_f = value.astype(f32)
        high, low = split(value_f * value_f)
        squares = dot(
            jnp.concatenate([high, low], axis=1), jnp.ones((2 * feat, feat), bf16)
        )
        one = squares.astype(bf16).astype(f32)
        two = (squares - one).astype(bf16).astype(f32)
        three = squares - one - two
        lane = lax.broadcasted_iota(jnp.int32, squares.shape, 1)
        extra = jnp.where((lane >= ones_at) & (lane < ones_at + 3), 1.0, 0.0)
        for i, piece in enumerate((one, two, three)):
            extra = jnp.where(lane == own_squares_at + i, -piece, extra)
        return extra.astype(bf16)

    def widen_train(which):
        value = r.train[which]
        r.train_w[which, :, pl.ds(0, feat)] = value + value
        r.train_w[which, :, pl.ds(feat, feat)] = widened(value, 3, 0)

    def widen_tests():
        def step(i, carry):
            part = pl.ds(pl.multiple_of(i * wide_rows, wide_rows), wide_rows)
            for h in range(2):
                value = r.gath[h, part]
                r.test_w[h, part, pl.ds(0, feat)] = value
                r.test_w[h, part, pl.ds(feat, feat)] = widened(value, 0, 3)
            return carry

        wide_rows = min(256, pairs * half)
        lax.fori_loop(0, pairs * half // wide_rows, step, 0)

    rate = spread_coef / feat * math.log2(math.e)
    chunk = min(128, pairs * half)

    def fill(which, h):
        def step(i, carry):
            part = pl.ds(pl.multiple_of(i * chunk, chunk), chunk)
            negative = dot_nt(r.test_w[h, part], r.train_w[which])
            r.kmat[h, part, pl.ds(which * points, points)] = jnp.exp2(rate * negative).astype(bf16)
            return carry

        lax.fori_loop(0, pairs * half // chunk, step, 0)

    tgt_load.wait()
    high, low = split(r.tgt[...])
    r.stack[pl.ds(0, width)] = high
    r.stack[pl.ds(width, width)] = low
    gram(1)
    turn(0)
    gram(2)
    for copy in test_loads:
        copy.wait()
    train_load.wait()
    pl.semaphore_wait(barrier, octets - 1 + OCTET - 1)
    first_send(1)
    own_test = r.gath.at[:, own_rows]

    def spread(k, carry):
        remote(own_test, own_test, r.ag_send, r.ag_recv, coords((pos + OCTET * k) % n_dev))
        return carry

    lax.fori_loop(1, octets, spread, 0)
    first_send(2)
    remote(r.train.at[0], r.train.at[1], r.tr_send, r.tr_recv, flip(1))
    turn(1)
    gram(3)
    first_send(3)
    turn(2)
    gram(4)
    first_send(4)
    widen_train(0)
    piv_load.wait()
    for lev in range(LEVELS):
        prepare(lev)
    first_take(1)
    first_take(2)
    drain(r.gath.at[:, pl.ds(0, (octets - 1) * half)], r.ag_recv)
    seat_test = r.gath.at[:, seat_rows]
    for k in range(2, OCTET, 2):
        remote(seat_test, seat_test, r.fw_send, r.fw_recv, flip(k))
    first_take(3)
    if group_of(n_dev, 3)[1] == 1:
        solve(3)
    first_take(4)
    if group_of(n_dev, 4)[1] == 1:
        solve(4)
    drain(r.train.at[0], r.tr_recv)
    widen_train(1)
    turn(LEVELS - 1)
    zero = jnp.zeros((width, points), bf16)
    for which in range(2):
        r.wts[which, 0, pl.ds(width, width)] = zero
        r.wts[which, 1, pl.ds(0, width)] = zero
    for level in (4, 3, 2, 1):
        if group_of(n_dev, level)[1] > 1:
            second_take(level)
            solve(level)
    drain(r.gath.at[:, pl.ds(0, (OCTET // 2 - 1) * octets * half)], r.fw_recv)
    widen_tests()
    fill(0, 0)
    fill(0, 1)
    fill(1, 0)
    fill(1, 1)

    pairs_ab = {}
    for level in range(2, LEVELS + 1):
        blocks = gathered(level)
        value = jnp.concatenate([blocks[0], blocks[1].astype(f32)], axis=0)
        for k in range(2, level):
            ab_high, ab_low = pairs_ab[k]
            value = value - dot(ab_high, blocks[k]) - dot(ab_low, blocks[k])
        pairs_ab[level] = split(value)
        r.ab[:, pl.ds((level - 2) * rank, rank)] = value
    b_high, b_low = split(r.ab[pl.ds(width, rank)])
    first = gathered(1)[0]
    s_high, s_low = split(first)
    later = r.ab[pl.ds(0, width)] - (dot(s_high, b_high) + dot(s_low, b_high) + dot(s_high, b_low))
    shares = jnp.concatenate([first, later], axis=1)
    share_high, share_low = split(shares)
    left_high = r.stack[pl.ds(2 * width, LEVELS * rank)]
    current = r.tgt[...] - (
        dot(share_high, left_high) + dot(share_low, left_high) + dot(share_high, r.ltl[...])
    )
    r.cur[...] = current
    weights = current.astype(bf16)
    r.wts[0, 0, pl.ds(0, width)] = weights
    r.wts[0, 1, pl.ds(width, width)] = weights
    r.wt[0] = weights
    remote(r.wt.at[0], r.wt.at[1], r.wt_send, r.wt_recv, flip(1))
    cur_copy = pltpu.make_async_copy(r.cur, r.cur_out, r.out_sem)
    cur_copy.start()

    big = min(256, pairs * half)

    def weigh(which):
        def step(i, carry):
            part = pl.ds(pl.multiple_of(i * big, big), big)
            there = pl.ds(which * points, points)
            value = dot_nt(r.kmat[0, part, there], r.wts[which, 0]) + dot_nt(
                r.kmat[1, part, there], r.wts[which, 1]
            )
            if which == 0:
                r.terms[part] = value
            else:
                r.term_b[part] = (r.terms[part] + value).astype(bf16)
            return carry

        lax.fori_loop(0, pairs * half // big, step, 0)

    weigh(0)
    drain(r.wt.at[1], r.wt_recv)
    weights = r.wt[1]
    r.wts[1, 0, pl.ds(0, width)] = weights
    r.wts[1, 1, pl.ds(width, width)] = weights
    weigh(1)

    def scatter(k, carry):
        block = (own_block + k) % pairs
        to = (block % octets) * (OCTET // 2) + block // octets
        remote(
            r.term_b.at[pl.ds(pl.multiple_of(block * half, half), half)],
            r.term_in.at[pl.ds(pl.multiple_of((k - 1) * half, half), half)],
            r.rs_send, r.rs_recv, coords(2 * to + parity),
        )
        return carry

    lax.fori_loop(1, pairs, scatter, 0)
    drain(r.gath.at[:, pl.ds(0, (octets - 1) * half)], r.ag_send)
    drain(r.gath.at[:, pl.ds(0, (OCTET // 2 - 1) * octets * half)], r.fw_send)
    drain(r.train.at[0], r.tr_send)
    drain(r.wt.at[0], r.wt_send)
    for level in range(1, LEVELS + 1):
        size, count = group_of(n_dev, level)
        lev = level - 1
        drain(getattr(r, f"recv{level}").at[pl.ds(1, size - 1)], r.p1_send.at[lev])
        if count > 1:
            drain(getattr(r, f"hop{level}").at[pl.ds(1, count - 1)], r.p2_send.at[lev])
        drain(getattr(r, f"share{level}").at[pl.ds(0, size - 1)], r.p3_send.at[lev])
    cur_copy.wait()
    total = r.term_b[own_rows].astype(f32)
    drain(r.term_in, r.rs_recv)
    total = total + jnp.sum(r.term_in[...].astype(f32).reshape(pairs - 1, half, 2 * width), axis=0)
    r.pred_out[pl.ds(0, half)] = total[:, :width]
    r.pred_out[pl.ds(half, half)] = total[:, width:]
    drain(r.term_in, r.rs_send)


def body(n_dev, narrow, targets, train, test, left, right, cap, pivots):
    points, width = targets.shape
    rank = left.shape[2]
    feat = train.shape[1]
    rows = test.shape[0]
    half = rows // 2
    pairs = n_dev // 2
    vmem = pltpu.VMEM
    dma = pltpu.SemaphoreType.DMA
    hbm_spec = pl.BlockSpec(memory_space=pl.ANY)
    vmem_spec = pl.BlockSpec(memory_space=pltpu.VMEM)
    scratch = {
        "tgt": vmem((width, points), f32),
        "piv": vmem(pivots.shape, jnp.int32),
        "train": vmem((2, points, feat), bf16),
        "gath": vmem((2, pairs * half, feat), bf16),
        "left": vmem((LEVELS, points, rank), f32),
        "right": vmem((LEVELS, points, rank), f32),
        "cap": vmem((LEVELS, 2 * rank, 2 * rank), f32),
        "caps": vmem((2, LEVELS, 2 * rank, 2 * rank), bf16),
        "chosen": vmem((LEVELS, 2 * rank, 2 * rank), bf16),
        "stack": vmem((2 * width + LEVELS * rank, points), bf16),
        "ltl": vmem((LEVELS * rank, points), bf16),
        "train_w": vmem((2, points, 2 * feat), bf16),
        "test_w": vmem((2, pairs * half, 2 * feat), bf16),
        "kmat": vmem((2, pairs * half, 2 * points), bf16),
        "ab": vmem((width + rank, (LEVELS - 1) * rank), f32),
        "cur": vmem((width, points), f32),
        "wt": vmem((2, width, points), bf16),
        "wts": vmem((2, 2, 2 * width, points), bf16),
        "terms": vmem((pairs * half, 2 * width), f32),
        "term_b": vmem((pairs * half, 2 * width), bf16),
        "term_in": vmem(((pairs - 1) * half, 2 * width), bf16),
    }
    for level in range(1, LEVELS + 1):
        size, count = group_of(n_dev, level)
        tall = (2 * width + (level - 1) * rank) // size
        for name in ("send", "recv", "share"):
            scratch[f"{name}{level}"] = vmem((size, tall, rank), bf16)
        scratch[f"out{level}"] = vmem((2, tall, rank), bf16)
        if count > 1:
            scratch[f"hop{level}"] = vmem((count, tall, rank), bf16)
    scratch["load_sem"] = dma((4 + 2 * LEVELS,))
    scratch["cap_sem"] = dma((LEVELS, 2))
    for name in ("p1_send", "p1_recv", "p2_send", "p2_recv", "p3_send", "p3_recv"):
        scratch[name] = dma((LEVELS,))
    for name in (
        "ag_send", "ag_recv", "tr_send", "tr_recv", "wt_send", "wt_recv", "rs_send", "rs_recv",
        "out_sem", "piv_sem", "fw_send", "fw_recv",
    ):
        scratch[name] = dma
    names = ["tgt_h", "train_h", "test_h", "left_h", "right_h", "cap_h", "piv_h"]
    names += ["cur_out", "pred_out"] + list(scratch)
    current, predictions = pl.pallas_call(
        functools.partial(kernel, n_dev, narrow, names),
        out_shape=(
            jax.ShapeDtypeStruct((width, points), f32),
            jax.ShapeDtypeStruct((rows, width), f32),
        ),
        in_specs=[pl.BlockSpec(memory_space=pltpu.HBM)] * 7,
        out_specs=(hbm_spec, vmem_spec),
        scratch_shapes=list(scratch.values()),
        compiler_params=pltpu.CompilerParams(
            collective_id=0, has_side_effects=True, vmem_limit_bytes=48 * 1024 * 1024
        ),
    )(*(
        pltpu.with_memory_space_constraint(value, pltpu.HBM)
        for value in (targets.T, train, test, left, right, cap, pivots)
    ))
    return current.T, predictions


def solution(mesh):
    both = ("wide", "narrow")
    placed = (
        P(both, None), P(both, None), P(both, None),
        P(both, None, None), P(both, None, None), P(), P(),
    )
    sizes = dict(mesh.shape)
    return jax.shard_map(
        functools.partial(body, sizes["wide"] * sizes["narrow"], sizes["narrow"]),
        mesh=mesh,
        in_specs=placed,
        out_specs=(P(both, None), P(both, None)),
        check_vma=False,
    )
```

```python
import functools
import math
import types

import jax
import jax.numpy as jnp
from jax import lax
from jax.experimental import pallas as pl
from jax.experimental.pallas import tpu as pltpu
from jax.sharding import PartitionSpec as P

LEVELS = 4
OCTET = 8
spread_coef = 3.0
MESH = pl.DeviceIdType.MESH
f32, bf16 = jnp.float32, jnp.bfloat16


def dot(a, b):
    return jnp.dot(a, b, preferred_element_type=f32)


def dot_nt(a, b):
    return lax.dot_general(a, b, (((1,), (1,)), ((), ())), preferred_element_type=f32)


def split(value):
    high = value.astype(bf16)
    return high, (value - high.astype(f32)).astype(bf16)


def halves_of(value):
    high = value.astype(bf16).astype(f32)
    return high, value - high


def group_of(n_dev, level):
    node = n_dev >> (level - 1)
    size = min(OCTET, node)
    return size, node // size


def kernel(n_dev, narrow, names, *refs):
    r = types.SimpleNamespace(**dict(zip(names, refs)))
    pos = lax.axis_index("wide") * narrow + lax.axis_index("narrow")
    width, points = r.tgt.shape
    rank = r.right.shape[2]
    feat = r.train.shape[2]
    rows = r.test_h.shape[0]
    half = rows // 2
    pairs = n_dev // 2
    parity = pos % 2
    slot = pos // 2
    octets = n_dev // OCTET
    seat = slot % (OCTET // 2)
    own_block = seat * octets + slot // (OCTET // 2)
    own_rows = pl.ds(pl.multiple_of(own_block * half, half), half)
    seat_rows = pl.ds(pl.multiple_of(seat * octets * half, octets * half), octets * half)

    def coords(dev):
        return (dev // narrow, dev % narrow)

    def flip(mask):
        dev = pos
        for bit in range(mask.bit_length()):
            if mask >> bit & 1:
                dev = dev + (1 << bit) * (1 - 2 * ((pos // (1 << bit)) % 2))
        return coords(dev)

    def remote(src, dst, send_sem, recv_sem, where):
        pltpu.make_async_remote_copy(
            src_ref=src, dst_ref=dst, send_sem=send_sem, recv_sem=recv_sem,
            device_id=where, device_id_type=MESH,
        ).start()

    def drain(part, sem):
        pltpu.make_async_copy(part, part, sem).wait()

    def load(src, dst, sem):
        copy = pltpu.make_async_copy(src, dst, sem)
        copy.start()
        return copy

    test_loads = [
        load(r.test_h.at[pl.ds(h * half, half)], r.gath.at[h, own_rows], r.load_sem.at[0 + h])
        for h in range(2)
    ]
    tgt_load = load(r.tgt_h, r.tgt, r.load_sem.at[2])
    piv_load = load(r.piv_h, r.piv, r.piv_sem)
    right_loads, left_loads = [], []
    train_load = None
    for lev in range(LEVELS):
        right_loads.append(load(r.right_h.at[:, lev, :], r.right.at[lev], r.load_sem.at[4 + lev]))
        if lev == 0:
            train_load = load(r.train_h, r.train.at[0], r.load_sem.at[3])
        left_loads.append(
            load(r.left_h.at[:, lev, :], r.left.at[lev], r.load_sem.at[4 + LEVELS + lev])
        )
    cap_loads, odds, heaps = [], [], []
    for level in range(1, LEVELS + 1):
        child = pos // (n_dev >> level)
        odd = child % 2
        odds.append(odd)
        heaps.append((1 << level - 1) - 1 + child // 2)
        cap_loads.append([
            load(
                r.cap_h.at[heaps[-1], pl.ds(pl.multiple_of(which * rank, rank), rank)],
                r.cap.at[level - 1, pl.ds(at * rank, rank)],
                r.cap_sem.at[level - 1, at],
            )
            for at, which in enumerate((odd, 1 - odd))
        ])

    barrier = pltpu.get_barrier_semaphore()

    def greet(k, carry):
        pl.semaphore_signal(
            barrier, inc=1, device_id=coords((pos + OCTET * k) % n_dev), device_id_type=MESH
        )
        return carry

    lax.fori_loop(1, octets, greet, 0)
    for k in range(1, OCTET):
        pl.semaphore_signal(barrier, inc=1, device_id=flip(k), device_id_type=MESH)

    def first_send(level):
        size, _ = group_of(n_dev, level)
        mine = pos % size
        lev = level - 1
        for k in range(1, size):
            to = mine
            for bit in range(k.bit_length()):
                if k >> bit & 1:
                    to = to + (1 << bit) * (1 - 2 * ((mine // (1 << bit)) % 2))
            remote(
                getattr(r, f"send{level}").at[to], getattr(r, f"recv{level}").at[k],
                r.p1_send.at[lev], r.p1_recv.at[lev], flip(k),
            )

    def gram(level):
        lev = level - 1
        size, _ = group_of(n_dev, level)
        right_loads[lev].wait()
        high, low = split(r.right[lev])
        product = dot(r.stack[pl.ds(0, 2 * width + lev * rank)], high)
        t = product[:width] + product[width : 2 * width] + dot(r.stack[pl.ds(0, width)], low)
        t_high, t_low = halves_of(t)
        part = width // size
        both = jnp.concatenate(
            [t_high.reshape(size, part, rank), t_low.reshape(size, part, rank)], axis=1
        )
        send = getattr(r, f"send{level}")
        send[:, pl.ds(0, 2 * part)] = both.astype(bf16)
        cut = rank // size
        for k in range(lev):
            piece = product[2 * width + k * rank : 2 * width + (k + 1) * rank]
            send[:, pl.ds(2 * part + k * cut, cut)] = piece.astype(bf16).reshape(size, cut, rank)

    def turn(lev):
        left_loads[lev].wait()
        high, low = split(r.left[lev].T)
        r.stack[pl.ds(2 * width + lev * rank, rank)] = high
        r.ltl[pl.ds(lev * rank, rank)] = low

    sums = {}

    def joined(value, level):
        part = width // group_of(n_dev, level)[0]
        top = value[:part] + value[part : 2 * part]
        return top if level == 1 else jnp.concatenate([top, value[2 * part :]], axis=0)

    def packed(value, level):
        part = width // group_of(n_dev, level)[0]
        high, low = halves_of(value[:part])
        pieces = [high, low] if level == 1 else [high, low, value[part:]]
        return jnp.concatenate(pieces, axis=0).astype(bf16)

    def first_take(level):
        size, count = group_of(n_dev, level)
        lev = level - 1
        recv, send = getattr(r, f"recv{level}"), getattr(r, f"send{level}")
        drain(recv.at[pl.ds(1, size - 1)], r.p1_recv.at[lev])
        near = send[pos % size].astype(f32)
        far = None
        for k in range(1, size):
            value = recv[k].astype(f32)
            if count > 1 or k < size // 2:
                near = near + value
            else:
                far = value if far is None else far + value
        near = joined(near, level)
        if count == 1:
            sums[level] = (near, joined(far, level))
            return
        sums[level] = (near, None)
        hop = getattr(r, f"hop{level}")
        hop[0] = packed(near, level)
        for j in range(1, count):
            remote(hop.at[0], hop.at[j], r.p2_send.at[lev], r.p2_recv.at[lev], flip(j * OCTET))

    def second_take(level):
        size, count = group_of(n_dev, level)
        if count == 1:
            return
        hop = getattr(r, f"hop{level}")
        drain(hop.at[pl.ds(1, count - 1)], r.p2_recv.at[level - 1])
        near, far = sums[level][0], None
        for j in range(1, count):
            value = joined(hop[j].astype(f32), level)
            if j < count // 2:
                near = near + value
            else:
                far = value if far is None else far + value
        sums[level] = (near, far)

    def solve(level):
        size, count = group_of(n_dev, level)
        lev = level - 1
        near, far = sums[level]
        cols = near.shape[0]
        both = jnp.concatenate([near, far], axis=1)
        high, low = halves_of(both)
        moved = dot(jnp.concatenate([high, low], axis=0).astype(bf16), r.chosen[lev])
        kids = 1 if count > 1 else 2
        cap_high = r.caps[0, lev, pl.ds(0, kids * rank)]
        cap_low = r.caps[1, lev, pl.ds(0, kids * rank)]
        result = dot_nt(moved.astype(bf16), cap_high)
        result = result[:cols] + result[cols:] + dot_nt(moved[:cols].astype(bf16), cap_low)
        share, out = getattr(r, f"share{level}"), getattr(r, f"out{level}")
        for kid in range(kids):
            out[kid] = packed(result[:, kid * rank : (kid + 1) * rank], level)
        mine = pos % size
        for k in range(1, size):
            kid = 1 if count == 1 and k >= size // 2 else 0
            remote(
                out.at[kid], share.at[mine], r.p3_send.at[lev], r.p3_recv.at[lev], flip(k)
            )
        share[mine] = out[0]

    def gathered(level):
        size, _ = group_of(n_dev, level)
        share = getattr(r, f"share{level}")
        drain(share.at[pl.ds(0, size - 1)], r.p3_recv.at[level - 1])
        part, cut = width // size, rank // size
        top = share[:, pl.ds(0, 2 * part)].astype(f32)
        top = (top[:, :part] + top[:, part:]).reshape(width, rank)
        return [top] + [
            share[:, pl.ds(2 * part + k * cut, cut)].reshape(rank, rank) for k in range(level - 1)
        ]

    def prepare(lev):
        for copy in cap_loads[lev]:
            copy.wait()
        high, low = split(r.cap[lev])
        r.caps[0, lev] = high
        r.caps[1, lev] = low
        order = lax.broadcasted_iota(jnp.int32, (2 * rank, 2 * rank), 0)
        pivots = r.piv[pl.ds(heaps[lev], 1), :]
        at = pivots + rank * (1 - odds[lev])
        at = jnp.where(at >= 2 * rank, at - 2 * rank, at)
        r.chosen[lev] = (order == at).astype(f32).astype(bf16)

    def widened(value, own_squares_at, ones_at):
        value_f = value.astype(f32)
        high, low = split(value_f * value_f)
        squares = dot(
            jnp.concatenate([high, low], axis=1), jnp.ones((2 * feat, feat), bf16)
        )
        one = squares.astype(bf16).astype(f32)
        two = (squares - one).astype(bf16).astype(f32)
        three = squares - one - two
        lane = lax.broadcasted_iota(jnp.int32, squares.shape, 1)
        extra = jnp.where((lane >= ones_at) & (lane < ones_at + 3), 1.0, 0.0)
        for i, piece in enumerate((one, two, three)):
            extra = jnp.where(lane == own_squares_at + i, -piece, extra)
        return extra.astype(bf16)

    def widen_train(which):
        value = r.train[which]
        r.train_w[which, :, pl.ds(0, feat)] = value + value
        r.train_w[which, :, pl.ds(feat, feat)] = widened(value, 3, 0)

    def widen_tests():
        def step(i, carry):
            part = pl.ds(pl.multiple_of(i * wide_rows, wide_rows), wide_rows)
            for h in range(2):
                value = r.gath[h, part]
                there = pl.ds(
                    pl.multiple_of(h * pairs * half + i * wide_rows, wide_rows), wide_rows
                )
                r.test_w[there, pl.ds(0, feat)] = value
                r.test_w[there, pl.ds(feat, feat)] = widened(value, 0, 3)
            return carry

        wide_rows = min(256, pairs * half)
        lax.fori_loop(0, pairs * half // wide_rows, step, 0)

    rate = spread_coef / feat * math.log2(math.e)
    chunk = min(512, pairs * rows)

    def fill(which):
        def step(i, carry):
            part = pl.ds(pl.multiple_of(i * chunk, chunk), chunk)
            negative = dot_nt(r.test_w[part], r.train_w[which])
            r.kmat[part, pl.ds(which * points, points)] = jnp.exp2(rate * negative).astype(bf16)
            return carry

        lax.fori_loop(0, pairs * rows // chunk, step, 0)

    tgt_load.wait()
    high, low = split(r.tgt[...])
    r.stack[pl.ds(0, width)] = high
    r.stack[pl.ds(width, width)] = low
    gram(1)
    turn(0)
    gram(2)
    for copy in test_loads:
        copy.wait()
    train_load.wait()
    pl.semaphore_wait(barrier, octets - 1 + OCTET - 1)
    first_send(1)
    own_test = r.gath.at[:, own_rows]

    def spread(k, carry):
        remote(own_test, own_test, r.ag_send, r.ag_recv, coords((pos + OCTET * k) % n_dev))
        return carry

    lax.fori_loop(1, octets, spread, 0)
    first_send(2)
    remote(r.train.at[0], r.train.at[1], r.tr_send, r.tr_recv, flip(1))
    turn(1)
    gram(3)
    first_send(3)
    turn(2)
    gram(4)
    first_send(4)
    widen_train(0)
    piv_load.wait()
    for lev in range(LEVELS):
        prepare(lev)
    first_take(1)
    first_take(2)
    drain(r.gath.at[:, pl.ds(0, (octets - 1) * half)], r.ag_recv)
    seat_test = r.gath.at[:, seat_rows]
    for k in range(2, OCTET, 2):
        remote(seat_test, seat_test, r.fw_send, r.fw_recv, flip(k))
    first_take(3)
    if group_of(n_dev, 3)[1] == 1:
        solve(3)
    first_take(4)
    if group_of(n_dev, 4)[1] == 1:
        solve(4)
    drain(r.train.at[0], r.tr_recv)
    widen_train(1)
    turn(LEVELS - 1)
    for level in (4, 3, 2, 1):
        if group_of(n_dev, level)[1] > 1:
            second_take(level)
            solve(level)
    drain(r.gath.at[:, pl.ds(0, (OCTET // 2 - 1) * octets * half)], r.fw_recv)
    widen_tests()
    fill(0)
    fill(1)

    pairs_ab = {}
    for level in range(2, LEVELS + 1):
        blocks = gathered(level)
        value = jnp.concatenate([blocks[0], blocks[1].astype(f32)], axis=0)
        for k in range(2, level):
            ab_high, ab_low = pairs_ab[k]
            value = value - dot(ab_high, blocks[k]) - dot(ab_low, blocks[k])
        pairs_ab[level] = split(value)
        r.ab[:, pl.ds((level - 2) * rank, rank)] = value
    b_high, b_low = split(r.ab[pl.ds(width, rank)])
    first = gathered(1)[0]
    s_high, s_low = split(first)
    later = r.ab[pl.ds(0, width)] - (dot(s_high, b_high) + dot(s_low, b_high) + dot(s_high, b_low))
    shares = jnp.concatenate([first, later], axis=1)
    share_high, share_low = split(shares)
    left_high = r.stack[pl.ds(2 * width, LEVELS * rank)]
    product = dot(jnp.concatenate([share_high, share_low], axis=0), left_high)
    current = r.tgt[...] - (product[:width] + product[width:] + dot(share_high, r.ltl[...]))
    r.cur[...] = current
    weights = current.astype(bf16)
    r.wt[0] = weights
    remote(r.wt.at[0], r.wt.at[1], r.wt_send, r.wt_recv, flip(1))
    cur_copy = pltpu.make_async_copy(r.cur, r.cur_out, r.out_sem)
    cur_copy.start()

    big = min(256, pairs * half)

    def weigh(which):
        twice = jnp.concatenate([r.wt[which], r.wt[which]], axis=0)
        first_half = lax.broadcasted_iota(jnp.int32, (big, 2 * width), 1) < width

        def step(i, carry):
            part = pl.ds(pl.multiple_of(i * big, big), big)
            other = pl.ds(pl.multiple_of(pairs * half + i * big, big), big)
            there = pl.ds(which * points, points)
            value = dot_nt(
                jnp.concatenate([r.kmat[part, there], r.kmat[other, there]], axis=0), twice
            )
            value = jnp.where(first_half, value[:big], value[big:])
            if which == 0:
                r.terms[part] = value
            else:
                r.term_b[part] = (r.terms[part] + value).astype(bf16)
            return carry

        lax.fori_loop(0, pairs * half // big, step, 0)

    weigh(0)
    drain(r.wt.at[1], r.wt_recv)
    weigh(1)

    def scatter(k, carry):
        block = (own_block + k) % pairs
        to = (block % octets) * (OCTET // 2) + block // octets
        remote(
            r.term_b.at[pl.ds(pl.multiple_of(block * half, half), half)],
            r.term_in.at[pl.ds(pl.multiple_of((k - 1) * half, half), half)],
            r.rs_send, r.rs_recv, coords(2 * to + parity),
        )
        return carry

    lax.fori_loop(1, pairs, scatter, 0)
    drain(r.gath.at[:, pl.ds(0, (octets - 1) * half)], r.ag_send)
    drain(r.gath.at[:, pl.ds(0, (OCTET // 2 - 1) * octets * half)], r.fw_send)
    drain(r.train.at[0], r.tr_send)
    drain(r.wt.at[0], r.wt_send)
    for level in range(1, LEVELS + 1):
        size, count = group_of(n_dev, level)
        lev = level - 1
        drain(getattr(r, f"recv{level}").at[pl.ds(1, size - 1)], r.p1_send.at[lev])
        if count > 1:
            drain(getattr(r, f"hop{level}").at[pl.ds(1, count - 1)], r.p2_send.at[lev])
        drain(getattr(r, f"share{level}").at[pl.ds(0, size - 1)], r.p3_send.at[lev])
    cur_copy.wait()
    total = r.term_b[own_rows].astype(f32)
    drain(r.term_in, r.rs_recv)
    total = total + jnp.sum(r.term_in[...].astype(f32).reshape(pairs - 1, half, 2 * width), axis=0)
    r.pred_out[pl.ds(0, half)] = total[:, :width]
    r.pred_out[pl.ds(half, half)] = total[:, width:]
    drain(r.term_in, r.rs_send)


def finish(cur_in, pred_in, cur_out, pred_out, sems):
    copies = [
        pltpu.make_async_copy(cur_in, cur_out, sems.at[0]),
        pltpu.make_async_copy(pred_in, pred_out, sems.at[1]),
    ]
    for copy in copies:
        copy.start()
    for copy in copies:
        copy.wait()


def body(n_dev, narrow, targets, train, test, left, right, cap, pivots):
    points, width = targets.shape
    rank = left.shape[2]
    feat = train.shape[1]
    rows = test.shape[0]
    half = rows // 2
    pairs = n_dev // 2
    vmem = pltpu.VMEM
    dma = pltpu.SemaphoreType.DMA
    hbm_spec = pl.BlockSpec(memory_space=pl.ANY)
    vmem_spec = pl.BlockSpec(memory_space=pltpu.VMEM)
    scratch = {
        "tgt": vmem((width, points), f32),
        "piv": vmem(pivots.shape, jnp.int32),
        "train": vmem((2, points, feat), bf16),
        "gath": vmem((2, pairs * half, feat), bf16),
        "left": vmem((LEVELS, points, rank), f32),
        "right": vmem((LEVELS, points, rank), f32),
        "cap": vmem((LEVELS, 2 * rank, 2 * rank), f32),
        "caps": vmem((2, LEVELS, 2 * rank, 2 * rank), bf16),
        "chosen": vmem((LEVELS, 2 * rank, 2 * rank), bf16),
        "stack": vmem((2 * width + LEVELS * rank, points), bf16),
        "ltl": vmem((LEVELS * rank, points), bf16),
        "train_w": vmem((2, points, 2 * feat), bf16),
        "test_w": vmem((pairs * rows, 2 * feat), bf16),
        "kmat": vmem((pairs * rows, 2 * points), bf16),
        "ab": vmem((width + rank, (LEVELS - 1) * rank), f32),
        "cur": vmem((width, points), f32),
        "wt": vmem((2, width, points), bf16),
        "terms": vmem((pairs * half, 2 * width), f32),
        "term_b": vmem((pairs * half, 2 * width), bf16),
        "term_in": vmem(((pairs - 1) * half, 2 * width), bf16),
    }
    for level in range(1, LEVELS + 1):
        size, count = group_of(n_dev, level)
        tall = (2 * width + (level - 1) * rank) // size
        for name in ("send", "recv", "share"):
            scratch[f"{name}{level}"] = vmem((size, tall, rank), bf16)
        scratch[f"out{level}"] = vmem((2, tall, rank), bf16)
        if count > 1:
            scratch[f"hop{level}"] = vmem((count, tall, rank), bf16)
    scratch["load_sem"] = dma((4 + 2 * LEVELS,))
    scratch["cap_sem"] = dma((LEVELS, 2))
    for name in ("p1_send", "p1_recv", "p2_send", "p2_recv", "p3_send", "p3_recv"):
        scratch[name] = dma((LEVELS,))
    for name in (
        "ag_send", "ag_recv", "tr_send", "tr_recv", "wt_send", "wt_recv", "rs_send", "rs_recv",
        "out_sem", "piv_sem", "fw_send", "fw_recv",
    ):
        scratch[name] = dma
    names = ["tgt_h", "train_h", "test_h", "left_h", "right_h", "cap_h", "piv_h"]
    names += ["cur_out", "pred_out"] + list(scratch)
    current, predictions = pl.pallas_call(
        functools.partial(kernel, n_dev, narrow, names),
        out_shape=(
            jax.ShapeDtypeStruct((width, points), f32),
            jax.ShapeDtypeStruct((rows, width), f32),
        ),
        in_specs=[pl.BlockSpec(memory_space=pltpu.HBM)] * 7,
        out_specs=(hbm_spec, vmem_spec),
        scratch_shapes=list(scratch.values()),
        compiler_params=pltpu.CompilerParams(
            collective_id=0, has_side_effects=True, vmem_limit_bytes=48 * 1024 * 1024
        ),
    )(*(
        pltpu.with_memory_space_constraint(value, pltpu.HBM)
        for value in (targets.T, train, test, left, right, cap, pivots)
    ))
    current, predictions = pl.pallas_call(
        finish,
        out_shape=(
            jax.ShapeDtypeStruct((width, points), f32),
            jax.ShapeDtypeStruct((rows, width), f32),
        ),
        in_specs=[vmem_spec] * 2,
        out_specs=(hbm_spec, hbm_spec),
        scratch_shapes=[dma((2,))],
    )(*(
        pltpu.with_memory_space_constraint(value, pltpu.VMEM) for value in (current, predictions)
    ))
    return current.T, predictions


def solution(mesh):
    both = ("wide", "narrow")
    placed = (
        P(both, None), P(both, None), P(both, None),
        P(both, None, None), P(both, None, None), P(), P(),
    )
    sizes = dict(mesh.shape)
    return jax.shard_map(
        functools.partial(body, sizes["wide"] * sizes["narrow"], sizes["narrow"]),
        mesh=mesh,
        in_specs=placed,
        out_specs=(P(both, None), P(both, None)),
        check_vma=False,
    )
```

```python
import functools
import math
import types

import jax
import jax.numpy as jnp
from jax import lax
from jax.experimental import pallas as pl
from jax.experimental.pallas import tpu as pltpu
from jax.sharding import PartitionSpec as P

LEVELS = 4
OCTET = 8
spread_coef = 3.0
MESH = pl.DeviceIdType.MESH
f32, bf16 = jnp.float32, jnp.bfloat16


def dot(a, b):
    return jnp.dot(a, b, preferred_element_type=f32)


def dot_nt(a, b):
    return lax.dot_general(a, b, (((1,), (1,)), ((), ())), preferred_element_type=f32)


def split(value):
    high = value.astype(bf16)
    return high, (value - high.astype(f32)).astype(bf16)


def halves_of(value):
    high = value.astype(bf16).astype(f32)
    return high, value - high


def group_of(n_dev, level):
    node = n_dev >> (level - 1)
    size = min(OCTET, node)
    return size, node // size


def kernel(n_dev, narrow, names, *refs):
    r = types.SimpleNamespace(**dict(zip(names, refs)))
    pos = lax.axis_index("wide") * narrow + lax.axis_index("narrow")
    width, points = r.tgt.shape
    rank = r.right.shape[2]
    feat = r.train.shape[2]
    rows = r.test_h.shape[0]
    half = rows // 2
    pairs = n_dev // 2
    parity = pos % 2
    slot = pos // 2
    octets = n_dev // OCTET
    seat = slot % (OCTET // 2)
    own_block = seat * octets + slot // (OCTET // 2)
    own_rows = pl.ds(pl.multiple_of(own_block * half, half), half)
    seat_rows = pl.ds(pl.multiple_of(seat * octets * half, octets * half), octets * half)

    def coords(dev):
        return (dev // narrow, dev % narrow)

    def flip(mask):
        dev = pos
        for bit in range(mask.bit_length()):
            if mask >> bit & 1:
                dev = dev + (1 << bit) * (1 - 2 * ((pos // (1 << bit)) % 2))
        return coords(dev)

    def remote(src, dst, send_sem, recv_sem, where):
        pltpu.make_async_remote_copy(
            src_ref=src, dst_ref=dst, send_sem=send_sem, recv_sem=recv_sem,
            device_id=where, device_id_type=MESH,
        ).start()

    def drain(part, sem):
        pltpu.make_async_copy(part, part, sem).wait()

    def load(src, dst, sem):
        copy = pltpu.make_async_copy(src, dst, sem)
        copy.start()
        return copy

    test_loads = [
        load(r.test_h.at[pl.ds(h * half, half)], r.gath.at[h, own_rows], r.load_sem.at[0 + h])
        for h in range(2)
    ]
    tgt_load = load(r.tgt_h, r.tgt, r.load_sem.at[2])
    piv_load = load(r.piv_h, r.piv, r.piv_sem)
    right_loads, left_loads = [], []
    train_load = None
    for lev in range(LEVELS):
        right_loads.append(load(r.right_h.at[:, lev, :], r.right.at[lev], r.load_sem.at[4 + lev]))
        if lev == 0:
            train_load = load(r.train_h, r.train.at[0], r.load_sem.at[3])
        left_loads.append(
            load(r.left_h.at[:, lev, :], r.left.at[lev], r.load_sem.at[4 + LEVELS + lev])
        )
    cap_loads, odds, heaps = [], [], []
    for level in range(1, LEVELS + 1):
        child = pos // (n_dev >> level)
        odd = child % 2
        odds.append(odd)
        heaps.append((1 << level - 1) - 1 + child // 2)
        cap_loads.append([
            load(
                r.cap_h.at[heaps[-1], pl.ds(pl.multiple_of(which * rank, rank), rank)],
                r.cap.at[level - 1, pl.ds(at * rank, rank)],
                r.cap_sem.at[level - 1, at],
            )
            for at, which in enumerate((odd, 1 - odd))
        ])

    barrier = pltpu.get_barrier_semaphore()

    def greet(k, carry):
        pl.semaphore_signal(
            barrier, inc=1, device_id=coords((pos + OCTET * k) % n_dev), device_id_type=MESH
        )
        return carry

    lax.fori_loop(1, octets, greet, 0)
    for k in range(1, OCTET):
        pl.semaphore_signal(barrier, inc=1, device_id=flip(k), device_id_type=MESH)

    def first_send(level):
        size, _ = group_of(n_dev, level)
        mine = pos % size
        lev = level - 1
        for k in range(1, size):
            to = mine
            for bit in range(k.bit_length()):
                if k >> bit & 1:
                    to = to + (1 << bit) * (1 - 2 * ((mine // (1 << bit)) % 2))
            remote(
                getattr(r, f"send{level}").at[to], getattr(r, f"recv{level}").at[k],
                r.p1_send.at[lev], r.p1_recv.at[lev], flip(k),
            )

    def gram(level):
        lev = level - 1
        size, _ = group_of(n_dev, level)
        right_loads[lev].wait()
        high, low = split(r.right[lev])
        product = dot(r.stack[pl.ds(0, 2 * width + lev * rank)], high)
        t = product[:width] + product[width : 2 * width] + dot(r.stack[pl.ds(0, width)], low)
        t_high, t_low = halves_of(t)
        part = width // size
        both = jnp.concatenate(
            [t_high.reshape(size, part, rank), t_low.reshape(size, part, rank)], axis=1
        )
        send = getattr(r, f"send{level}")
        send[:, pl.ds(0, 2 * part)] = both.astype(bf16)
        cut = rank // size
        for k in range(lev):
            piece = product[2 * width + k * rank : 2 * width + (k + 1) * rank]
            send[:, pl.ds(2 * part + k * cut, cut)] = piece.astype(bf16).reshape(size, cut, rank)

    def turn(lev):
        left_loads[lev].wait()
        high, low = split(r.left[lev].T)
        r.stack[pl.ds(2 * width + lev * rank, rank)] = high
        r.ltl[pl.ds(lev * rank, rank)] = low

    sums = {}

    def joined(value, level):
        part = width // group_of(n_dev, level)[0]
        top = value[:part] + value[part : 2 * part]
        return top if level == 1 else jnp.concatenate([top, value[2 * part :]], axis=0)

    def packed(value, level):
        part = width // group_of(n_dev, level)[0]
        high, low = halves_of(value[:part])
        pieces = [high, low] if level == 1 else [high, low, value[part:]]
        return jnp.concatenate(pieces, axis=0).astype(bf16)

    def first_take(level):
        size, count = group_of(n_dev, level)
        lev = level - 1
        recv, send = getattr(r, f"recv{level}"), getattr(r, f"send{level}")
        drain(recv.at[pl.ds(1, size - 1)], r.p1_recv.at[lev])
        near = send[pos % size].astype(f32)
        far = None
        for k in range(1, size):
            value = recv[k].astype(f32)
            if count > 1 or k < size // 2:
                near = near + value
            else:
                far = value if far is None else far + value
        near = joined(near, level)
        if count == 1:
            sums[level] = (near, joined(far, level))
            return
        sums[level] = (near, None)
        hop = getattr(r, f"hop{level}")
        hop[0] = packed(near, level)
        for j in range(1, count):
            remote(hop.at[0], hop.at[j], r.p2_send.at[lev], r.p2_recv.at[lev], flip(j * OCTET))

    def second_take(level):
        size, count = group_of(n_dev, level)
        if count == 1:
            return
        hop = getattr(r, f"hop{level}")
        drain(hop.at[pl.ds(1, count - 1)], r.p2_recv.at[level - 1])
        near, far = sums[level][0], None
        for j in range(1, count):
            value = joined(hop[j].astype(f32), level)
            if j < count // 2:
                near = near + value
            else:
                far = value if far is None else far + value
        sums[level] = (near, far)

    def solve(level):
        size, count = group_of(n_dev, level)
        lev = level - 1
        near, far = sums[level]
        cols = near.shape[0]
        both = jnp.concatenate([near, far], axis=1)
        high, low = halves_of(both)
        moved = dot(jnp.concatenate([high, low], axis=0).astype(bf16), r.chosen[lev])
        kids = 1 if count > 1 else 2
        cap_high = r.caps[0, lev, pl.ds(0, kids * rank)]
        cap_low = r.caps[1, lev, pl.ds(0, kids * rank)]
        result = dot_nt(moved.astype(bf16), cap_high)
        result = result[:cols] + result[cols:] + dot_nt(moved[:cols].astype(bf16), cap_low)
        share, out = getattr(r, f"share{level}"), getattr(r, f"out{level}")
        for kid in range(kids):
            out[kid] = packed(result[:, kid * rank : (kid + 1) * rank], level)
        mine = pos % size
        for k in range(1, size):
            kid = 1 if count == 1 and k >= size // 2 else 0
            remote(
                out.at[kid], share.at[mine], r.p3_send.at[lev], r.p3_recv.at[lev], flip(k)
            )
        share[mine] = out[0]

    def gathered(level):
        size, _ = group_of(n_dev, level)
        share = getattr(r, f"share{level}")
        drain(share.at[pl.ds(0, size - 1)], r.p3_recv.at[level - 1])
        part, cut = width // size, rank // size
        top = share[:, pl.ds(0, 2 * part)].astype(f32)
        top = (top[:, :part] + top[:, part:]).reshape(width, rank)
        return [top] + [
            share[:, pl.ds(2 * part + k * cut, cut)].reshape(rank, rank) for k in range(level - 1)
        ]

    def prepare(lev):
        for copy in cap_loads[lev]:
            copy.wait()
        high, low = split(r.cap[lev])
        r.caps[0, lev] = high
        r.caps[1, lev] = low
        order = lax.broadcasted_iota(jnp.int32, (2 * rank, 2 * rank), 0)
        pivots = r.piv[pl.ds(heaps[lev], 1), :]
        at = pivots + rank * (1 - odds[lev])
        at = jnp.where(at >= 2 * rank, at - 2 * rank, at)
        r.chosen[lev] = (order == at).astype(f32).astype(bf16)

    def widened(value, own_squares_at, ones_at):
        value_f = value.astype(f32)
        high, low = split(value_f * value_f)
        squares = dot(
            jnp.concatenate([high, low], axis=1), jnp.ones((2 * feat, feat), bf16)
        )
        one = squares.astype(bf16).astype(f32)
        two = (squares - one).astype(bf16).astype(f32)
        three = squares - one - two
        lane = lax.broadcasted_iota(jnp.int32, squares.shape, 1)
        extra = jnp.where((lane >= ones_at) & (lane < ones_at + 3), 1.0, 0.0)
        for i, piece in enumerate((one, two, three)):
            extra = jnp.where(lane == own_squares_at + i, -piece, extra)
        return extra.astype(bf16)

    def widen_train(which):
        value = r.train[which]
        r.train_w[which, :, pl.ds(0, feat)] = value + value
        r.train_w[which, :, pl.ds(feat, feat)] = widened(value, 3, 0)

    def widen_tests():
        def step(i, carry):
            part = pl.ds(pl.multiple_of(i * wide_rows, wide_rows), wide_rows)
            for h in range(2):
                value = r.gath[h, part]
                there = pl.ds(
                    pl.multiple_of(h * pairs * half + i * wide_rows, wide_rows), wide_rows
                )
                r.test_w[there, pl.ds(0, feat)] = value
                r.test_w[there, pl.ds(feat, feat)] = widened(value, 0, 3)
            return carry

        wide_rows = min(256, pairs * half)
        lax.fori_loop(0, pairs * half // wide_rows, step, 0)

    rate = spread_coef / feat * math.log2(math.e)
    chunk = min(512, pairs * rows)

    def fill(which):
        def step(i, carry):
            part = pl.ds(pl.multiple_of(i * chunk, chunk), chunk)
            negative = dot_nt(r.test_w[part], r.train_w[which])
            r.kmat[part, pl.ds(which * points, points)] = jnp.exp2(rate * negative).astype(bf16)
            return carry

        lax.fori_loop(0, pairs * rows // chunk, step, 0)

    tgt_load.wait()
    high, low = split(r.tgt[...])
    r.stack[pl.ds(0, width)] = high
    r.stack[pl.ds(width, width)] = low
    gram(1)
    turn(0)
    for copy in test_loads:
        copy.wait()
    train_load.wait()
    pl.semaphore_wait(barrier, octets - 1 + OCTET - 1)
    first_send(1)
    own_test = r.gath.at[:, own_rows]

    def spread(k, carry):
        remote(own_test, own_test, r.ag_send, r.ag_recv, coords((pos + OCTET * k) % n_dev))
        return carry

    lax.fori_loop(1, octets, spread, 0)
    gram(2)
    first_send(2)
    remote(r.train.at[0], r.train.at[1], r.tr_send, r.tr_recv, flip(1))
    turn(1)
    gram(3)
    first_send(3)
    turn(2)
    gram(4)
    first_send(4)
    widen_train(0)
    piv_load.wait()
    for lev in range(LEVELS):
        prepare(lev)
    first_take(1)
    first_take(2)
    drain(r.gath.at[:, pl.ds(0, (octets - 1) * half)], r.ag_recv)
    seat_test = r.gath.at[:, seat_rows]
    for k in range(2, OCTET, 2):
        remote(seat_test, seat_test, r.fw_send, r.fw_recv, flip(k))
    first_take(3)
    if group_of(n_dev, 3)[1] == 1:
        solve(3)
    first_take(4)
    if group_of(n_dev, 4)[1] == 1:
        solve(4)
    drain(r.train.at[0], r.tr_recv)
    widen_train(1)
    turn(LEVELS - 1)
    for level in (4, 3, 2, 1):
        if group_of(n_dev, level)[1] > 1:
            second_take(level)
            solve(level)
    drain(r.gath.at[:, pl.ds(0, (OCTET // 2 - 1) * octets * half)], r.fw_recv)
    widen_tests()
    fill(0)
    fill(1)

    third, fourth = gathered(3), gathered(4)
    high, low = split(third[0])
    product = dot(jnp.concatenate([high, low, third[1], third[2]], axis=0), fourth[3])
    r.base[:, pl.ds(0, rank)] = third[0]
    r.base[:, pl.ds(rank, rank)] = fourth[0] - (product[:width] + product[width : 2 * width])
    for k in range(2):
        there = pl.ds(k * rank, rank)
        r.mix[there, pl.ds(0, rank)] = third[1 + k]
        at = 2 * width + k * rank
        high, low = split(fourth[1 + k].astype(f32) - product[at : at + rank])
        r.mix[there, pl.ds(rank, rank)] = high
        r.mix_low[there] = low
    second = gathered(2)
    first = gathered(1)[0]
    high, low = split(first)
    product = dot(jnp.concatenate([high, low], axis=0), second[1])
    upper = jnp.concatenate([first, second[0] - (product[:width] + product[width:])], axis=1)
    high, low = split(upper)
    product = dot(jnp.concatenate([high, low], axis=0), r.mix[...])
    lower = r.base[...] - (product[:width] + product[width:])
    shares = jnp.concatenate(
        [upper, lower[:, :rank], lower[:, rank:] - dot(high, r.mix_low[...])], axis=1
    )
    share_high, share_low = split(shares)
    left_high = r.stack[pl.ds(2 * width, LEVELS * rank)]
    product = dot(jnp.concatenate([share_high, share_low], axis=0), left_high)
    current = r.tgt[...] - (product[:width] + product[width:] + dot(share_high, r.ltl[...]))
    r.cur[...] = current
    weights = current.astype(bf16)
    r.wt[0] = weights
    remote(r.wt.at[0], r.wt.at[1], r.wt_send, r.wt_recv, flip(1))
    cur_copy = pltpu.make_async_copy(r.cur, r.cur_out, r.out_sem)
    cur_copy.start()

    big = min(256, pairs * half)

    def weigh(which):
        twice = jnp.concatenate([r.wt[which], r.wt[which]], axis=0)
        first_half = lax.broadcasted_iota(jnp.int32, (big, 2 * width), 1) < width

        def step(i, carry):
            part = pl.ds(pl.multiple_of(i * big, big), big)
            other = pl.ds(pl.multiple_of(pairs * half + i * big, big), big)
            there = pl.ds(which * points, points)
            value = jnp.where(
                first_half, dot_nt(r.kmat[part, there], twice), dot_nt(r.kmat[other, there], twice)
            )
            if which == 0:
                r.terms[part] = value
            else:
                r.term_b[part] = (r.terms[part] + value).astype(bf16)
            return carry

        lax.fori_loop(0, pairs * half // big, step, 0)

    weigh(0)
    drain(r.wt.at[1], r.wt_recv)
    weigh(1)

    own_copy = pltpu.make_async_copy(
        r.term_b.at[own_rows], r.term_out.at[pl.ds((pairs - 1) * half, half)], r.own_sem
    )
    own_copy.start()
    for turned in (3, 2, 1, 0):
        base = pos
        for bit in range(2):
            if turned >> bit & 1:
                base = base + (2 << bit) * (1 - 2 * ((pos // (2 << bit)) % 2))

        def scatter(j, carry, base=base, turned=turned):
            to = (base + OCTET * j) % n_dev
            block = ((to // 2) % (OCTET // 2)) * octets + to // OCTET
            remote(
                r.term_b.at[pl.ds(pl.multiple_of(block * half, half), half)],
                r.term_out.at[pl.ds(pl.multiple_of((turned * octets + j - 1) * half, half), half)],
                r.rs_send, r.rs_recv, coords(to),
            )
            return carry

        start = 0 if turned else 1
        if octets <= 4:
            for j in range(start, octets):
                scatter(j, 0)
        else:
            lax.fori_loop(start, octets, scatter, 0)
    drain(r.gath.at[:, pl.ds(0, (octets - 1) * half)], r.ag_send)
    drain(r.gath.at[:, pl.ds(0, (OCTET // 2 - 1) * octets * half)], r.fw_send)
    drain(r.train.at[0], r.tr_send)
    drain(r.wt.at[0], r.wt_send)
    for level in range(1, LEVELS + 1):
        size, count = group_of(n_dev, level)
        lev = level - 1
        drain(getattr(r, f"recv{level}").at[pl.ds(1, size - 1)], r.p1_send.at[lev])
        if count > 1:
            drain(getattr(r, f"hop{level}").at[pl.ds(1, count - 1)], r.p2_send.at[lev])
        drain(getattr(r, f"share{level}").at[pl.ds(0, size - 1)], r.p3_send.at[lev])
    cur_copy.wait()
    own_copy.wait()
    landed = r.term_out.at[pl.ds(0, (pairs - 1) * half)]
    drain(landed, r.rs_recv)
    drain(landed, r.rs_send)


def finish(cur_in, terms_in, cur_out, pred_out, pred, sems):
    cur_copy = pltpu.make_async_copy(cur_in, cur_out, sems.at[0])
    cur_copy.start()
    half, width = pred.shape[0] // 2, pred.shape[1]
    terms = terms_in[...].astype(f32)
    total = jnp.sum(terms.reshape(terms.shape[0] // half, half, 2 * width), axis=0)
    pred[pl.ds(0, half)] = total[:, :width]
    pred[pl.ds(half, half)] = total[:, width:]
    pred_copy = pltpu.make_async_copy(pred, pred_out, sems.at[1])
    pred_copy.start()
    cur_copy.wait()
    pred_copy.wait()


def body(n_dev, narrow, targets, train, test, left, right, cap, pivots):
    points, width = targets.shape
    rank = left.shape[2]
    feat = train.shape[1]
    rows = test.shape[0]
    half = rows // 2
    pairs = n_dev // 2
    vmem = pltpu.VMEM
    dma = pltpu.SemaphoreType.DMA
    hbm_spec = pl.BlockSpec(memory_space=pl.ANY)
    vmem_spec = pl.BlockSpec(memory_space=pltpu.VMEM)
    scratch = {
        "tgt": vmem((width, points), f32),
        "piv": vmem(pivots.shape, jnp.int32),
        "train": vmem((2, points, feat), bf16),
        "gath": vmem((2, pairs * half, feat), bf16),
        "left": vmem((LEVELS, points, rank), f32),
        "right": vmem((LEVELS, points, rank), f32),
        "cap": vmem((LEVELS, 2 * rank, 2 * rank), f32),
        "caps": vmem((2, LEVELS, 2 * rank, 2 * rank), bf16),
        "chosen": vmem((LEVELS, 2 * rank, 2 * rank), bf16),
        "stack": vmem((2 * width + LEVELS * rank, points), bf16),
        "ltl": vmem((LEVELS * rank, points), bf16),
        "train_w": vmem((2, points, 2 * feat), bf16),
        "test_w": vmem((pairs * rows, 2 * feat), bf16),
        "kmat": vmem((pairs * rows, 2 * points), bf16),
        "base": vmem((width, 2 * rank), f32),
        "mix": vmem((2 * rank, 2 * rank), bf16),
        "mix_low": vmem((2 * rank, rank), bf16),
        "cur": vmem((width, points), f32),
        "wt": vmem((2, width, points), bf16),
        "terms": vmem((pairs * half, 2 * width), f32),
        "term_b": vmem((pairs * half, 2 * width), bf16),
    }
    for level in range(1, LEVELS + 1):
        size, count = group_of(n_dev, level)
        tall = (2 * width + (level - 1) * rank) // size
        for name in ("send", "recv", "share"):
            scratch[f"{name}{level}"] = vmem((size, tall, rank), bf16)
        scratch[f"out{level}"] = vmem((2, tall, rank), bf16)
        if count > 1:
            scratch[f"hop{level}"] = vmem((count, tall, rank), bf16)
    scratch["load_sem"] = dma((4 + 2 * LEVELS,))
    scratch["cap_sem"] = dma((LEVELS, 2))
    for name in ("p1_send", "p1_recv", "p2_send", "p2_recv", "p3_send", "p3_recv"):
        scratch[name] = dma((LEVELS,))
    for name in (
        "ag_send", "ag_recv", "tr_send", "tr_recv", "wt_send", "wt_recv", "rs_send", "rs_recv",
        "out_sem", "own_sem", "piv_sem", "fw_send", "fw_recv",
    ):
        scratch[name] = dma
    names = ["tgt_h", "train_h", "test_h", "left_h", "right_h", "cap_h", "piv_h"]
    names += ["cur_out", "term_out"] + list(scratch)
    current, terms = pl.pallas_call(
        functools.partial(kernel, n_dev, narrow, names),
        out_shape=(
            jax.ShapeDtypeStruct((width, points), f32),
            jax.ShapeDtypeStruct((pairs * half, 2 * width), bf16),
        ),
        in_specs=[pl.BlockSpec(memory_space=pltpu.HBM)] * 7,
        out_specs=(hbm_spec, hbm_spec),
        scratch_shapes=list(scratch.values()),
        compiler_params=pltpu.CompilerParams(
            collective_id=0, has_side_effects=True, vmem_limit_bytes=48 * 1024 * 1024
        ),
    )(*(
        pltpu.with_memory_space_constraint(value, pltpu.HBM)
        for value in (targets.T, train, test, left, right, cap, pivots)
    ))
    current, predictions = pl.pallas_call(
        finish,
        out_shape=(
            jax.ShapeDtypeStruct((width, points), f32),
            jax.ShapeDtypeStruct((rows, width), f32),
        ),
        in_specs=[vmem_spec] * 2,
        out_specs=(hbm_spec, hbm_spec),
        scratch_shapes=[vmem((rows, width), f32), dma((2,))],
    )(*(
        pltpu.with_memory_space_constraint(value, pltpu.VMEM) for value in (current, terms)
    ))
    return current.T, predictions


def solution(mesh):
    both = ("wide", "narrow")
    placed = (
        P(both, None), P(both, None), P(both, None),
        P(both, None, None), P(both, None, None), P(), P(),
    )
    sizes = dict(mesh.shape)
    return jax.shard_map(
        functools.partial(body, sizes["wide"] * sizes["narrow"], sizes["narrow"]),
        mesh=mesh,
        in_specs=placed,
        out_specs=(P(both, None), P(both, None)),
        check_vma=False,
    )
```

```python
import functools
import math
import types

import jax
import jax.numpy as jnp
from jax import lax
from jax.experimental import pallas as pl
from jax.experimental.pallas import tpu as pltpu
from jax.sharding import PartitionSpec as P

LEVELS = 4
OCTET = 8
spread_coef = 3.0
MESH = pl.DeviceIdType.MESH
f32, bf16 = jnp.float32, jnp.bfloat16


def dot(a, b):
    return jnp.dot(a, b, preferred_element_type=f32)


def dot_nt(a, b):
    return lax.dot_general(a, b, (((1,), (1,)), ((), ())), preferred_element_type=f32)


def split(value):
    high = value.astype(bf16)
    return high, (value - high.astype(f32)).astype(bf16)


def halves_of(value):
    high = value.astype(bf16).astype(f32)
    return high, value - high


def group_of(n_dev, level):
    node = n_dev >> (level - 1)
    size = min(OCTET, node)
    return size, node // size


def kernel(n_dev, narrow, names, *refs):
    r = types.SimpleNamespace(**dict(zip(names, refs)))
    pos = lax.axis_index("wide") * narrow + lax.axis_index("narrow")
    width, points = r.tgt.shape
    rank = r.right_h.shape[2]
    feat = r.train.shape[2]
    half = r.test_h.shape[1]
    rows = 2 * half
    pairs = n_dev // 2
    parity = pos % 2
    slot = pos // 2
    octets = n_dev // OCTET
    seat = slot % (OCTET // 2)
    own_block = seat * octets + slot // (OCTET // 2)
    own_rows = pl.ds(pl.multiple_of(own_block * half, half), half)
    seat_rows = pl.ds(pl.multiple_of(seat * octets * half, octets * half), octets * half)

    def coords(dev):
        return (dev // narrow, dev % narrow)

    def flip(mask):
        dev = pos
        for bit in range(mask.bit_length()):
            if mask >> bit & 1:
                dev = dev + (1 << bit) * (1 - 2 * ((pos // (1 << bit)) % 2))
        return coords(dev)

    def remote(src, dst, send_sem, recv_sem, where):
        pltpu.make_async_remote_copy(
            src_ref=src, dst_ref=dst, send_sem=send_sem, recv_sem=recv_sem,
            device_id=where, device_id_type=MESH,
        ).start()

    def drain(part, sem):
        pltpu.make_async_copy(part, part, sem).wait()

    def load(src, dst, sem):
        copy = pltpu.make_async_copy(src, dst, sem)
        copy.start()
        return copy

    barrier = pltpu.get_barrier_semaphore()

    def greet(k, carry):
        pl.semaphore_signal(
            barrier, inc=1, device_id=coords((pos + OCTET * k) % n_dev), device_id_type=MESH
        )
        return carry

    lax.fori_loop(1, octets, greet, 0)
    for k in range(1, OCTET):
        pl.semaphore_signal(barrier, inc=1, device_id=flip(k), device_id_type=MESH)

    def side(i, count=1):
        return pl.ds(i * points, count * points)

    tgt_load = load(r.tgt_h, r.tgt, r.load_sem.at[0])
    for i in range(2 * LEVELS):
        source = (r.right_h, r.left_h)[i % 2].at[:, i // 2, :]
        load(source, r.side.at[side(i)], r.side_sem.at[(i + 1) // 2])
        if i == 0:
            test_load = load(r.test_h, r.gath.at[:, own_rows], r.load_sem.at[1])
            train_load = load(r.train_h, r.train.at[0], r.load_sem.at[2])
    piv_load = load(r.piv_h, r.piv, r.load_sem.at[3])
    odds, heaps = [], []
    for level in range(1, LEVELS + 1):
        child = pos // (n_dev >> level)
        odds.append(child % 2)
        heaps.append((1 << level - 1) - 1 + child // 2)
        load(r.cap_h.at[heaps[-1]], r.cap.at[level - 1], r.load_sem.at[4])

    def first_send(level):
        size, _ = group_of(n_dev, level)
        mine = pos % size
        lev = level - 1
        for k in range(1, size):
            to = mine
            for bit in range(k.bit_length()):
                if k >> bit & 1:
                    to = to + (1 << bit) * (1 - 2 * ((mine // (1 << bit)) % 2))
            remote(
                getattr(r, f"send{level}").at[to], getattr(r, f"recv{level}").at[k],
                r.all_send, r.p1_recv.at[lev], flip(k),
            )

    def gram(level):
        lev = level - 1
        size, _ = group_of(n_dev, level)
        if level == 1:
            drain(r.side.at[side(0)], r.side_sem.at[0])
        high, low = split(r.side[side(2 * lev)])
        product = dot(r.stack[pl.ds(0, 2 * width + lev * rank)], high)
        t = product[:width] + product[width : 2 * width] + dot(r.stack[pl.ds(0, width)], low)
        t_high, t_low = halves_of(t)
        part = width // size
        both = jnp.concatenate(
            [t_high.reshape(size, part, rank), t_low.reshape(size, part, rank)], axis=1
        )
        send = getattr(r, f"send{level}")
        send[:, pl.ds(0, 2 * part)] = both.astype(bf16)
        cut = rank // size
        for k in range(lev):
            piece = product[2 * width + k * rank : 2 * width + (k + 1) * rank]
            send[:, pl.ds(2 * part + k * cut, cut)] = piece.astype(bf16).reshape(size, cut, rank)

    def turn(lev):
        drain(r.side.at[side(2 * lev + 1, min(2, 2 * LEVELS - 1 - 2 * lev))], r.side_sem.at[lev + 1])
        high, low = split(r.side[side(2 * lev + 1)].T)
        r.stack[pl.ds(2 * width + lev * rank, rank)] = high
        r.ltl[pl.ds(lev * rank, rank)] = low

    sums = {}

    def joined(value, level):
        part = width // group_of(n_dev, level)[0]
        top = value[:part] + value[part : 2 * part]
        return top if level == 1 else jnp.concatenate([top, value[2 * part :]], axis=0)

    def packed(value, level):
        part = width // group_of(n_dev, level)[0]
        high, low = halves_of(value[:part])
        pieces = [high, low] if level == 1 else [high, low, value[part:]]
        return jnp.concatenate(pieces, axis=0).astype(bf16)

    def first_take(level):
        size, count = group_of(n_dev, level)
        lev = level - 1
        recv, send = getattr(r, f"recv{level}"), getattr(r, f"send{level}")
        drain(recv.at[pl.ds(1, size - 1)], r.p1_recv.at[lev])
        near = send[pos % size].astype(f32)
        far = None
        for k in range(1, size):
            value = recv[k].astype(f32)
            if count > 1 or k < size // 2:
                near = near + value
            else:
                far = value if far is None else far + value
        near = joined(near, level)
        if count == 1:
            sums[level] = (near, joined(far, level))
            return
        sums[level] = (near, None)
        hop = getattr(r, f"hop{level}")
        hop[0] = packed(near, level)
        for j in range(1, count):
            remote(hop.at[0], hop.at[j], r.all_send, r.p2_recv.at[lev], flip(j * OCTET))

    def second_take(level):
        size, count = group_of(n_dev, level)
        if count == 1:
            return
        hop = getattr(r, f"hop{level}")
        drain(hop.at[pl.ds(1, count - 1)], r.p2_recv.at[level - 1])
        near, far = sums[level][0], None
        for j in range(1, count):
            value = joined(hop[j].astype(f32), level)
            if j < count // 2:
                near = near + value
            else:
                far = value if far is None else far + value
        sums[level] = (near, far)

    def solve(level):
        size, count = group_of(n_dev, level)
        lev = level - 1
        near, far = sums[level]
        cols = near.shape[0]
        both = jnp.concatenate([near, far], axis=1)
        high, low = halves_of(both)
        moved = dot(jnp.concatenate([high, low], axis=0).astype(bf16), r.chosen[lev])
        odd = odds[lev]
        kids = 1 if count > 1 else 2
        taken = pl.ds(pl.multiple_of(odd * rank, rank), rank) if kids == 1 else pl.ds(0, 2 * rank)
        cap_high, cap_low = r.caps[0, lev, taken], r.caps[1, lev, taken]
        result = dot_nt(moved.astype(bf16), cap_high)
        result = result[:cols] + result[cols:] + dot_nt(moved[:cols].astype(bf16), cap_low)
        share, out = getattr(r, f"share{level}"), getattr(r, f"out{level}")
        for kid in range(kids):
            out[kid] = packed(result[:, kid * rank : (kid + 1) * rank], level)
        mine = pos % size
        for k in range(1, size):
            kid = 0 if kids == 1 else odd if k < size // 2 else 1 - odd
            remote(
                out.at[kid], share.at[mine], r.all_send, r.p3_recv.at[lev], flip(k)
            )
        share[mine] = out[0 if kids == 1 else odd]

    def gathered(level):
        size, _ = group_of(n_dev, level)
        share = getattr(r, f"share{level}")
        drain(share.at[pl.ds(0, size - 1)], r.p3_recv.at[level - 1])
        part, cut = width // size, rank // size
        top = share[:, pl.ds(0, 2 * part)].astype(f32)
        top = (top[:, :part] + top[:, part:]).reshape(width, rank)
        return [top] + [
            share[:, pl.ds(2 * part + k * cut, cut)].reshape(rank, rank) for k in range(level - 1)
        ]

    def prepare(lev):
        high, low = split(r.cap[lev])
        r.caps[0, lev] = high
        r.caps[1, lev] = low
        order = lax.broadcasted_iota(jnp.int32, (2 * rank, 2 * rank), 0)
        pivots = r.piv[pl.ds(heaps[lev], 1), :]
        at = pivots + rank * (1 - odds[lev])
        at = jnp.where(at >= 2 * rank, at - 2 * rank, at)
        r.chosen[lev] = (order == at).astype(f32).astype(bf16)

    def widened(value, own_squares_at, ones_at):
        value_f = value.astype(f32)
        high, low = split(value_f * value_f)
        squares = dot(
            jnp.concatenate([high, low], axis=1), jnp.ones((2 * feat, feat), bf16)
        )
        one = squares.astype(bf16).astype(f32)
        two = (squares - one).astype(bf16).astype(f32)
        three = squares - one - two
        lane = lax.broadcasted_iota(jnp.int32, squares.shape, 1)
        extra = jnp.where((lane >= ones_at) & (lane < ones_at + 3), 1.0, 0.0)
        for i, piece in enumerate((one, two, three)):
            extra = jnp.where(lane == own_squares_at + i, -piece, extra)
        return extra.astype(bf16)

    def widen_train(which):
        value = r.train[which]
        r.train_w[which, :, pl.ds(0, feat)] = value + value
        r.train_w[which, :, pl.ds(feat, feat)] = widened(value, 3, 0)

    def widen_tests():
        def step(i, carry):
            part = pl.ds(pl.multiple_of(i * wide_rows, wide_rows), wide_rows)
            for h in range(2):
                value = r.gath[h, part]
                there = pl.ds(
                    pl.multiple_of(h * pairs * half + i * wide_rows, wide_rows), wide_rows
                )
                r.test_w[there, pl.ds(0, feat)] = value
                r.test_w[there, pl.ds(feat, feat)] = widened(value, 0, 3)
            return carry

        wide_rows = min(256, pairs * half)
        lax.fori_loop(0, pairs * half // wide_rows, step, 0)

    rate = spread_coef / feat * math.log2(math.e)
    chunk = min(512, pairs * rows)

    def fill(which):
        def step(i, carry):
            part = pl.ds(pl.multiple_of(i * chunk, chunk), chunk)
            negative = dot_nt(r.test_w[part], r.train_w[which])
            r.kmat[part, pl.ds(which * points, points)] = jnp.exp2(rate * negative).astype(bf16)
            return carry

        lax.fori_loop(0, pairs * rows // chunk, step, 0)

    tgt_load.wait()
    high, low = split(r.tgt[...])
    r.stack[pl.ds(0, width)] = high
    r.stack[pl.ds(width, width)] = low
    gram(1)
    turn(0)
    test_load.wait()
    train_load.wait()
    pl.semaphore_wait(barrier, octets - 1 + OCTET - 1)
    first_send(1)
    own_test = r.gath.at[:, own_rows]

    def spread(k, carry):
        remote(own_test, own_test, r.all_send, r.ag_recv, coords((pos + OCTET * k) % n_dev))
        return carry

    lax.fori_loop(1, octets, spread, 0)
    gram(2)
    first_send(2)
    remote(r.train.at[0], r.train.at[1], r.all_send, r.tr_recv, flip(1))
    turn(1)
    gram(3)
    first_send(3)
    turn(2)
    gram(4)
    first_send(4)
    widen_train(0)
    piv_load.wait()
    drain(r.cap, r.load_sem.at[4])
    for lev in range(LEVELS):
        prepare(lev)
    first_take(1)
    first_take(2)
    drain(r.gath.at[:, pl.ds(0, (octets - 1) * half)], r.ag_recv)
    seat_test = r.gath.at[:, seat_rows]
    for k in range(2, OCTET, 2):
        remote(seat_test, seat_test, r.all_send, r.fw_recv, flip(k))
    first_take(3)
    if group_of(n_dev, 3)[1] == 1:
        solve(3)
    first_take(4)
    if group_of(n_dev, 4)[1] == 1:
        solve(4)
    drain(r.train.at[0], r.tr_recv)
    widen_train(1)
    turn(LEVELS - 1)
    for level in (4, 3, 2, 1):
        if group_of(n_dev, level)[1] > 1:
            second_take(level)
            solve(level)
    drain(r.gath.at[:, pl.ds(0, (OCTET // 2 - 1) * octets * half)], r.fw_recv)
    widen_tests()
    fill(0)
    fill(1)

    third, fourth = gathered(3), gathered(4)
    high, low = split(third[0])
    product = dot(jnp.concatenate([high, low, third[1], third[2]], axis=0), fourth[3])
    r.base[:, pl.ds(0, rank)] = third[0]
    r.base[:, pl.ds(rank, rank)] = fourth[0] - (product[:width] + product[width : 2 * width])
    for k in range(2):
        there = pl.ds(k * rank, rank)
        r.mix[there, pl.ds(0, rank)] = third[1 + k]
        at = 2 * width + k * rank
        high, low = split(fourth[1 + k].astype(f32) - product[at : at + rank])
        r.mix[there, pl.ds(rank, rank)] = high
        r.mix_low[there] = low
    base_high, base_low = split(r.base[...])
    mixed = jnp.concatenate([base_high, base_low, r.mix[...]], axis=0)
    mixed_high = jnp.concatenate([base_high, r.mix[...]], axis=0)
    wide = min(512, points)
    for i in range(points // wide):
        cut = pl.ds(i * wide, wide)
        top = dot(mixed, r.stack[pl.ds(2 * width + 2 * rank, 2 * rank), cut])
        bottom = dot(mixed_high, r.ltl[pl.ds(2 * rank, 2 * rank), cut])
        r.cur0[:, cut] = r.tgt[:, cut] - (top[:width] + top[width : 2 * width] + bottom[:width])
        rest = dot(r.mix_low[...], r.stack[pl.ds(2 * width + 3 * rank, rank), cut])
        own = r.stack[pl.ds(2 * width, 2 * rank), cut].astype(f32)
        own = own + r.ltl[pl.ds(0, 2 * rank), cut].astype(f32)
        high, low = split(own - (top[2 * width :] + bottom[width:] + rest))
        r.leff[0, :, cut] = high
        r.leff[1, :, cut] = low
    second = gathered(2)
    first = gathered(1)[0]
    high, low = split(first)
    product = dot(jnp.concatenate([high, low], axis=0), second[1])
    upper = jnp.concatenate([first, second[0] - (product[:width] + product[width:])], axis=1)
    high, low = split(upper)
    product = dot(jnp.concatenate([high, low], axis=0), r.leff[0])
    current = r.cur0[...] - (product[:width] + product[width:] + dot(high, r.leff[1]))
    r.cur[...] = current
    weights = current.astype(bf16)
    r.wt[0] = weights
    remote(r.wt.at[0], r.wt.at[1], r.all_send, r.wt_recv, flip(1))
    cur_copy = pltpu.make_async_copy(r.cur, r.cur_out, r.out_sem)
    cur_copy.start()

    big = min(256, pairs * half)

    def weigh(which):
        twice = jnp.concatenate([r.wt[which], r.wt[which]], axis=0)
        first_half = lax.broadcasted_iota(jnp.int32, (big, 2 * width), 1) < width

        def step(i, carry):
            part = pl.ds(pl.multiple_of(i * big, big), big)
            other = pl.ds(pl.multiple_of(pairs * half + i * big, big), big)
            there = pl.ds(which * points, points)
            value = jnp.where(
                first_half, dot_nt(r.kmat[part, there], twice), dot_nt(r.kmat[other, there], twice)
            )
            if which == 0:
                r.terms[part] = value
            else:
                r.term_b[part] = (r.terms[part] + value).astype(bf16)
            return carry

        lax.fori_loop(0, pairs * half // big, step, 0)

    weigh(0)
    drain(r.wt.at[1], r.wt_recv)
    weigh(1)

    own_copy = pltpu.make_async_copy(
        r.term_b.at[own_rows], r.term_out.at[pl.ds((pairs - 1) * half, half)], r.own_sem
    )
    own_copy.start()
    for turned in (3, 2, 1, 0):
        base = pos
        for bit in range(2):
            if turned >> bit & 1:
                base = base + (2 << bit) * (1 - 2 * ((pos // (2 << bit)) % 2))

        def scatter(j, carry, base=base, turned=turned):
            to = (base + OCTET * j) % n_dev
            block = ((to // 2) % (OCTET // 2)) * octets + to // OCTET
            remote(
                r.term_b.at[pl.ds(pl.multiple_of(block * half, half), half)],
                r.term_out.at[pl.ds(pl.multiple_of((turned * octets + j - 1) * half, half), half)],
                r.all_send, r.rs_recv, coords(to),
            )
            return carry

        start = 0 if turned else 1
        if octets <= 4:
            for j in range(start, octets):
                scatter(j, 0)
        else:
            lax.fori_loop(start, octets, scatter, 0)
    cur_copy.wait()
    own_copy.wait()
    landed = r.term_out.at[pl.ds(0, (pairs - 1) * half)]
    drain(landed, r.rs_recv)
    sent = 2 * points * feat + 2 * width * points
    sent += 2 * 2 * half * feat * (octets - 1 + (OCTET // 2 - 1) * octets) + 2 * (pairs - 1) * half * 2 * width
    for level in range(1, LEVELS + 1):
        size, count = group_of(n_dev, level)
        piece = 2 * getattr(r, f"send{level}").shape[1] * rank
        sent += piece * (2 * (size - 1) + count - 1)
    drain(r.side.at[pl.ds(0, sent // (4 * rank))], r.all_send)


def finish(cur_in, terms_in, cur_out, pred_out, pred, sems):
    cur_copy = pltpu.make_async_copy(cur_in, cur_out, sems.at[0])
    cur_copy.start()
    half, width = pred.shape[0] // 2, pred.shape[1]
    terms = terms_in[...].astype(f32)
    total = jnp.sum(terms.reshape(terms.shape[0] // half, half, 2 * width), axis=0)
    pred[pl.ds(0, half)] = total[:, :width]
    pred[pl.ds(half, half)] = total[:, width:]
    pred_copy = pltpu.make_async_copy(pred, pred_out, sems.at[1])
    pred_copy.start()
    cur_copy.wait()
    pred_copy.wait()


def body(n_dev, narrow, targets, train, test, left, right, cap, pivots):
    points, width = targets.shape
    rank = left.shape[2]
    feat = train.shape[1]
    rows = test.shape[0]
    half = rows // 2
    pairs = n_dev // 2
    vmem = pltpu.VMEM
    dma = pltpu.SemaphoreType.DMA
    hbm_spec = pl.BlockSpec(memory_space=pl.ANY)
    vmem_spec = pl.BlockSpec(memory_space=pltpu.VMEM)
    scratch = {
        "tgt": vmem((width, points), f32),
        "piv": vmem(pivots.shape, jnp.int32),
        "train": vmem((2, points, feat), bf16),
        "gath": vmem((2, pairs * half, feat), bf16),
        "side": vmem((2 * LEVELS * points, rank), f32),
        "cur0": vmem((width, points), f32),
        "leff": vmem((2, 2 * rank, points), bf16),
        "cap": vmem((LEVELS, 2 * rank, 2 * rank), f32),
        "caps": vmem((2, LEVELS, 2 * rank, 2 * rank), bf16),
        "chosen": vmem((LEVELS, 2 * rank, 2 * rank), bf16),
        "stack": vmem((2 * width + LEVELS * rank, points), bf16),
        "ltl": vmem((LEVELS * rank, points), bf16),
        "train_w": vmem((2, points, 2 * feat), bf16),
        "test_w": vmem((pairs * rows, 2 * feat), bf16),
        "kmat": vmem((pairs * rows, 2 * points), bf16),
        "base": vmem((width, 2 * rank), f32),
        "mix": vmem((2 * rank, 2 * rank), bf16),
        "mix_low": vmem((2 * rank, rank), bf16),
        "cur": vmem((width, points), f32),
        "wt": vmem((2, width, points), bf16),
        "terms": vmem((pairs * half, 2 * width), f32),
        "term_b": vmem((pairs * half, 2 * width), bf16),
    }
    for level in range(1, LEVELS + 1):
        size, count = group_of(n_dev, level)
        tall = (2 * width + (level - 1) * rank) // size
        for name in ("send", "recv", "share"):
            scratch[f"{name}{level}"] = vmem((size, tall, rank), bf16)
        scratch[f"out{level}"] = vmem((2, tall, rank), bf16)
        if count > 1:
            scratch[f"hop{level}"] = vmem((count, tall, rank), bf16)
    scratch["load_sem"] = dma((5,))
    scratch["side_sem"] = dma((LEVELS + 1,))
    scratch["p1_recv"] = dma((LEVELS,))
    scratch["p2_recv"] = dma((sum(group_of(n_dev, i + 1)[1] > 1 for i in range(LEVELS)),))
    scratch["p3_recv"] = dma((LEVELS,))
    for name in (
        "all_send", "ag_recv", "fw_recv", "tr_recv", "wt_recv", "rs_recv", "out_sem", "own_sem",
    ):
        scratch[name] = dma
    names = ["tgt_h", "train_h", "test_h", "left_h", "right_h", "cap_h", "piv_h"]
    names += ["cur_out", "term_out"] + list(scratch)
    current, terms = pl.pallas_call(
        functools.partial(kernel, n_dev, narrow, names),
        out_shape=(
            jax.ShapeDtypeStruct((width, points), f32),
            jax.ShapeDtypeStruct((pairs * half, 2 * width), bf16),
        ),
        in_specs=[pl.BlockSpec(memory_space=pltpu.HBM)] * 7,
        out_specs=(hbm_spec, hbm_spec),
        scratch_shapes=list(scratch.values()),
        compiler_params=pltpu.CompilerParams(
            collective_id=0, has_side_effects=True, vmem_limit_bytes=48 * 1024 * 1024
        ),
    )(*(
        pltpu.with_memory_space_constraint(value, pltpu.HBM)
        for value in (
            targets.T, train, test.reshape(2, half, feat), left, right, cap, pivots
        )
    ))
    current, predictions = pl.pallas_call(
        finish,
        out_shape=(
            jax.ShapeDtypeStruct((width, points), f32),
            jax.ShapeDtypeStruct((rows, width), f32),
        ),
        in_specs=[vmem_spec] * 2,
        out_specs=(hbm_spec, hbm_spec),
        scratch_shapes=[vmem((rows, width), f32), dma((2,))],
    )(*(
        pltpu.with_memory_space_constraint(value, pltpu.VMEM) for value in (current, terms)
    ))
    return current.T, predictions


def solution(mesh):
    both = ("wide", "narrow")
    placed = (
        P(both, None), P(both, None), P(both, None),
        P(both, None, None), P(both, None, None), P(), P(),
    )
    sizes = dict(mesh.shape)
    return jax.shard_map(
        functools.partial(body, sizes["wide"] * sizes["narrow"], sizes["narrow"]),
        mesh=mesh,
        in_specs=placed,
        out_specs=(P(both, None), P(both, None)),
        check_vma=False,
    )
```

```python
import functools
import math
import types

import jax
import jax.numpy as jnp
from jax import lax
from jax.experimental import pallas as pl
from jax.experimental.pallas import tpu as pltpu
from jax.sharding import PartitionSpec as P

LEVELS = 4
OCTET = 8
spread_coef = 3.0
MESH = pl.DeviceIdType.MESH
f32, bf16 = jnp.float32, jnp.bfloat16


def dot(a, b):
    return jnp.dot(a, b, preferred_element_type=f32)


def dot_nt(a, b):
    return lax.dot_general(a, b, (((1,), (1,)), ((), ())), preferred_element_type=f32)


def split(value):
    high = value.astype(bf16)
    return high, (value - high.astype(f32)).astype(bf16)


def halves_of(value):
    high = value.astype(bf16).astype(f32)
    return high, value - high


def far_first(size):
    return sorted(range(1, size), key=lambda k: -(k >> 1).bit_count())


def group_of(n_dev, level):
    node = n_dev >> (level - 1)
    size = min(OCTET, node)
    return size, node // size


def kernel(n_dev, narrow, names, *refs):
    r = types.SimpleNamespace(**dict(zip(names, refs)))
    pos = lax.axis_index("wide") * narrow + lax.axis_index("narrow")
    width, points = r.tgt.shape
    rank = r.right_h.shape[2]
    feat = r.train.shape[2]
    half = r.test_h.shape[1]
    rows = 2 * half
    pairs = n_dev // 2
    parity = pos % 2
    slot = pos // 2
    octets = n_dev // OCTET
    seat = slot % (OCTET // 2)
    own_block = seat * octets + slot // (OCTET // 2)
    own_rows = pl.ds(pl.multiple_of(own_block * half, half), half)
    seat_rows = pl.ds(pl.multiple_of(seat * octets * half, octets * half), octets * half)

    def coords(dev):
        return (dev // narrow, dev % narrow)

    def flip(mask):
        dev = pos
        for bit in range(mask.bit_length()):
            if mask >> bit & 1:
                dev = dev + (1 << bit) * (1 - 2 * ((pos // (1 << bit)) % 2))
        return coords(dev)

    def remote(src, dst, send_sem, recv_sem, where):
        pltpu.make_async_remote_copy(
            src_ref=src, dst_ref=dst, send_sem=send_sem, recv_sem=recv_sem,
            device_id=where, device_id_type=MESH,
        ).start()

    def drain(part, sem):
        pltpu.make_async_copy(part, part, sem).wait()

    def load(src, dst, sem):
        copy = pltpu.make_async_copy(src, dst, sem)
        copy.start()
        return copy

    barrier = pltpu.get_barrier_semaphore()

    def greet(k, carry):
        pl.semaphore_signal(
            barrier, inc=1, device_id=coords((pos + OCTET * k) % n_dev), device_id_type=MESH
        )
        return carry

    def side(i, count=1):
        return pl.ds(i * points, count * points)

    def load_side(i):
        source = (r.right_h, r.left_h)[i % 2].at[:, i // 2, :]
        load(source, r.side.at[side(i)], r.side_sem.at[(i + 1) // 2])

    tgt_load = load(r.tgt_h, r.tgt, r.load_sem.at[0])
    load_side(0)
    lax.fori_loop(1, octets, greet, 0)
    for k in range(1, OCTET):
        pl.semaphore_signal(barrier, inc=1, device_id=flip(k), device_id_type=MESH)
    test_load = load(r.test_h, r.gath.at[:, own_rows], r.load_sem.at[1])
    train_load = load(r.train_h, r.train.at[0], r.load_sem.at[2])
    for i in range(1, 2 * LEVELS):
        load_side(i)
    piv_load = load(r.piv_h, r.piv, r.load_sem.at[3])
    odds, heaps = [], []
    for level in range(1, LEVELS + 1):
        child = pos // (n_dev >> level)
        odds.append(child % 2)
        heaps.append((1 << level - 1) - 1 + child // 2)
        load(r.cap_h.at[heaps[-1]], r.cap.at[level - 1], r.load_sem.at[4])

    def first_send(level):
        size, _ = group_of(n_dev, level)
        mine = pos % size
        lev = level - 1
        for k in far_first(size):
            to = mine
            for bit in range(k.bit_length()):
                if k >> bit & 1:
                    to = to + (1 << bit) * (1 - 2 * ((mine // (1 << bit)) % 2))
            remote(
                getattr(r, f"send{level}").at[to], getattr(r, f"recv{level}").at[k],
                r.all_send, r.p1_recv.at[lev], flip(k),
            )

    def gram(level):
        lev = level - 1
        size, _ = group_of(n_dev, level)
        if level == 1:
            drain(r.side.at[side(0)], r.side_sem.at[0])
        high, low = split(r.side[side(2 * lev)])
        product = dot(r.stack[pl.ds(0, 2 * width + lev * rank)], high)
        t = product[:width] + product[width : 2 * width] + dot(r.stack[pl.ds(0, width)], low)
        t_high, t_low = halves_of(t)
        part = width // size
        both = jnp.concatenate(
            [t_high.reshape(size, part, rank), t_low.reshape(size, part, rank)], axis=1
        )
        send = getattr(r, f"send{level}")
        send[:, pl.ds(0, 2 * part)] = both.astype(bf16)
        cut = rank // size
        for k in range(lev):
            piece = product[2 * width + k * rank : 2 * width + (k + 1) * rank]
            send[:, pl.ds(2 * part + k * cut, cut)] = piece.astype(bf16).reshape(size, cut, rank)

    def turn(lev):
        drain(r.side.at[side(2 * lev + 1, min(2, 2 * LEVELS - 1 - 2 * lev))], r.side_sem.at[lev + 1])
        high, low = split(r.side[side(2 * lev + 1)].T)
        r.stack[pl.ds(2 * width + lev * rank, rank)] = high
        r.ltl[pl.ds(lev * rank, rank)] = low

    sums = {}

    def joined(value, level):
        part = width // group_of(n_dev, level)[0]
        top = value[:part] + value[part : 2 * part]
        return top if level == 1 else jnp.concatenate([top, value[2 * part :]], axis=0)

    def packed(value, level):
        part = width // group_of(n_dev, level)[0]
        high, low = halves_of(value[:part])
        pieces = [high, low] if level == 1 else [high, low, value[part:]]
        return jnp.concatenate(pieces, axis=0).astype(bf16)

    def first_take(level):
        size, count = group_of(n_dev, level)
        lev = level - 1
        recv, send = getattr(r, f"recv{level}"), getattr(r, f"send{level}")
        drain(recv.at[pl.ds(1, size - 1)], r.p1_recv.at[lev])
        near = send[pos % size].astype(f32)
        far = None
        for k in range(1, size):
            value = recv[k].astype(f32)
            if count > 1 or k < size // 2:
                near = near + value
            else:
                far = value if far is None else far + value
        near = joined(near, level)
        if count == 1:
            sums[level] = (near, joined(far, level))
            return
        sums[level] = (near, None)
        hop = getattr(r, f"hop{level}")
        hop[0] = packed(near, level)
        for j in range(count - 1, 0, -1):
            remote(hop.at[0], hop.at[j], r.all_send, r.p2_recv.at[lev], flip(j * OCTET))

    def second_take(level):
        size, count = group_of(n_dev, level)
        if count == 1:
            return
        hop = getattr(r, f"hop{level}")
        drain(hop.at[pl.ds(1, count - 1)], r.p2_recv.at[level - 1])
        near, far = sums[level][0], None
        for j in range(1, count):
            value = joined(hop[j].astype(f32), level)
            if j < count // 2:
                near = near + value
            else:
                far = value if far is None else far + value
        sums[level] = (near, far)

    def solve(level):
        size, count = group_of(n_dev, level)
        lev = level - 1
        near, far = sums[level]
        cols = near.shape[0]
        both = jnp.concatenate([near, far], axis=1)
        high, low = halves_of(both)
        moved = dot(jnp.concatenate([high, low], axis=0).astype(bf16), r.chosen[lev])
        odd = odds[lev]
        kids = 1 if count > 1 else 2
        taken = pl.ds(pl.multiple_of(odd * rank, rank), rank) if kids == 1 else pl.ds(0, 2 * rank)
        cap_high, cap_low = r.caps[0, lev, taken], r.caps[1, lev, taken]
        result = dot_nt(moved.astype(bf16), cap_high)
        result = result[:cols] + result[cols:] + dot_nt(moved[:cols].astype(bf16), cap_low)
        share, out = getattr(r, f"share{level}"), getattr(r, f"out{level}")
        for kid in range(kids):
            out[kid] = packed(result[:, kid * rank : (kid + 1) * rank], level)
        mine = pos % size
        for k in far_first(size):
            kid = 0 if kids == 1 else odd if k < size // 2 else 1 - odd
            remote(
                out.at[kid], share.at[mine], r.all_send, r.p3_recv.at[lev], flip(k)
            )
        share[mine] = out[0 if kids == 1 else odd]

    def gathered(level):
        size, _ = group_of(n_dev, level)
        share = getattr(r, f"share{level}")
        drain(share.at[pl.ds(0, size - 1)], r.p3_recv.at[level - 1])
        part, cut = width // size, rank // size
        top = share[:, pl.ds(0, 2 * part)].astype(f32)
        top = (top[:, :part] + top[:, part:]).reshape(width, rank)
        return [top] + [
            share[:, pl.ds(2 * part + k * cut, cut)].reshape(rank, rank) for k in range(level - 1)
        ]

    def prepare(lev):
        high, low = split(r.cap[lev])
        r.caps[0, lev] = high
        r.caps[1, lev] = low
        order = lax.broadcasted_iota(jnp.int32, (2 * rank, 2 * rank), 0)
        pivots = r.piv[pl.ds(heaps[lev], 1), :]
        at = pivots + rank * (1 - odds[lev])
        at = jnp.where(at >= 2 * rank, at - 2 * rank, at)
        r.chosen[lev] = (order == at).astype(f32).astype(bf16)

    def widened(value, own_squares_at, ones_at):
        value_f = value.astype(f32)
        high, low = split(value_f * value_f)
        squares = dot(
            jnp.concatenate([high, low], axis=1), jnp.ones((2 * feat, feat), bf16)
        )
        one = squares.astype(bf16).astype(f32)
        two = (squares - one).astype(bf16).astype(f32)
        three = squares - one - two
        lane = lax.broadcasted_iota(jnp.int32, squares.shape, 1)
        extra = jnp.where((lane >= ones_at) & (lane < ones_at + 3), 1.0, 0.0)
        for i, piece in enumerate((one, two, three)):
            extra = jnp.where(lane == own_squares_at + i, -piece, extra)
        return extra.astype(bf16)

    def widen_train(which):
        value = r.train[which]
        r.train_w[which, :, pl.ds(0, feat)] = value + value
        r.train_w[which, :, pl.ds(feat, feat)] = widened(value, 3, 0)

    def widen_tests():
        def step(i, carry):
            part = pl.ds(pl.multiple_of(i * wide_rows, wide_rows), wide_rows)
            for h in range(2):
                value = r.gath[h, part]
                there = pl.ds(
                    pl.multiple_of(h * pairs * half + i * wide_rows, wide_rows), wide_rows
                )
                r.test_w[there, pl.ds(0, feat)] = value
                r.test_w[there, pl.ds(feat, feat)] = widened(value, 0, 3)
            return carry

        wide_rows = min(256, pairs * half)
        lax.fori_loop(0, pairs * half // wide_rows, step, 0)

    rate = spread_coef / feat * math.log2(math.e)
    chunk = min(512, pairs * rows)

    def fill(which):
        def step(i, carry):
            part = pl.ds(pl.multiple_of(i * chunk, chunk), chunk)
            negative = dot_nt(r.test_w[part], r.train_w[which])
            r.kmat[part, pl.ds(which * points, points)] = jnp.exp2(rate * negative).astype(bf16)
            return carry

        lax.fori_loop(0, pairs * rows // chunk, step, 0)

    tgt_load.wait()
    high, low = split(r.tgt[...])
    r.stack[pl.ds(0, width)] = high
    r.stack[pl.ds(width, width)] = low
    gram(1)
    test_load.wait()
    pl.semaphore_wait(barrier, octets - 1 + OCTET - 1)
    first_send(1)
    own_test = r.gath.at[:, own_rows]

    def spread(k, carry):
        remote(own_test, own_test, r.all_send, r.ag_recv, coords((pos + OCTET * k) % n_dev))
        return carry

    lax.fori_loop(1, octets, spread, 0)
    turn(0)
    gram(2)
    first_send(2)
    train_load.wait()
    remote(r.train.at[0], r.train.at[1], r.all_send, r.tr_recv, flip(1))
    turn(1)
    gram(3)
    first_send(3)
    turn(2)
    gram(4)
    first_send(4)
    widen_train(0)
    piv_load.wait()
    drain(r.cap, r.load_sem.at[4])
    for lev in range(LEVELS):
        prepare(lev)
    first_take(1)
    first_take(2)
    drain(r.gath.at[:, pl.ds(0, (octets - 1) * half)], r.ag_recv)
    seat_test = r.gath.at[:, seat_rows]
    for k in range(2, OCTET, 2):
        remote(seat_test, seat_test, r.all_send, r.fw_recv, flip(k))
    first_take(3)
    if group_of(n_dev, 3)[1] == 1:
        solve(3)
    first_take(4)
    if group_of(n_dev, 4)[1] == 1:
        solve(4)
    drain(r.train.at[0], r.tr_recv)
    widen_train(1)
    turn(LEVELS - 1)
    for level in (4, 3, 2, 1):
        if group_of(n_dev, level)[1] > 1:
            second_take(level)
            solve(level)
    drain(r.gath.at[:, pl.ds(0, (OCTET // 2 - 1) * octets * half)], r.fw_recv)
    widen_tests()
    fill(0)
    fill(1)

    third, fourth = gathered(3), gathered(4)
    high, low = split(third[0])
    product = dot(jnp.concatenate([high, low, third[1], third[2]], axis=0), fourth[3])
    r.base[:, pl.ds(0, rank)] = third[0]
    r.base[:, pl.ds(rank, rank)] = fourth[0] - (product[:width] + product[width : 2 * width])
    for k in range(2):
        there = pl.ds(k * rank, rank)
        r.mix[there, pl.ds(0, rank)] = third[1 + k]
        at = 2 * width + k * rank
        high, low = split(fourth[1 + k].astype(f32) - product[at : at + rank])
        r.mix[there, pl.ds(rank, rank)] = high
        r.mix_low[there] = low
    base_high, base_low = split(r.base[...])
    mixed = jnp.concatenate([base_high, base_low, r.mix[...]], axis=0)
    mixed_high = jnp.concatenate([base_high, r.mix[...]], axis=0)
    wide = min(512, points)
    for i in range(points // wide):
        cut = pl.ds(i * wide, wide)
        top = dot(mixed, r.stack[pl.ds(2 * width + 2 * rank, 2 * rank), cut])
        bottom = dot(mixed_high, r.ltl[pl.ds(2 * rank, 2 * rank), cut])
        r.cur0[:, cut] = r.tgt[:, cut] - (top[:width] + top[width : 2 * width] + bottom[:width])
        rest = dot(r.mix_low[...], r.stack[pl.ds(2 * width + 3 * rank, rank), cut])
        own = r.stack[pl.ds(2 * width, 2 * rank), cut].astype(f32)
        own = own + r.ltl[pl.ds(0, 2 * rank), cut].astype(f32)
        high, low = split(own - (top[2 * width :] + bottom[width:] + rest))
        r.leff[0, :, cut] = high
        r.leff[1, :, cut] = low
    second = gathered(2)
    first = gathered(1)[0]
    high, low = split(first)
    product = dot(jnp.concatenate([high, low], axis=0), second[1])
    upper = jnp.concatenate([first, second[0] - (product[:width] + product[width:])], axis=1)
    high, low = split(upper)
    product = dot(jnp.concatenate([high, low], axis=0), r.leff[0])
    current = r.cur0[...] - (product[:width] + product[width:] + dot(high, r.leff[1]))
    r.cur[...] = current
    weights = current.astype(bf16)
    for h in range(2):
        r.wt[0, h] = weights[:, h * (points // 2) : (h + 1) * (points // 2)]
    for h in range(2):
        remote(r.wt.at[0, h], r.wt.at[1, h], r.all_send, r.wt_recv.at[h], flip(1))
    cur_copy = pltpu.make_async_copy(r.cur, r.cur_out, r.out_sem)
    cur_copy.start()

    big = min(256, pairs * half)

    def weigh(which, h):
        twice = jnp.concatenate([r.wt[which, h], r.wt[which, h]], axis=0)
        first_half = lax.broadcasted_iota(jnp.int32, (big, 2 * width), 1) < width

        def step(i, carry):
            part = pl.ds(pl.multiple_of(i * big, big), big)
            other = pl.ds(pl.multiple_of(pairs * half + i * big, big), big)
            there = pl.ds((2 * which + h) * (points // 2), points // 2)
            value = jnp.where(
                first_half, dot_nt(r.kmat[part, there], twice), dot_nt(r.kmat[other, there], twice)
            )
            if which or h:
                value = r.terms[part] + value
            if which and h:
                r.term_b[part] = value.astype(bf16)
            else:
                r.terms[part] = value
            return carry

        lax.fori_loop(0, pairs * half // big, step, 0)

    for which in range(2):
        for h in range(2):
            if which:
                drain(r.wt.at[1, h], r.wt_recv.at[h])
            weigh(which, h)

    own_copy = pltpu.make_async_copy(
        r.term_b.at[own_rows], r.term_out.at[pl.ds((pairs - 1) * half, half)], r.own_sem
    )
    own_copy.start()
    for turned in (3, 2, 1, 0):
        base = pos
        for bit in range(2):
            if turned >> bit & 1:
                base = base + (2 << bit) * (1 - 2 * ((pos // (2 << bit)) % 2))

        def scatter(j, carry, base=base, turned=turned):
            to = (base + OCTET * j) % n_dev
            block = ((to // 2) % (OCTET // 2)) * octets + to // OCTET
            remote(
                r.term_b.at[pl.ds(pl.multiple_of(block * half, half), half)],
                r.term_out.at[pl.ds(pl.multiple_of((turned * octets + j - 1) * half, half), half)],
                r.all_send, r.rs_recv, coords(to),
            )
            return carry

        start = 0 if turned else 1
        if octets <= 4:
            for j in range(start, octets):
                scatter(j, 0)
        else:
            lax.fori_loop(start, octets, scatter, 0)
    cur_copy.wait()
    own_copy.wait()
    landed = r.term_out.at[pl.ds(0, (pairs - 1) * half)]
    drain(landed, r.rs_recv)
    sent = 2 * points * feat + 2 * width * points
    sent += 2 * 2 * half * feat * (octets - 1 + (OCTET // 2 - 1) * octets) + 2 * (pairs - 1) * half * 2 * width
    for level in range(1, LEVELS + 1):
        size, count = group_of(n_dev, level)
        piece = 2 * getattr(r, f"send{level}").shape[1] * rank
        sent += piece * (2 * (size - 1) + count - 1)
    drain(r.side.at[pl.ds(0, sent // (4 * rank))], r.all_send)


def finish(cur_in, terms_in, cur_out, pred_out, pred, sems):
    parts = sems.shape[0] - 1
    tall = cur_in.shape[0] // parts
    copies = [
        pltpu.make_async_copy(
            cur_in.at[pl.ds(i * tall, tall)], cur_out.at[pl.ds(i * tall, tall)], sems.at[i]
        )
        for i in range(parts)
    ]
    for copy in copies:
        copy.start()
    half, width = pred.shape[0] // 2, pred.shape[1]
    terms = terms_in[...].astype(f32)
    total = jnp.sum(terms.reshape(terms.shape[0] // half, half, 2 * width), axis=0)
    pred[pl.ds(0, half)] = total[:, :width]
    pred[pl.ds(half, half)] = total[:, width:]
    copies.append(pltpu.make_async_copy(pred, pred_out, sems.at[parts]))
    copies[-1].start()
    for copy in copies:
        copy.wait()


def body(n_dev, narrow, targets, train, test, left, right, cap, pivots):
    points, width = targets.shape
    rank = left.shape[2]
    feat = train.shape[1]
    rows = test.shape[0]
    half = rows // 2
    pairs = n_dev // 2
    vmem = pltpu.VMEM
    dma = pltpu.SemaphoreType.DMA
    hbm_spec = pl.BlockSpec(memory_space=pl.ANY)
    vmem_spec = pl.BlockSpec(memory_space=pltpu.VMEM)
    scratch = {
        "tgt": vmem((width, points), f32),
        "piv": vmem(pivots.shape, jnp.int32),
        "train": vmem((2, points, feat), bf16),
        "gath": vmem((2, pairs * half, feat), bf16),
        "side": vmem((2 * LEVELS * points, rank), f32),
        "cur0": vmem((width, points), f32),
        "leff": vmem((2, 2 * rank, points), bf16),
        "cap": vmem((LEVELS, 2 * rank, 2 * rank), f32),
        "caps": vmem((2, LEVELS, 2 * rank, 2 * rank), bf16),
        "chosen": vmem((LEVELS, 2 * rank, 2 * rank), bf16),
        "stack": vmem((2 * width + LEVELS * rank, points), bf16),
        "ltl": vmem((LEVELS * rank, points), bf16),
        "train_w": vmem((2, points, 2 * feat), bf16),
        "test_w": vmem((pairs * rows, 2 * feat), bf16),
        "kmat": vmem((pairs * rows, 2 * points), bf16),
        "base": vmem((width, 2 * rank), f32),
        "mix": vmem((2 * rank, 2 * rank), bf16),
        "mix_low": vmem((2 * rank, rank), bf16),
        "cur": vmem((width, points), f32),
        "wt": vmem((2, 2, width, points // 2), bf16),
        "terms": vmem((pairs * half, 2 * width), f32),
        "term_b": vmem((pairs * half, 2 * width), bf16),
    }
    for level in range(1, LEVELS + 1):
        size, count = group_of(n_dev, level)
        tall = (2 * width + (level - 1) * rank) // size
        for name in ("send", "recv", "share"):
            scratch[f"{name}{level}"] = vmem((size, tall, rank), bf16)
        scratch[f"out{level}"] = vmem((2, tall, rank), bf16)
        if count > 1:
            scratch[f"hop{level}"] = vmem((count, tall, rank), bf16)
    scratch["load_sem"] = dma((5,))
    scratch["side_sem"] = dma((LEVELS + 1,))
    scratch["wt_recv"] = dma((2,))
    scratch["p1_recv"] = dma((LEVELS,))
    scratch["p2_recv"] = dma((sum(group_of(n_dev, i + 1)[1] > 1 for i in range(LEVELS)),))
    scratch["p3_recv"] = dma((LEVELS,))
    for name in (
        "all_send", "ag_recv", "fw_recv", "tr_recv", "rs_recv", "out_sem", "own_sem",
    ):
        scratch[name] = dma
    names = ["tgt_h", "train_h", "test_h", "left_h", "right_h", "cap_h", "piv_h"]
    names += ["cur_out", "term_out"] + list(scratch)
    current, terms = pl.pallas_call(
        functools.partial(kernel, n_dev, narrow, names),
        out_shape=(
            jax.ShapeDtypeStruct((width, points), f32),
            jax.ShapeDtypeStruct((pairs * half, 2 * width), bf16),
        ),
        in_specs=[pl.BlockSpec(memory_space=pltpu.HBM)] * 7,
        out_specs=(hbm_spec, hbm_spec),
        scratch_shapes=list(scratch.values()),
        compiler_params=pltpu.CompilerParams(
            collective_id=0, has_side_effects=True, vmem_limit_bytes=48 * 1024 * 1024
        ),
    )(*(
        pltpu.with_memory_space_constraint(value, pltpu.HBM)
        for value in (
            targets.T, train, test.reshape(2, half, feat), left, right, cap, pivots
        )
    ))
    current, predictions = pl.pallas_call(
        finish,
        out_shape=(
            jax.ShapeDtypeStruct((width, points), f32),
            jax.ShapeDtypeStruct((rows, width), f32),
        ),
        in_specs=[vmem_spec] * 2,
        out_specs=(hbm_spec, hbm_spec),
        scratch_shapes=[vmem((rows, width), f32), dma((5,))],
    )(*(
        pltpu.with_memory_space_constraint(value, pltpu.VMEM) for value in (current, terms)
    ))
    return current.T, predictions


def solution(mesh):
    both = ("wide", "narrow")
    placed = (
        P(both, None), P(both, None), P(both, None),
        P(both, None, None), P(both, None, None), P(), P(),
    )
    sizes = dict(mesh.shape)
    return jax.shard_map(
        functools.partial(body, sizes["wide"] * sizes["narrow"], sizes["narrow"]),
        mesh=mesh,
        in_specs=placed,
        out_specs=(P(both, None), P(both, None)),
        check_vma=False,
    )
```

```python
import functools
import math
import types

import jax
import jax.numpy as jnp
from jax import lax
from jax.experimental import pallas as pl
from jax.experimental.pallas import tpu as pltpu
from jax.sharding import PartitionSpec as P

LEVELS = 4
OCTET = 8
spread_coef = 3.0
MESH = pl.DeviceIdType.MESH
f32, bf16 = jnp.float32, jnp.bfloat16


def dot(a, b):
    return jnp.dot(a, b, preferred_element_type=f32)


def dot_nt(a, b):
    return lax.dot_general(a, b, (((1,), (1,)), ((), ())), preferred_element_type=f32)


def split(value):
    high = value.astype(bf16)
    return high, (value - high.astype(f32)).astype(bf16)


def halves_of(value):
    high = value.astype(bf16).astype(f32)
    return high, value - high


def far_first(size):
    return sorted(range(1, size), key=lambda k: -(k >> 1).bit_count())


def group_of(n_dev, level):
    node = n_dev >> (level - 1)
    size = min(OCTET, node)
    return size, node // size


def kernel(n_dev, narrow, names, *refs):
    r = types.SimpleNamespace(**dict(zip(names, refs)))
    pos = lax.axis_index("wide") * narrow + lax.axis_index("narrow")
    width, points = r.tgt.shape
    rank = r.right_h.shape[2]
    feat = r.train.shape[2]
    half = r.test_h.shape[1]
    rows = 2 * half
    pairs = n_dev // 2
    parity = pos % 2
    slot = pos // 2
    octets = n_dev // OCTET
    seat = slot % (OCTET // 2)
    own_block = seat * octets + slot // (OCTET // 2)
    own_rows = pl.ds(pl.multiple_of(own_block * half, half), half)
    seat_rows = pl.ds(pl.multiple_of(seat * octets * half, octets * half), octets * half)

    def coords(dev):
        return (dev // narrow, dev % narrow)

    def flip(mask):
        dev = pos
        for bit in range(mask.bit_length()):
            if mask >> bit & 1:
                dev = dev + (1 << bit) * (1 - 2 * ((pos // (1 << bit)) % 2))
        return coords(dev)

    def remote(src, dst, send_sem, recv_sem, where):
        pltpu.make_async_remote_copy(
            src_ref=src, dst_ref=dst, send_sem=send_sem, recv_sem=recv_sem,
            device_id=where, device_id_type=MESH,
        ).start()

    def drain(part, sem):
        pltpu.make_async_copy(part, part, sem).wait()

    def load(src, dst, sem):
        copy = pltpu.make_async_copy(src, dst, sem)
        copy.start()
        return copy

    barrier = pltpu.get_barrier_semaphore()

    def greet(k, carry):
        pl.semaphore_signal(
            barrier, inc=1, device_id=coords((pos + OCTET * k) % n_dev), device_id_type=MESH
        )
        return carry

    def side(i, count=1):
        return pl.ds(i * points, count * points)

    def load_side(i):
        source = (r.right_h, r.left_h)[i % 2].at[:, i // 2, :]
        load(source, r.side.at[side(i)], r.side_sem.at[(i + 1) // 2])

    tgt_load = load(r.tgt_h, r.tgt, r.load_sem.at[0])
    load_side(0)
    lax.fori_loop(1, octets, greet, 0)
    for k in range(1, OCTET):
        pl.semaphore_signal(barrier, inc=1, device_id=flip(k), device_id_type=MESH)
    test_load = load(r.test_h, r.gath.at[:, own_rows], r.load_sem.at[1])
    for i in range(1, 2 * LEVELS):
        load_side(i)
        if i == 2:
            train_load = load(r.train_h, r.train.at[0], r.load_sem.at[2])
    piv_load = load(r.piv_h, r.piv, r.load_sem.at[3])
    odds, heaps = [], []
    for level in range(1, LEVELS + 1):
        child = pos // (n_dev >> level)
        odds.append(child % 2)
        heaps.append((1 << level - 1) - 1 + child // 2)
        load(r.cap_h.at[heaps[-1]], r.cap.at[level - 1], r.load_sem.at[4])

    def first_send(level):
        size, _ = group_of(n_dev, level)
        mine = pos % size
        lev = level - 1
        for k in far_first(size):
            to = mine
            for bit in range(k.bit_length()):
                if k >> bit & 1:
                    to = to + (1 << bit) * (1 - 2 * ((mine // (1 << bit)) % 2))
            remote(
                getattr(r, f"send{level}").at[to], getattr(r, f"recv{level}").at[k],
                r.all_send, r.p1_recv.at[lev], flip(k),
            )

    def gram(level):
        lev = level - 1
        size, _ = group_of(n_dev, level)
        if level == 1:
            drain(r.side.at[side(0)], r.side_sem.at[0])
        high, low = split(r.side[side(2 * lev)])
        product = dot(r.stack[pl.ds(0, 2 * width + lev * rank)], high)
        t = product[:width] + product[width : 2 * width] + dot(r.stack[pl.ds(0, width)], low)
        t_high, t_low = halves_of(t)
        part = width // size
        both = jnp.concatenate(
            [t_high.reshape(size, part, rank), t_low.reshape(size, part, rank)], axis=1
        )
        send = getattr(r, f"send{level}")
        send[:, pl.ds(0, 2 * part)] = both.astype(bf16)
        cut = rank // size
        for k in range(lev):
            piece = product[2 * width + k * rank : 2 * width + (k + 1) * rank]
            send[:, pl.ds(2 * part + k * cut, cut)] = piece.astype(bf16).reshape(size, cut, rank)

    def turn(lev):
        drain(r.side.at[side(2 * lev + 1, min(2, 2 * LEVELS - 1 - 2 * lev))], r.side_sem.at[lev + 1])
        high, low = split(r.side[side(2 * lev + 1)].T)
        r.stack[pl.ds(2 * width + lev * rank, rank)] = high
        r.ltl[pl.ds(lev * rank, rank)] = low

    sums = {}

    def joined(value, level):
        part = width // group_of(n_dev, level)[0]
        top = value[:part] + value[part : 2 * part]
        return top if level == 1 else jnp.concatenate([top, value[2 * part :]], axis=0)

    def packed(value, level):
        part = width // group_of(n_dev, level)[0]
        high, low = halves_of(value[:part])
        pieces = [high, low] if level == 1 else [high, low, value[part:]]
        return jnp.concatenate(pieces, axis=0).astype(bf16)

    def first_take(level):
        size, count = group_of(n_dev, level)
        lev = level - 1
        recv, send = getattr(r, f"recv{level}"), getattr(r, f"send{level}")
        drain(recv.at[pl.ds(1, size - 1)], r.p1_recv.at[lev])
        near = send[pos % size].astype(f32)
        far = None
        for k in range(1, size):
            value = recv[k].astype(f32)
            if count > 1 or k < size // 2:
                near = near + value
            else:
                far = value if far is None else far + value
        near = joined(near, level)
        if count == 1:
            sums[level] = (near, joined(far, level))
            return
        sums[level] = (near, None)
        hop = getattr(r, f"hop{level}")
        hop[0] = packed(near, level)
        for j in range(count - 1, 0, -1):
            remote(hop.at[0], hop.at[j], r.all_send, r.p2_recv.at[lev], flip(j * OCTET))

    def second_take(level):
        size, count = group_of(n_dev, level)
        if count == 1:
            return
        hop = getattr(r, f"hop{level}")
        drain(hop.at[pl.ds(1, count - 1)], r.p2_recv.at[level - 1])
        near, far = sums[level][0], None
        for j in range(1, count):
            value = joined(hop[j].astype(f32), level)
            if j < count // 2:
                near = near + value
            else:
                far = value if far is None else far + value
        sums[level] = (near, far)

    def solved(level):
        _, count = group_of(n_dev, level)
        lev = level - 1
        near, far = sums[level]
        cols = near.shape[0]
        both = jnp.concatenate([near, far], axis=1)
        high, low = halves_of(both)
        moved = dot(jnp.concatenate([high, low], axis=0).astype(bf16), r.chosen[lev])
        odd = odds[lev]
        kids = 1 if count > 1 else 2
        taken = pl.ds(pl.multiple_of(odd * rank, rank), rank) if kids == 1 else pl.ds(0, 2 * rank)
        cap_high, cap_low = r.caps[0, lev, taken], r.caps[1, lev, taken]
        result = dot_nt(moved.astype(bf16), cap_high)
        return result[:cols] + result[cols:] + dot_nt(moved[:cols].astype(bf16), cap_low)

    def give(level, result):
        size, count = group_of(n_dev, level)
        lev = level - 1
        odd = odds[lev]
        kids = 1 if count > 1 else 2
        share, out = getattr(r, f"share{level}"), getattr(r, f"out{level}")
        for kid in range(kids):
            out[kid] = packed(result[:, kid * rank : (kid + 1) * rank], level)
        mine = pos % size
        for k in far_first(size):
            kid = 0 if kids == 1 else odd if k < size // 2 else 1 - odd
            remote(
                out.at[kid], share.at[mine], r.all_send, r.p3_recv.at[lev], flip(k)
            )
        share[mine] = out[0 if kids == 1 else odd]

    def gathered(level):
        size, _ = group_of(n_dev, level)
        share = getattr(r, f"share{level}")
        drain(share.at[pl.ds(0, size - 1)], r.p3_recv.at[level - 1])
        part, cut = width // size, rank // size
        top = share[:, pl.ds(0, 2 * part)].astype(f32)
        top = (top[:, :part] + top[:, part:]).reshape(width, rank)
        return [top] + [
            share[:, pl.ds(2 * part + k * cut, cut)].reshape(rank, rank) for k in range(level - 1)
        ]

    def prepare(lev):
        high, low = split(r.cap[lev])
        r.caps[0, lev] = high
        r.caps[1, lev] = low
        order = lax.broadcasted_iota(jnp.int32, (2 * rank, 2 * rank), 0)
        pivots = r.piv[pl.ds(heaps[lev], 1), :]
        at = pivots + rank * (1 - odds[lev])
        at = jnp.where(at >= 2 * rank, at - 2 * rank, at)
        r.chosen[lev] = (order == at).astype(f32).astype(bf16)

    def widened(value, own_squares_at, ones_at):
        value_f = value.astype(f32)
        high, low = split(value_f * value_f)
        squares = dot(
            jnp.concatenate([high, low], axis=1), jnp.ones((2 * feat, feat), bf16)
        )
        one = squares.astype(bf16).astype(f32)
        two = (squares - one).astype(bf16).astype(f32)
        three = squares - one - two
        lane = lax.broadcasted_iota(jnp.int32, squares.shape, 1)
        extra = jnp.where((lane >= ones_at) & (lane < ones_at + 3), 1.0, 0.0)
        for i, piece in enumerate((one, two, three)):
            extra = jnp.where(lane == own_squares_at + i, -piece, extra)
        return extra.astype(bf16)

    def widen_train(which):
        value = r.train[which]
        r.train_w[which, :, pl.ds(0, feat)] = value + value
        r.train_w[which, :, pl.ds(feat, feat)] = widened(value, 3, 0)

    def widen_tests():
        def step(i, carry):
            part = pl.ds(pl.multiple_of(i * wide_rows, wide_rows), wide_rows)
            for h in range(2):
                value = r.gath[h, part]
                there = pl.ds(
                    pl.multiple_of(h * pairs * half + i * wide_rows, wide_rows), wide_rows
                )
                r.test_w[there, pl.ds(0, feat)] = value
                r.test_w[there, pl.ds(feat, feat)] = widened(value, 0, 3)
            return carry

        wide_rows = min(256, pairs * half)
        lax.fori_loop(0, pairs * half // wide_rows, step, 0)

    rate = spread_coef / feat * math.log2(math.e)
    chunk = min(512, pairs * rows)

    def fill(which):
        def step(i, carry):
            part = pl.ds(pl.multiple_of(i * chunk, chunk), chunk)
            negative = dot_nt(r.test_w[part], r.train_w[which])
            r.kmat[part, pl.ds(which * points, points)] = jnp.exp2(rate * negative).astype(bf16)
            return carry

        lax.fori_loop(0, pairs * rows // chunk, step, 0)

    tgt_load.wait()
    high, low = split(r.tgt[...])
    r.stack[pl.ds(0, width)] = high
    r.stack[pl.ds(width, width)] = low
    gram(1)
    turn(0)
    test_load.wait()
    pl.semaphore_wait(barrier, octets - 1 + OCTET - 1)
    first_send(1)
    own_test = r.gath.at[:, own_rows]

    def spread(k, carry):
        remote(own_test, own_test, r.all_send, r.ag_recv, coords((pos + OCTET * k) % n_dev))
        return carry

    lax.fori_loop(1, octets, spread, 0)
    gram(2)
    first_send(2)
    train_load.wait()
    remote(r.train.at[0], r.train.at[1], r.all_send, r.tr_recv, flip(1))
    turn(1)
    gram(3)
    first_send(3)
    turn(2)
    gram(4)
    first_send(4)
    widen_train(0)
    piv_load.wait()
    drain(r.cap, r.load_sem.at[4])
    for lev in range(LEVELS):
        prepare(lev)
    first_take(1)
    drain(r.gath.at[:, pl.ds(0, (octets - 1) * half)], r.ag_recv)
    seat_test = r.gath.at[:, seat_rows]
    for k in range(2, OCTET, 2):
        remote(seat_test, seat_test, r.all_send, r.fw_recv, flip(k))
    first_take(2)
    first_take(3)
    if group_of(n_dev, 3)[1] == 1:
        give(3, solved(3))
    first_take(4)
    if group_of(n_dev, 4)[1] == 1:
        give(4, solved(4))
    late = [level for level in range(1, LEVELS + 1) if group_of(n_dev, level)[1] > 1]
    for level in late:
        second_take(level)
    results = [solved(level) for level in late]
    for level, result in zip(late, results):
        give(level, result)
    drain(r.train.at[0], r.tr_recv)
    widen_train(1)
    turn(LEVELS - 1)
    drain(r.gath.at[:, pl.ds(0, (OCTET // 2 - 1) * octets * half)], r.fw_recv)
    widen_tests()
    fill(0)
    fill(1)

    third, fourth = gathered(3), gathered(4)
    high, low = split(third[0])
    product = dot(jnp.concatenate([high, low, third[1], third[2]], axis=0), fourth[3])
    r.base[:, pl.ds(0, rank)] = third[0]
    r.base[:, pl.ds(rank, rank)] = fourth[0] - (product[:width] + product[width : 2 * width])
    for k in range(2):
        there = pl.ds(k * rank, rank)
        r.mix[there, pl.ds(0, rank)] = third[1 + k]
        at = 2 * width + k * rank
        high, low = split(fourth[1 + k].astype(f32) - product[at : at + rank])
        r.mix[there, pl.ds(rank, rank)] = high
        r.mix_low[there] = low
    base_high, base_low = split(r.base[...])
    mixed = jnp.concatenate([base_high, base_low, r.mix[...]], axis=0)
    mixed_high = jnp.concatenate([base_high, r.mix[...]], axis=0)
    wide = min(512, points)
    for i in range(points // wide):
        cut = pl.ds(i * wide, wide)
        top = dot(mixed, r.stack[pl.ds(2 * width + 2 * rank, 2 * rank), cut])
        bottom = dot(mixed_high, r.ltl[pl.ds(2 * rank, 2 * rank), cut])
        r.cur0[:, cut] = r.tgt[:, cut] - (top[:width] + top[width : 2 * width] + bottom[:width])
        rest = dot(r.mix_low[...], r.stack[pl.ds(2 * width + 3 * rank, rank), cut])
        own = r.stack[pl.ds(2 * width, 2 * rank), cut].astype(f32)
        own = own + r.ltl[pl.ds(0, 2 * rank), cut].astype(f32)
        high, low = split(own - (top[2 * width :] + bottom[width:] + rest))
        r.leff[0, :, cut] = high
        r.leff[1, :, cut] = low
    second = gathered(2)
    first = gathered(1)[0]
    high, low = split(first)
    product = dot(jnp.concatenate([high, low], axis=0), second[1])
    upper = jnp.concatenate([first, second[0] - (product[:width] + product[width:])], axis=1)
    high, low = split(upper)
    both = jnp.concatenate([high, low], axis=0)
    for h in range(2):
        cut = pl.ds(h * (points // 2), points // 2)
        product = dot(both, r.leff[0, :, cut])
        current = r.cur0[:, cut] - (product[:width] + product[width:] + dot(high, r.leff[1, :, cut]))
        r.cur[:, cut] = current
        r.wt[0, h] = current.astype(bf16)
        remote(r.wt.at[0, h], r.wt.at[1, h], r.all_send, r.wt_recv.at[h], flip(1))
    cur_copy = pltpu.make_async_copy(r.cur, r.cur_out, r.out_sem)
    cur_copy.start()

    big = min(256, pairs * half)

    def weigh(which, h):
        twice = jnp.concatenate([r.wt[which, h], r.wt[which, h]], axis=0)
        first_half = lax.broadcasted_iota(jnp.int32, (big, 2 * width), 1) < width

        def step(i, carry):
            part = pl.ds(pl.multiple_of(i * big, big), big)
            other = pl.ds(pl.multiple_of(pairs * half + i * big, big), big)
            there = pl.ds((2 * which + h) * (points // 2), points // 2)
            value = jnp.where(
                first_half, dot_nt(r.kmat[part, there], twice), dot_nt(r.kmat[other, there], twice)
            )
            if which or h:
                value = r.terms[part] + value
            if which and h:
                r.term_b[part] = value.astype(bf16)
            else:
                r.terms[part] = value
            return carry

        lax.fori_loop(0, pairs * half // big, step, 0)

    for which in range(2):
        for h in range(2):
            if which:
                drain(r.wt.at[1, h], r.wt_recv.at[h])
            weigh(which, h)

    own_copy = pltpu.make_async_copy(
        r.term_b.at[own_rows], r.term_out.at[pl.ds((pairs - 1) * half, half)], r.own_sem
    )
    own_copy.start()
    for turned in (3, 2, 1, 0):
        base = pos
        for bit in range(2):
            if turned >> bit & 1:
                base = base + (2 << bit) * (1 - 2 * ((pos // (2 << bit)) % 2))

        def scatter(j, carry, base=base, turned=turned):
            to = (base + OCTET * j) % n_dev
            block = ((to // 2) % (OCTET // 2)) * octets + to // OCTET
            remote(
                r.term_b.at[pl.ds(pl.multiple_of(block * half, half), half)],
                r.term_out.at[pl.ds(pl.multiple_of((turned * octets + j - 1) * half, half), half)],
                r.all_send, r.rs_recv, coords(to),
            )
            return carry

        start = 0 if turned else 1
        if octets <= 4:
            for j in range(start, octets):
                scatter(j, 0)
        else:
            lax.fori_loop(start, octets, scatter, 0)
    cur_copy.wait()
    own_copy.wait()
    landed = r.term_out.at[pl.ds(0, (pairs - 1) * half)]
    drain(landed, r.rs_recv)
    sent = 2 * points * feat + 2 * width * points
    sent += 2 * 2 * half * feat * (octets - 1 + (OCTET // 2 - 1) * octets) + 2 * (pairs - 1) * half * 2 * width
    for level in range(1, LEVELS + 1):
        size, count = group_of(n_dev, level)
        piece = 2 * getattr(r, f"send{level}").shape[1] * rank
        sent += piece * (2 * (size - 1) + count - 1)
    drain(r.side.at[pl.ds(0, sent // (4 * rank))], r.all_send)


def finish(cur_in, terms_in, cur_out, pred_out, pred, sems):
    parts = sems.shape[0] - 1
    tall = cur_in.shape[0] // parts
    copies = [
        pltpu.make_async_copy(
            cur_in.at[pl.ds(i * tall, tall)], cur_out.at[pl.ds(i * tall, tall)], sems.at[i]
        )
        for i in range(parts)
    ]
    for copy in copies:
        copy.start()
    half, width = pred.shape[0] // 2, pred.shape[1]
    terms = terms_in[...].astype(f32)
    total = jnp.sum(terms.reshape(terms.shape[0] // half, half, 2 * width), axis=0)
    pred[pl.ds(0, half)] = total[:, :width]
    pred[pl.ds(half, half)] = total[:, width:]
    copies.append(pltpu.make_async_copy(pred, pred_out, sems.at[parts]))
    copies[-1].start()
    for copy in copies:
        copy.wait()


def body(n_dev, narrow, targets, train, test, left, right, cap, pivots):
    points, width = targets.shape
    rank = left.shape[2]
    feat = train.shape[1]
    rows = test.shape[0]
    half = rows // 2
    pairs = n_dev // 2
    vmem = pltpu.VMEM
    dma = pltpu.SemaphoreType.DMA
    hbm_spec = pl.BlockSpec(memory_space=pl.ANY)
    vmem_spec = pl.BlockSpec(memory_space=pltpu.VMEM)
    scratch = {
        "tgt": vmem((width, points), f32),
        "piv": vmem(pivots.shape, jnp.int32),
        "train": vmem((2, points, feat), bf16),
        "gath": vmem((2, pairs * half, feat), bf16),
        "side": vmem((2 * LEVELS * points, rank), f32),
        "cur0": vmem((width, points), f32),
        "leff": vmem((2, 2 * rank, points), bf16),
        "cap": vmem((LEVELS, 2 * rank, 2 * rank), f32),
        "caps": vmem((2, LEVELS, 2 * rank, 2 * rank), bf16),
        "chosen": vmem((LEVELS, 2 * rank, 2 * rank), bf16),
        "stack": vmem((2 * width + LEVELS * rank, points), bf16),
        "ltl": vmem((LEVELS * rank, points), bf16),
        "train_w": vmem((2, points, 2 * feat), bf16),
        "test_w": vmem((pairs * rows, 2 * feat), bf16),
        "kmat": vmem((pairs * rows, 2 * points), bf16),
        "base": vmem((width, 2 * rank), f32),
        "mix": vmem((2 * rank, 2 * rank), bf16),
        "mix_low": vmem((2 * rank, rank), bf16),
        "cur": vmem((width, points), f32),
        "wt": vmem((2, 2, width, points // 2), bf16),
        "terms": vmem((pairs * half, 2 * width), f32),
        "term_b": vmem((pairs * half, 2 * width), bf16),
    }
    for level in range(1, LEVELS + 1):
        size, count = group_of(n_dev, level)
        tall = (2 * width + (level - 1) * rank) // size
        for name in ("send", "recv", "share"):
            scratch[f"{name}{level}"] = vmem((size, tall, rank), bf16)
        scratch[f"out{level}"] = vmem((2, tall, rank), bf16)
        if count > 1:
            scratch[f"hop{level}"] = vmem((count, tall, rank), bf16)
    scratch["load_sem"] = dma((5,))
    scratch["side_sem"] = dma((LEVELS + 1,))
    scratch["wt_recv"] = dma((2,))
    scratch["p1_recv"] = dma((LEVELS,))
    scratch["p2_recv"] = dma((sum(group_of(n_dev, i + 1)[1] > 1 for i in range(LEVELS)),))
    scratch["p3_recv"] = dma((LEVELS,))
    for name in (
        "all_send", "ag_recv", "fw_recv", "tr_recv", "rs_recv", "out_sem", "own_sem",
    ):
        scratch[name] = dma
    names = ["tgt_h", "train_h", "test_h", "left_h", "right_h", "cap_h", "piv_h"]
    names += ["cur_out", "term_out"] + list(scratch)
    current, terms = pl.pallas_call(
        functools.partial(kernel, n_dev, narrow, names),
        out_shape=(
            jax.ShapeDtypeStruct((width, points), f32),
            jax.ShapeDtypeStruct((pairs * half, 2 * width), bf16),
        ),
        in_specs=[pl.BlockSpec(memory_space=pltpu.HBM)] * 7,
        out_specs=(hbm_spec, hbm_spec),
        scratch_shapes=list(scratch.values()),
        compiler_params=pltpu.CompilerParams(
            collective_id=0, has_side_effects=True, vmem_limit_bytes=48 * 1024 * 1024
        ),
    )(*(
        pltpu.with_memory_space_constraint(value, pltpu.HBM)
        for value in (
            targets.T, train, test.reshape(2, half, feat), left, right, cap, pivots
        )
    ))
    current, predictions = pl.pallas_call(
        finish,
        out_shape=(
            jax.ShapeDtypeStruct((width, points), f32),
            jax.ShapeDtypeStruct((rows, width), f32),
        ),
        in_specs=[vmem_spec] * 2,
        out_specs=(hbm_spec, hbm_spec),
        scratch_shapes=[vmem((rows, width), f32), dma((5,))],
    )(*(
        pltpu.with_memory_space_constraint(value, pltpu.VMEM) for value in (current, terms)
    ))
    return current.T, predictions


def solution(mesh):
    both = ("wide", "narrow")
    placed = (
        P(both, None), P(both, None), P(both, None),
        P(both, None, None), P(both, None, None), P(), P(),
    )
    sizes = dict(mesh.shape)
    return jax.shard_map(
        functools.partial(body, sizes["wide"] * sizes["narrow"], sizes["narrow"]),
        mesh=mesh,
        in_specs=placed,
        out_specs=(P(both, None), P(both, None)),
        check_vma=False,
    )
```

```python
import functools
import math
import types

import jax
import jax.numpy as jnp
from jax import lax
from jax.experimental import pallas as pl
from jax.experimental.pallas import tpu as pltpu
from jax.sharding import PartitionSpec as P

LEVELS = 4
OCTET = 8
spread_coef = 3.0
MESH = pl.DeviceIdType.MESH
f32, bf16 = jnp.float32, jnp.bfloat16


def dot(a, b):
    return jnp.dot(a, b, preferred_element_type=f32)


def dot_nt(a, b):
    return lax.dot_general(a, b, (((1,), (1,)), ((), ())), preferred_element_type=f32)


def split(value):
    high = value.astype(bf16)
    return high, (value - high.astype(f32)).astype(bf16)


def halves_of(value):
    high = value.astype(bf16).astype(f32)
    return high, value - high


def far_first(size):
    return sorted(range(1, size), key=lambda k: -(k >> 1).bit_count())


def group_of(n_dev, level):
    node = n_dev >> (level - 1)
    size = min(OCTET, node)
    return size, node // size


def kernel(n_dev, narrow, names, *refs):
    r = types.SimpleNamespace(**dict(zip(names, refs)))
    pos = lax.axis_index("wide") * narrow + lax.axis_index("narrow")
    width, points = r.tgt.shape
    rank = r.right_h.shape[2]
    feat = r.train.shape[2]
    half = r.test_h.shape[1]
    rows = 2 * half
    pairs = n_dev // 2
    parity = pos % 2
    slot = pos // 2
    octets = n_dev // OCTET
    seat = slot % (OCTET // 2)
    own_block = seat * octets + slot // (OCTET // 2)
    own_rows = pl.ds(pl.multiple_of(own_block * half, half), half)
    seat_rows = pl.ds(pl.multiple_of(seat * octets * half, octets * half), octets * half)

    def coords(dev):
        return (dev // narrow, dev % narrow)

    def flip(mask):
        dev = pos
        for bit in range(mask.bit_length()):
            if mask >> bit & 1:
                dev = dev + (1 << bit) * (1 - 2 * ((pos // (1 << bit)) % 2))
        return coords(dev)

    def remote(src, dst, send_sem, recv_sem, where):
        pltpu.make_async_remote_copy(
            src_ref=src, dst_ref=dst, send_sem=send_sem, recv_sem=recv_sem,
            device_id=where, device_id_type=MESH,
        ).start()

    def drain(part, sem):
        pltpu.make_async_copy(part, part, sem).wait()

    def load(src, dst, sem):
        copy = pltpu.make_async_copy(src, dst, sem)
        copy.start()
        return copy

    barrier = pltpu.get_barrier_semaphore()

    def greet(k, carry):
        pl.semaphore_signal(
            barrier, inc=1, device_id=coords((pos + OCTET * k) % n_dev), device_id_type=MESH
        )
        return carry

    def side(i, count=1):
        return pl.ds(i * points, count * points)

    def load_side(i):
        source = (r.right_h, r.left_h)[i % 2].at[:, i // 2, :]
        load(source, r.side.at[side(i)], r.side_sem.at[(i + 1) // 2])

    tgt_load = load(r.tgt_h, r.tgt, r.load_sem.at[0])
    load_side(0)
    lax.fori_loop(1, octets, greet, 0)
    for k in range(1, OCTET):
        pl.semaphore_signal(barrier, inc=1, device_id=flip(k), device_id_type=MESH)
    test_load = load(r.test_h, r.gath.at[:, own_rows], r.load_sem.at[1])
    for i in range(1, 2 * LEVELS):
        load_side(i)
        if i == 2:
            train_load = load(r.train_h, r.train.at[0], r.load_sem.at[2])
    piv_load = load(r.piv_h, r.piv, r.load_sem.at[3])
    odds, heaps = [], []
    for level in range(1, LEVELS + 1):
        child = pos // (n_dev >> level)
        odds.append(child % 2)
        heaps.append((1 << level - 1) - 1 + child // 2)
        load(r.cap_h.at[heaps[-1]], r.cap.at[level - 1], r.load_sem.at[4])

    def first_send(level):
        size, _ = group_of(n_dev, level)
        mine = pos % size
        lev = level - 1
        for k in far_first(size):
            to = mine
            for bit in range(k.bit_length()):
                if k >> bit & 1:
                    to = to + (1 << bit) * (1 - 2 * ((mine // (1 << bit)) % 2))
            remote(
                getattr(r, f"send{level}").at[to], getattr(r, f"recv{level}").at[k],
                r.all_send, r.p1_recv.at[lev], flip(k),
            )

    def gram(level):
        lev = level - 1
        size, _ = group_of(n_dev, level)
        if level == 1:
            drain(r.side.at[side(0)], r.side_sem.at[0])
        high, low = split(r.side[side(2 * lev)])
        product = dot(r.stack[pl.ds(0, 2 * width + lev * rank)], high)
        t = product[:width] + product[width : 2 * width] + dot(r.stack[pl.ds(0, width)], low)
        t_high, t_low = halves_of(t)
        part = width // size
        both = jnp.concatenate(
            [t_high.reshape(size, part, rank), t_low.reshape(size, part, rank)], axis=1
        )
        send = getattr(r, f"send{level}")
        send[:, pl.ds(0, 2 * part)] = both.astype(bf16)
        cut = rank // size
        for k in range(lev):
            piece = product[2 * width + k * rank : 2 * width + (k + 1) * rank]
            send[:, pl.ds(2 * part + k * cut, cut)] = piece.astype(bf16).reshape(size, cut, rank)

    def turn(lev):
        drain(r.side.at[side(2 * lev + 1, min(2, 2 * LEVELS - 1 - 2 * lev))], r.side_sem.at[lev + 1])
        high, low = split(r.side[side(2 * lev + 1)].T)
        r.stack[pl.ds(2 * width + lev * rank, rank)] = high
        r.ltl[pl.ds(lev * rank, rank)] = low

    sums = {}
    late = [level for level in range(1, LEVELS + 1) if group_of(n_dev, level)[1] > 1]
    landed_late = []

    def tall_of(level):
        return getattr(r, f"send{level}").shape[1]

    def late_at(level):
        return sum(tall_of(other) for other in late if other < level)

    def joined(value, level):
        part = width // group_of(n_dev, level)[0]
        top = value[:part] + value[part : 2 * part]
        return top if level == 1 else jnp.concatenate([top, value[2 * part :]], axis=0)

    def packed(value, level):
        part = width // group_of(n_dev, level)[0]
        high, low = halves_of(value[:part])
        pieces = [high, low] if level == 1 else [high, low, value[part:]]
        return jnp.concatenate(pieces, axis=0).astype(bf16)

    def first_take(level):
        size, count = group_of(n_dev, level)
        lev = level - 1
        recv, send = getattr(r, f"recv{level}"), getattr(r, f"send{level}")
        drain(recv.at[pl.ds(1, size - 1)], r.p1_recv.at[lev])
        near = send[pos % size].astype(f32)
        far = None
        for k in range(1, size):
            value = recv[k].astype(f32)
            if count > 1 or k < size // 2:
                near = near + value
            else:
                far = value if far is None else far + value
        near = joined(near, level)
        if count == 1:
            sums[level] = (near, joined(far, level))
            return
        sums[level] = (near, None)
        hop = getattr(r, f"hop{level}")
        hop[0] = packed(near, level)
        for j in range(count - 1, 0, -1):
            remote(hop.at[0], hop.at[j], r.all_send, r.p2_recv.at[lev], flip(j * OCTET))

    def second_take(level):
        size, count = group_of(n_dev, level)
        if count == 1:
            return
        hop = getattr(r, f"hop{level}")
        drain(hop.at[pl.ds(1, count - 1)], r.p2_recv.at[level - 1])
        near, far = sums[level][0], None
        for j in range(1, count):
            value = joined(hop[j].astype(f32), level)
            if j < count // 2:
                near = near + value
            else:
                far = value if far is None else far + value
        sums[level] = (near, far)

    def solved(level):
        _, count = group_of(n_dev, level)
        lev = level - 1
        near, far = sums[level]
        cols = near.shape[0]
        both = jnp.concatenate([near, far], axis=1)
        high, low = halves_of(both)
        moved = dot(jnp.concatenate([high, low], axis=0).astype(bf16), r.chosen[lev])
        odd = odds[lev]
        kids = 1 if count > 1 else 2
        taken = pl.ds(pl.multiple_of(odd * rank, rank), rank) if kids == 1 else pl.ds(0, 2 * rank)
        cap_high, cap_low = r.caps[0, lev, taken], r.caps[1, lev, taken]
        result = dot_nt(moved.astype(bf16), cap_high)
        return result[:cols] + result[cols:] + dot_nt(moved[:cols].astype(bf16), cap_low)

    def give(level, result):
        size, count = group_of(n_dev, level)
        lev = level - 1
        odd = odds[lev]
        kids = 1 if count > 1 else 2
        share, out = getattr(r, f"share{level}"), getattr(r, f"out{level}")
        for kid in range(kids):
            out[kid] = packed(result[:, kid * rank : (kid + 1) * rank], level)
        mine = pos % size
        for k in far_first(size):
            kid = 0 if kids == 1 else odd if k < size // 2 else 1 - odd
            remote(
                out.at[kid], share.at[mine], r.all_send, r.p3_recv.at[lev], flip(k)
            )
        share[mine] = out[0 if kids == 1 else odd]

    def gathered(level):
        size, _ = group_of(n_dev, level)
        share, base = (r.share_late, late_at(level)) if level in late else (getattr(r, f"share{level}"), 0)
        if level not in late:
            drain(share.at[pl.ds(0, size - 1)], r.p3_recv.at[level - 1])
        elif not landed_late:
            landed_late.append(level)
            drain(share.at[pl.ds(0, size - 1)], r.late_recv)
        part, cut = width // size, rank // size
        top = share[:, pl.ds(base, 2 * part)].astype(f32)
        top = (top[:, :part] + top[:, part:]).reshape(width, rank)
        return [top] + [
            share[:, pl.ds(base + 2 * part + k * cut, cut)].reshape(rank, rank)
            for k in range(level - 1)
        ]

    def prepare(lev):
        high, low = split(r.cap[lev])
        r.caps[0, lev] = high
        r.caps[1, lev] = low
        order = lax.broadcasted_iota(jnp.int32, (2 * rank, 2 * rank), 0)
        pivots = r.piv[pl.ds(heaps[lev], 1), :]
        at = pivots + rank * (1 - odds[lev])
        at = jnp.where(at >= 2 * rank, at - 2 * rank, at)
        r.chosen[lev] = (order == at).astype(f32).astype(bf16)

    def widened(value, own_squares_at, ones_at):
        value_f = value.astype(f32)
        high, low = split(value_f * value_f)
        squares = dot(
            jnp.concatenate([high, low], axis=1), jnp.ones((2 * feat, feat), bf16)
        )
        one = squares.astype(bf16).astype(f32)
        two = (squares - one).astype(bf16).astype(f32)
        three = squares - one - two
        lane = lax.broadcasted_iota(jnp.int32, squares.shape, 1)
        extra = jnp.where((lane >= ones_at) & (lane < ones_at + 3), 1.0, 0.0)
        for i, piece in enumerate((one, two, three)):
            extra = jnp.where(lane == own_squares_at + i, -piece, extra)
        return extra.astype(bf16)

    def widen_train(which):
        value = r.train[which]
        r.train_w[which, :, pl.ds(0, feat)] = value + value
        r.train_w[which, :, pl.ds(feat, feat)] = widened(value, 3, 0)

    def widen_tests():
        def step(i, carry):
            part = pl.ds(pl.multiple_of(i * wide_rows, wide_rows), wide_rows)
            for h in range(2):
                value = r.gath[h, part]
                there = pl.ds(
                    pl.multiple_of(h * pairs * half + i * wide_rows, wide_rows), wide_rows
                )
                r.test_w[there, pl.ds(0, feat)] = value
                r.test_w[there, pl.ds(feat, feat)] = widened(value, 0, 3)
            return carry

        wide_rows = min(256, pairs * half)
        lax.fori_loop(0, pairs * half // wide_rows, step, 0)

    rate = spread_coef / feat * math.log2(math.e)
    chunk = min(512, pairs * rows)

    def fill(which):
        def step(i, carry):
            part = pl.ds(pl.multiple_of(i * chunk, chunk), chunk)
            negative = dot_nt(r.test_w[part], r.train_w[which])
            r.kmat[part, pl.ds(which * points, points)] = jnp.exp2(rate * negative).astype(bf16)
            return carry

        lax.fori_loop(0, pairs * rows // chunk, step, 0)

    tgt_load.wait()
    high, low = split(r.tgt[...])
    r.stack[pl.ds(0, width)] = high
    r.stack[pl.ds(width, width)] = low
    gram(1)
    turn(0)
    test_load.wait()
    pl.semaphore_wait(barrier, octets - 1 + OCTET - 1)
    first_send(1)
    own_test = r.gath.at[:, own_rows]

    def spread(k, carry):
        remote(own_test, own_test, r.all_send, r.ag_recv, coords((pos + OCTET * k) % n_dev))
        return carry

    lax.fori_loop(1, octets, spread, 0)
    gram(2)
    first_send(2)
    train_load.wait()
    remote(r.train.at[0], r.train.at[1], r.all_send, r.tr_recv, flip(1))
    turn(1)
    gram(3)
    first_send(3)
    turn(2)
    gram(4)
    first_send(4)
    widen_train(0)
    piv_load.wait()
    drain(r.cap, r.load_sem.at[4])
    for lev in range(LEVELS):
        prepare(lev)
    first_take(1)
    drain(r.gath.at[:, pl.ds(0, (octets - 1) * half)], r.ag_recv)
    seat_test = r.gath.at[:, seat_rows]
    for k in range(2, OCTET, 2):
        remote(seat_test, seat_test, r.all_send, r.fw_recv, flip(k))
    first_take(2)
    first_take(3)
    if group_of(n_dev, 3)[1] == 1:
        give(3, solved(3))
    first_take(4)
    if group_of(n_dev, 4)[1] == 1:
        give(4, solved(4))
    for level in late:
        second_take(level)
    results = [solved(level) for level in late]
    for level, result in zip(late, results):
        r.out_late[pl.ds(late_at(level), tall_of(level))] = packed(result, level)
    seat_in_group = pos % OCTET
    for k in far_first(OCTET):
        remote(
            r.out_late, r.share_late.at[seat_in_group], r.all_send, r.late_recv, flip(k)
        )
    r.share_late[seat_in_group] = r.out_late[...]
    drain(r.train.at[0], r.tr_recv)
    widen_train(1)
    turn(LEVELS - 1)
    drain(r.gath.at[:, pl.ds(0, (OCTET // 2 - 1) * octets * half)], r.fw_recv)
    widen_tests()
    fill(0)
    fill(1)

    third, fourth = gathered(3), gathered(4)
    high, low = split(third[0])
    product = dot(jnp.concatenate([high, low, third[1], third[2]], axis=0), fourth[3])
    r.base[:, pl.ds(0, rank)] = third[0]
    r.base[:, pl.ds(rank, rank)] = fourth[0] - (product[:width] + product[width : 2 * width])
    for k in range(2):
        there = pl.ds(k * rank, rank)
        r.mix[there, pl.ds(0, rank)] = third[1 + k]
        at = 2 * width + k * rank
        high, low = split(fourth[1 + k].astype(f32) - product[at : at + rank])
        r.mix[there, pl.ds(rank, rank)] = high
        r.mix_low[there] = low
    base_high, base_low = split(r.base[...])
    mixed = jnp.concatenate([base_high, base_low, r.mix[...]], axis=0)
    mixed_high = jnp.concatenate([base_high, r.mix[...]], axis=0)
    wide = min(512, points)
    for i in range(points // wide):
        cut = pl.ds(i * wide, wide)
        top = dot(mixed, r.stack[pl.ds(2 * width + 2 * rank, 2 * rank), cut])
        bottom = dot(mixed_high, r.ltl[pl.ds(2 * rank, 2 * rank), cut])
        r.cur0[:, cut] = r.tgt[:, cut] - (top[:width] + top[width : 2 * width] + bottom[:width])
        rest = dot(r.mix_low[...], r.stack[pl.ds(2 * width + 3 * rank, rank), cut])
        own = r.stack[pl.ds(2 * width, 2 * rank), cut].astype(f32)
        own = own + r.ltl[pl.ds(0, 2 * rank), cut].astype(f32)
        high, low = split(own - (top[2 * width :] + bottom[width:] + rest))
        r.leff[0, :, cut] = high
        r.leff[1, :, cut] = low
    second = gathered(2)
    first = gathered(1)[0]
    high, low = split(first)
    product = dot(jnp.concatenate([high, low], axis=0), second[1])
    upper = jnp.concatenate([first, second[0] - (product[:width] + product[width:])], axis=1)
    high, low = split(upper)
    both = jnp.concatenate([high, low], axis=0)
    for h in range(2):
        cut = pl.ds(h * (points // 2), points // 2)
        product = dot(both, r.leff[0, :, cut])
        current = r.cur0[:, cut] - (product[:width] + product[width:] + dot(high, r.leff[1, :, cut]))
        r.cur[:, cut] = current
        r.wt[0, h] = current.astype(bf16)
        remote(r.wt.at[0, h], r.wt.at[1, h], r.all_send, r.wt_recv.at[h], flip(1))
    cur_copy = pltpu.make_async_copy(r.cur, r.cur_out, r.out_sem)
    cur_copy.start()

    big = min(256, pairs * half)

    def weigh(which, h):
        twice = jnp.concatenate([r.wt[which, h], r.wt[which, h]], axis=0)
        first_half = lax.broadcasted_iota(jnp.int32, (big, 2 * width), 1) < width

        def step(i, carry):
            part = pl.ds(pl.multiple_of(i * big, big), big)
            other = pl.ds(pl.multiple_of(pairs * half + i * big, big), big)
            there = pl.ds((2 * which + h) * (points // 2), points // 2)
            value = jnp.where(
                first_half, dot_nt(r.kmat[part, there], twice), dot_nt(r.kmat[other, there], twice)
            )
            if which or h:
                value = r.terms[part] + value
            if which and h:
                r.term_b[part] = value.astype(bf16)
            else:
                r.terms[part] = value
            return carry

        lax.fori_loop(0, pairs * half // big, step, 0)

    for which in range(2):
        for h in range(2):
            if which:
                drain(r.wt.at[1, h], r.wt_recv.at[h])
            weigh(which, h)

    own_copy = pltpu.make_async_copy(
        r.term_b.at[own_rows], r.term_out.at[pl.ds((pairs - 1) * half, half)], r.own_sem
    )
    own_copy.start()
    for turned in (3, 2, 1, 0):
        base = pos
        for bit in range(2):
            if turned >> bit & 1:
                base = base + (2 << bit) * (1 - 2 * ((pos // (2 << bit)) % 2))

        def scatter(j, carry, base=base, turned=turned):
            to = (base + OCTET * j) % n_dev
            block = ((to // 2) % (OCTET // 2)) * octets + to // OCTET
            remote(
                r.term_b.at[pl.ds(pl.multiple_of(block * half, half), half)],
                r.term_out.at[pl.ds(pl.multiple_of((turned * octets + j - 1) * half, half), half)],
                r.all_send, r.rs_recv, coords(to),
            )
            return carry

        start = 0 if turned else 1
        if octets <= 4:
            for j in range(start, octets):
                scatter(j, 0)
        else:
            lax.fori_loop(start, octets, scatter, 0)
    cur_copy.wait()
    own_copy.wait()
    landed = r.term_out.at[pl.ds(0, (pairs - 1) * half)]
    drain(landed, r.rs_recv)
    sent = 2 * points * feat + 2 * width * points
    sent += 2 * 2 * half * feat * (octets - 1 + (OCTET // 2 - 1) * octets) + 2 * (pairs - 1) * half * 2 * width
    for level in range(1, LEVELS + 1):
        size, count = group_of(n_dev, level)
        piece = 2 * getattr(r, f"send{level}").shape[1] * rank
        sent += piece * (2 * (size - 1) + count - 1)
    drain(r.side.at[pl.ds(0, sent // (4 * rank))], r.all_send)


def finish(cur_in, terms_in, cur_out, pred_out, pred, sems):
    parts = sems.shape[0] - 1
    tall = cur_in.shape[0] // parts
    copies = [
        pltpu.make_async_copy(
            cur_in.at[pl.ds(i * tall, tall)], cur_out.at[pl.ds(i * tall, tall)], sems.at[i]
        )
        for i in range(parts)
    ]
    for copy in copies:
        copy.start()
    half, width = pred.shape[0] // 2, pred.shape[1]
    terms = terms_in[...].astype(f32)
    total = jnp.sum(terms.reshape(terms.shape[0] // half, half, 2 * width), axis=0)
    pred[pl.ds(0, half)] = total[:, :width]
    pred[pl.ds(half, half)] = total[:, width:]
    copies.append(pltpu.make_async_copy(pred, pred_out, sems.at[parts]))
    copies[-1].start()
    for copy in copies:
        copy.wait()


def body(n_dev, narrow, targets, train, test, left, right, cap, pivots):
    points, width = targets.shape
    rank = left.shape[2]
    feat = train.shape[1]
    rows = test.shape[0]
    half = rows // 2
    pairs = n_dev // 2
    vmem = pltpu.VMEM
    dma = pltpu.SemaphoreType.DMA
    hbm_spec = pl.BlockSpec(memory_space=pl.ANY)
    vmem_spec = pl.BlockSpec(memory_space=pltpu.VMEM)
    scratch = {
        "tgt": vmem((width, points), f32),
        "piv": vmem(pivots.shape, jnp.int32),
        "train": vmem((2, points, feat), bf16),
        "gath": vmem((2, pairs * half, feat), bf16),
        "side": vmem((2 * LEVELS * points, rank), f32),
        "cur0": vmem((width, points), f32),
        "leff": vmem((2, 2 * rank, points), bf16),
        "cap": vmem((LEVELS, 2 * rank, 2 * rank), f32),
        "caps": vmem((2, LEVELS, 2 * rank, 2 * rank), bf16),
        "chosen": vmem((LEVELS, 2 * rank, 2 * rank), bf16),
        "stack": vmem((2 * width + LEVELS * rank, points), bf16),
        "ltl": vmem((LEVELS * rank, points), bf16),
        "train_w": vmem((2, points, 2 * feat), bf16),
        "test_w": vmem((pairs * rows, 2 * feat), bf16),
        "kmat": vmem((pairs * rows, 2 * points), bf16),
        "base": vmem((width, 2 * rank), f32),
        "mix": vmem((2 * rank, 2 * rank), bf16),
        "mix_low": vmem((2 * rank, rank), bf16),
        "cur": vmem((width, points), f32),
        "wt": vmem((2, 2, width, points // 2), bf16),
        "terms": vmem((pairs * half, 2 * width), f32),
        "term_b": vmem((pairs * half, 2 * width), bf16),
    }
    tall_late = 0
    for level in range(1, LEVELS + 1):
        size, count = group_of(n_dev, level)
        tall = (2 * width + (level - 1) * rank) // size
        for name in ("send", "recv") if count > 1 else ("send", "recv", "share"):
            scratch[f"{name}{level}"] = vmem((size, tall, rank), bf16)
        if count == 1:
            scratch[f"out{level}"] = vmem((2, tall, rank), bf16)
        else:
            tall_late += tall
            scratch[f"hop{level}"] = vmem((count, tall, rank), bf16)
    scratch["out_late"] = vmem((tall_late, rank), bf16)
    scratch["share_late"] = vmem((OCTET, tall_late, rank), bf16)
    scratch["late_recv"] = dma
    scratch["load_sem"] = dma((5,))
    scratch["side_sem"] = dma((LEVELS + 1,))
    scratch["wt_recv"] = dma((2,))
    scratch["p1_recv"] = dma((LEVELS,))
    scratch["p2_recv"] = dma((sum(group_of(n_dev, i + 1)[1] > 1 for i in range(LEVELS)),))
    scratch["p3_recv"] = dma((LEVELS,))
    for name in (
        "all_send", "ag_recv", "fw_recv", "tr_recv", "rs_recv", "out_sem", "own_sem",
    ):
        scratch[name] = dma
    names = ["tgt_h", "train_h", "test_h", "left_h", "right_h", "cap_h", "piv_h"]
    names += ["cur_out", "term_out"] + list(scratch)
    current, terms = pl.pallas_call(
        functools.partial(kernel, n_dev, narrow, names),
        out_shape=(
            jax.ShapeDtypeStruct((width, points), f32),
            jax.ShapeDtypeStruct((pairs * half, 2 * width), bf16),
        ),
        in_specs=[pl.BlockSpec(memory_space=pltpu.HBM)] * 7,
        out_specs=(hbm_spec, hbm_spec),
        scratch_shapes=list(scratch.values()),
        compiler_params=pltpu.CompilerParams(
            collective_id=0, has_side_effects=True, vmem_limit_bytes=48 * 1024 * 1024
        ),
    )(*(
        pltpu.with_memory_space_constraint(value, pltpu.HBM)
        for value in (
            targets.T, train, test.reshape(2, half, feat), left, right, cap, pivots
        )
    ))
    current, predictions = pl.pallas_call(
        finish,
        out_shape=(
            jax.ShapeDtypeStruct((width, points), f32),
            jax.ShapeDtypeStruct((rows, width), f32),
        ),
        in_specs=[vmem_spec] * 2,
        out_specs=(hbm_spec, hbm_spec),
        scratch_shapes=[vmem((rows, width), f32), dma((5,))],
    )(*(
        pltpu.with_memory_space_constraint(value, pltpu.VMEM) for value in (current, terms)
    ))
    return current.T, predictions


def solution(mesh):
    both = ("wide", "narrow")
    placed = (
        P(both, None), P(both, None), P(both, None),
        P(both, None, None), P(both, None, None), P(), P(),
    )
    sizes = dict(mesh.shape)
    return jax.shard_map(
        functools.partial(body, sizes["wide"] * sizes["narrow"], sizes["narrow"]),
        mesh=mesh,
        in_specs=placed,
        out_specs=(P(both, None), P(both, None)),
        check_vma=False,
    )
```
